8 devices in a mesh: dp: 1 (over z), tp: 2 (over y), sq: 4 (over x, core).
Axes of the slice: x: 2, y: 2, z: 1, core: 2. Of those that a mesh axis runs over, the one named last changes fastest.
Arguments:
- hidden: bfloat16 [256, 4096], P('dp')
- cache_lens: int32 [256], P('dp')
- k_cache: bfloat16 [256, 1024, 128], P('dp', 'sq')
- v_cache: bfloat16 [256, 1024, 128], P('dp', 'sq')
- ln_gain: float32 [4096], replicated
- ln_bias: float32 [4096], replicated
- w_query: bfloat16 [4096, 4096], P(None, 'tp')
- b_query: float32 [4096], P('tp')
- w_kv: bfloat16 [4096, 256], replicated
- b_kv: float32 [256], replicated
- w_out: bfloat16 [4096, 4096], P('tp')
- b_out: float32 [4096], replicated
Outputs:
- output 1: bfloat16 [256, 4096], P('dp')
- output 2: bfloat16 [256, 1024, 128], P('dp', 'sq')
- output 3: bfloat16 [256, 1024, 128], P('dp', 'sq')
All inputs are finite; a program needn't handle non-finite values.
Results may differ from the reference program's by a relative error of at most 0.00346761.
Values sent between devices are 32-bit elements.
A program may use at most 1 GiB of HBM per device.

```python
import math
import jax
import jax.numpy as jnp
from jax import lax

BATCH = 256
CACHE_LEN = 1024
D_MODEL = 4096
HEADS = 32
HEAD_DIM = 128


def layer_norm(x_rows, ln_gain, ln_bias):
    x_wide = x_rows.astype(jnp.float32)
    mean_val = jnp.mean(x_wide, axis=-1, keepdims=True)
    centered = x_wide - mean_val
    variance = jnp.mean(centered * centered, axis=-1, keepdims=True)
    normed = centered * lax.rsqrt(variance + 1e-5)
    return (normed * ln_gain + ln_bias).astype(jnp.bfloat16)


def setup_inputs(seed: int = 0, part: int = 0) -> dict:
    own_keys = jax.random.split(jax.random.fold_in(jax.random.key(seed), part), 5)
    shared_keys = jax.random.split(jax.random.key(seed + 1), 10)
    q_width = HEADS * HEAD_DIM
    score_var = max(1.0, math.log(CACHE_LEN / 32.0))
    key_scale = math.sqrt(score_var / 2.0)
    self_bias = (math.log(0.6 * CACHE_LEN) + 0.5 * score_var) / math.sqrt(HEAD_DIM)
    hidden = jax.random.normal(own_keys[0], (BATCH, D_MODEL), jnp.float32).astype(jnp.bfloat16)
    drawn = CACHE_LEN - 1 - jax.random.randint(own_keys[1], (BATCH,), 0, CACHE_LEN // 2)
    order = jax.random.permutation(own_keys[2], BATCH)
    seq_ids = jnp.arange(BATCH)
    cache_lens = jnp.where(seq_ids == order[0], CACHE_LEN - 1, jnp.where(seq_ids == order[1], 1, drawn)).astype(jnp.int32)
    k_cache = (key_scale * jax.random.normal(own_keys[3], (BATCH, CACHE_LEN, HEAD_DIM), jnp.float32)).astype(jnp.bfloat16)
    v_cache = jax.random.normal(own_keys[4], (BATCH, CACHE_LEN, HEAD_DIM), jnp.float32).astype(jnp.bfloat16)
    ln_gain = 1.0 + 0.3 * jax.random.normal(shared_keys[0], (D_MODEL,), jnp.float32)
    ln_bias = 0.3 * jax.random.normal(shared_keys[1], (D_MODEL,), jnp.float32)
    w_query = (jax.random.normal(shared_keys[2], (D_MODEL, q_width), jnp.float32) * D_MODEL ** -0.5).astype(jnp.bfloat16)
    shared_dir = jax.random.normal(shared_keys[3], (HEAD_DIM,), jnp.float32)
    b_query = jnp.tile(shared_dir, HEADS) + 0.2 * jax.random.normal(shared_keys[4], (q_width,), jnp.float32)
    w_kv = (jax.random.normal(shared_keys[5], (D_MODEL, 2 * HEAD_DIM), jnp.float32) * D_MODEL ** -0.5).astype(jnp.bfloat16)
    key_bias = self_bias * shared_dir + 0.2 * jax.random.normal(shared_keys[6], (HEAD_DIM,), jnp.float32)
    val_bias = 0.5 * jax.random.normal(shared_keys[7], (HEAD_DIM,), jnp.float32)
    b_kv = jnp.concatenate([key_bias, val_bias])
    w_out = (jax.random.normal(shared_keys[8], (q_width, D_MODEL), jnp.float32) * q_width ** -0.5).astype(jnp.bfloat16)
    b_out = 0.3 * jax.random.normal(shared_keys[9], (D_MODEL,), jnp.float32)
    return {"hidden": hidden, "cache_lens": cache_lens, "k_cache": k_cache, "v_cache": v_cache, "ln_gain": ln_gain, "ln_bias": ln_bias, "w_query": w_query, "b_query": b_query, "w_kv": w_kv, "b_kv": b_kv, "w_out": w_out, "b_out": b_out}


def reference(hidden, cache_lens, k_cache, v_cache, ln_gain, ln_bias, w_query, b_query, w_kv, b_kv, w_out, b_out):
    normed = layer_norm(hidden, ln_gain, ln_bias)
    query = (jnp.dot(normed, w_query, preferred_element_type=jnp.float32) + b_query).astype(jnp.bfloat16)
    query = query.reshape(BATCH, HEADS, HEAD_DIM)
    key_val = (jnp.dot(normed, w_kv, preferred_element_type=jnp.float32) + b_kv).astype(jnp.bfloat16)
    positions = jnp.arange(CACHE_LEN, dtype=jnp.int32)
    at_slot = (positions[None, :] == cache_lens[:, None])[:, :, None]
    key_new = jnp.where(at_slot, key_val[:, None, :HEAD_DIM], k_cache)
    val_new = jnp.where(at_slot, key_val[:, None, HEAD_DIM:], v_cache)

    def one_sequence(packed):
        query_row, key_rows, val_rows, length = packed
        scores = jnp.einsum("nd,td->nt", query_row.astype(jnp.float32), key_rows.astype(jnp.float32)) * (HEAD_DIM ** -0.5)
        valid = positions <= length
        scores = jnp.where(valid[None, :], scores, -jnp.inf)
        weights = jax.nn.softmax(scores, axis=-1)
        return jnp.einsum("nt,td->nd", weights, val_rows.astype(jnp.float32)).astype(jnp.bfloat16)

    attended = lax.map(one_sequence, (query, key_new, val_new, cache_lens))
    projected = jnp.dot(attended.reshape(BATCH, HEADS * HEAD_DIM), w_out, preferred_element_type=jnp.float32)
    out_hidden = (hidden.astype(jnp.float32) + projected + b_out).astype(jnp.bfloat16)
    return (out_hidden, key_new, val_new)
```

```python
import functools
import math

import jax
import jax.numpy as jnp
from jax import lax
from jax.experimental import pallas as pl
from jax.experimental.pallas import tpu as pltpu
from jax.sharding import PartitionSpec as P

MESH = pl.DeviceIdType.MESH
F32 = jnp.float32
BF16 = jnp.bfloat16
NEG = -1e30
B = 256
D = 4096
H = 16
DH = 128
T = 256
NC = 4
CS = B // NC
S = CS // 4
HALF = S // 2
QB = 512
NQ = H * DH // QB
QSCALE = DH ** -0.5 * math.log2(math.e)
GROUP = 8
MIB = 1024 * 1024


def attention_kernel(lens, hid_hbm, k_hbm, v_hbm, gain_ref, bias_ref, wq_hbm, bq_ref, wkv_hbm, bkv_ref,
                     o_ref, lse_ref, ko_hbm, vo_hbm,
                     hid, h, wq, wkv, q3, kv, kbuf, vbuf, wsem, ksem, vsem, osem):
    first = lax.axis_index("sq") * T
    load_h = pltpu.make_async_copy(hid_hbm, hid, wsem.at[NQ])
    load_h.start()
    load_wq = []
    for j in range(NQ):
        cols = pl.ds(j * QB, QB)
        load_wq.append(pltpu.make_async_copy(wq_hbm.at[:, cols], wq.at[:, cols], wsem.at[j]))
    load_wkv = pltpu.make_async_copy(wkv_hbm, wkv, wsem.at[NQ + 1])
    load_wkv.start()
    for c in load_wq:
        c.start()
    load_k, load_v = [], []
    for k in range(NC):
        rows = pl.ds(k * CS, CS)
        load_k.append(pltpu.make_async_copy(k_hbm.at[rows], kbuf.at[rows], ksem.at[k]))
        load_v.append(pltpu.make_async_copy(v_hbm.at[rows], vbuf.at[rows], vsem.at[k]))
        load_k[-1].start()
        load_v[-1].start()
    load_h.wait()

    def norm_rows(i, _):
        rows = pl.ds(pl.multiple_of(i * 16, 16), 16)
        x = hid[rows, :].astype(F32)
        mean = jnp.sum(x, axis=-1, keepdims=True) * (1.0 / D)
        cen = x - mean
        var = jnp.sum(cen * cen, axis=-1, keepdims=True) * (1.0 / D)
        y = cen * lax.rsqrt(var + 1e-5)
        h[rows, :] = (y * gain_ref[...] + bias_ref[...]).astype(BF16)
        return 0

    lax.fori_loop(0, B // 16, norm_rows, 0, unroll=2)
    load_wkv.wait()
    new_kv = (jnp.dot(h[...], wkv[...], preferred_element_type=F32) + bkv_ref[...]).astype(BF16).astype(F32)
    kv[0:B, :] = new_kv[:, :DH]
    kv[B:2 * B, :] = new_kv[:, DH:]
    for j in range(NQ):
        load_wq[j].wait()
        cols = pl.ds(j * QB, QB)
        q = jnp.dot(h[...], wq[:, cols], preferred_element_type=F32) + bq_ref[:, cols]
        q = q.astype(BF16).astype(F32)
        for n in range(QB // DH):
            q3[pl.ds(j * (QB // DH) + n, B, stride=H), :] = q[:, n * DH:(n + 1) * DH]

    sub = lax.broadcasted_iota(jnp.int32, (16, DH), 0)
    lane = lax.broadcasted_iota(jnp.int32, (H, DH), 1)
    pos = lax.broadcasted_iota(jnp.int32, (H, T), 1)
    zero = jnp.zeros((H, DH), BF16)

    def insert(b, _):
        row = lens[b] - first
        start = pl.multiple_of((jnp.clip(row, 0, T - 1) // 16) * 16, 16)
        hit = sub == row - start
        for buf, c in ((kbuf, 0), (vbuf, 1)):
            new = kv[pl.ds(c * B + b, 1), :]
            old = buf[b, pl.ds(start, 16), :].astype(F32)
            buf[b, pl.ds(start, 16), :] = jnp.where(hit, new, old).astype(BF16)
        return 0

    def attend(i, k):
        base = i * GROUP
        lses = lse_ref[pl.ds(k * H, H), :]
        for u in range(0, GROUP, 2):
            b = base + u
            q0 = q3[pl.ds(pl.multiple_of(b * H, H), H), :].astype(BF16)
            q1 = q3[pl.ds(pl.multiple_of(b * H + H, H), H), :].astype(BF16)
            lhs = jnp.concatenate([jnp.concatenate([q0, zero], 1), jnp.concatenate([zero, q1], 1)], 0)
            keys = jnp.concatenate([kbuf[b], kbuf[b + 1]], 1)
            vals = jnp.concatenate([vbuf[b], vbuf[b + 1]], 1)
            s = lax.dot_general(lhs, keys, (((1,), (1,)), ((), ())), preferred_element_type=F32)
            ps, ls, ms = [], [], []
            for e in range(2):
                se = jnp.where(pos <= lens[b + e] - first, s[e * H:(e + 1) * H] * QSCALE, NEG)
                m = jnp.max(se, axis=1, keepdims=True)
                p = jnp.exp2(se - m)
                ps.append(p)
                ms.append(m)
                ls.append(jnp.sum(p, axis=1, keepdims=True))
            o = jnp.dot(jnp.concatenate(ps, 0).astype(BF16), vals, preferred_element_type=F32)
            for e in range(2):
                o_ref[pl.ds(pl.multiple_of((b + e) * H, H), H), :] = o[e * H:(e + 1) * H, e * DH:(e + 1) * DH] / ls[e]
                lses = jnp.where(lane == b + e - k * CS, ms[e] + jnp.log2(ls[e]), lses)
        lse_ref[pl.ds(k * H, H), :] = lses
        return k

    stores = []
    for k in range(NC):
        load_k[k].wait()
        load_v[k].wait()
        lse_ref[pl.ds(k * H, H), :] = jnp.zeros((H, DH), F32)
        lax.fori_loop(k * CS, (k + 1) * CS, insert, 0, unroll=4)
        lax.fori_loop(k * CS // GROUP, (k + 1) * CS // GROUP, lambda i, c, k=k: attend(i, k), k)
        rows = pl.ds(k * CS, CS)
        for e, (buf, out) in enumerate(((kbuf, ko_hbm), (vbuf, vo_hbm))):
            st = pltpu.make_async_copy(buf.at[rows], out.at[rows], osem.at[2 * k + e])
            st.start()
            stores.append(st)
    for st in stores:
        st.wait()


def column(tile, j):
    return tile[:, j:j + 1]


def merge(la, lb):
    top = jnp.maximum(la, lb)
    wa, wb = jnp.exp2(la - top), jnp.exp2(lb - top)
    tot = wa + wb
    return wa / tot, wb / tot, top + jnp.log2(tot)


def combine_kernel(o_ref, lse_ref, wo_hbm, y_ref,
                   wo, o_core, l_core, o_mix, l_mix, o_x, l_x, a3, part, p_y,
                   wsem, a0s, a0r, a1s, a1r, bs, br, cs, cr, ds, dr):
    sq, tp = lax.axis_index("sq"), lax.axis_index("tp")
    x, c = sq // 2, sq % 2
    mate = {"sq": x * 2 + 1 - c}
    over_x = {"sq": (1 - x) * 2 + c}
    over_y = {"tp": 1 - tp}
    load = pltpu.make_async_copy(wo_hbm, wo, wsem)
    load.start()
    bar = pltpu.get_barrier_semaphore()
    for dev in (mate, over_x, over_y):
        pl.semaphore_signal(bar, inc=1, device_id=dev, device_id_type=MESH)
    pl.semaphore_wait(bar, 3)

    def send(src, dst, ssem, rsem, dev):
        cp = pltpu.make_async_remote_copy(src, dst, ssem, rsem, device_id=dev, device_id_type=MESH)
        cp.start()
        return cp

    W = 2 * S * H
    sent = []
    hop0, hop1, hopb, hopc, hopd = [], [], [], [], []
    for k in range(NC):
        other = pl.multiple_of(k * CS * H + (1 - c) * W, W)
        hop0.append((send(o_ref.at[pl.ds(other, W)], o_core.at[k], a0s.at[k, 0], a0r.at[k, 0], mate),
                     send(lse_ref.at[pl.ds(k * H, H)], l_core.at[k], a0s.at[k, 1], a0r.at[k, 1], mate)))
    for k in range(NC):
        for cp in hop0[k]:
            cp.wait_recv()
        shift = lax.rem(DH - c * 2 * S, DH)
        fa, fb, lm = merge(pltpu.roll(lse_ref[pl.ds(k * H, H), :], shift, 1), pltpu.roll(l_core[k], shift, 1))
        l_mix[k] = lm
        mine = k * CS * H + c * W
        for j in range(2 * S):
            oa = o_ref[pl.ds(pl.multiple_of(mine + j * H, H), H), :]
            ob = o_core[k, j * H:(j + 1) * H, :]
            o_mix[k, j * H:(j + 1) * H, :] = column(fa, j) * oa + column(fb, j) * ob
        far = pl.multiple_of((1 - x) * S * H, S * H)
        hop1.append((send(o_mix.at[k, pl.ds(far, S * H)], o_x.at[k], a1s.at[k, 0], a1r.at[k, 0], over_x),
                     send(l_mix.at[k], l_x.at[k], a1s.at[k, 1], a1r.at[k, 1], over_x)))

    def project(k):
        for cp in hop1[k]:
            cp.wait_recv()
        shift = lax.rem(DH - x * S, DH)
        fa, fb, _ = merge(pltpu.roll(l_mix[k], shift, 1), pltpu.roll(l_x[k], shift, 1))
        near = x * S * H
        for j in range(S):
            oa = o_mix[k, pl.ds(pl.multiple_of(near + j * H, H), H), :]
            ob = o_x[k, j * H:(j + 1) * H, :]
            a3[j * H:(j + 1) * H, :] = column(fa, j) * oa + column(fb, j) * ob
        a = jnp.concatenate([a3[pl.ds(n, S, stride=H), :].astype(BF16) for n in range(H)], 1)
        if k == 0:
            load.wait()

        def cols(i, _):
            cc = pl.ds(pl.multiple_of(i * 1024, 1024), 1024)
            part[k, :, cc] = jnp.dot(a, wo[:, cc], preferred_element_type=F32)
            return 0

        lax.fori_loop(0, D // 1024, cols, 0)
        far = pl.multiple_of((1 - tp) * HALF, HALF)
        hopb.append(send(part.at[k, pl.ds(far, HALF)], p_y.at[k], bs.at[k], br.at[k], over_y))

    def rows_of(k, xx, yy):
        return pl.ds(pl.multiple_of(k * CS + (c * 2 + xx) * S + yy * HALF, HALF), HALF)

    def finish(k):
        hopb[k].wait_recv()
        rows = rows_of(k, x, tp)
        y_ref[rows, :] = part[k, pl.ds(pl.multiple_of(tp * HALF, HALF), HALF), :] + p_y[k]
        hopc.append((send(y_ref.at[rows], y_ref.at[rows], cs.at[k, 0], cr.at[k, 0], over_x),
                     send(y_ref.at[rows], y_ref.at[rows], cs.at[k, 1], cr.at[k, 1], over_y)))
        hopd.append([send(y_ref.at[rows], y_ref.at[rows], ds.at[k, 0], dr.at[k, 0], mate)])

    def relay(k):
        hopc[k][0].wait_recv()
        rows, lo, hi = rows_of(k, 1 - x, tp), pl.ds(0, D // 2), pl.ds(D // 2, D // 2)
        d1 = send(y_ref.at[rows, lo], y_ref.at[rows, lo], cs.at[k, 2], cr.at[k, 2], over_y)
        hopd[k].append(send(y_ref.at[rows], y_ref.at[rows], ds.at[k, 1], dr.at[k, 1], mate))
        hopc[k][1].wait_recv()
        rows = rows_of(k, x, 1 - tp)
        d2 = send(y_ref.at[rows, hi], y_ref.at[rows, hi], cs.at[k, 3], cr.at[k, 3], over_x)
        hopd[k].append(send(y_ref.at[rows], y_ref.at[rows], ds.at[k, 2], dr.at[k, 2], mate))
        hopc[k] = hopc[k] + (d1, d2)

    def last(k):
        hopc[k][2].wait_recv()
        hopc[k][3].wait_recv()
        rows = rows_of(k, 1 - x, 1 - tp)
        hopd[k].append(send(y_ref.at[rows], y_ref.at[rows], ds.at[k, 3], dr.at[k, 3], mate))

    for step in range(NC + 3):
        if step < NC:
            project(step)
        if 0 <= step - 1 < NC:
            finish(step - 1)
        if 0 <= step - 2 < NC:
            relay(step - 2)
        if 0 <= step - 3 < NC:
            last(step - 3)
    for k in range(NC):
        for cp in hopd[k]:
            cp.wait_recv()
    for k in range(NC):
        for cp in hop0[k] + hop1[k] + (hopb[k],) + hopc[k] + tuple(hopd[k]):
            cp.wait_send()


def solution(mesh):
    def local_step(hidden, cache_lens, k_cache, v_cache, ln_gain, ln_bias, w_query, b_query, w_kv, b_kv, w_out, b_out):
        hbm = pl.BlockSpec(memory_space=pltpu.HBM)
        vm = pl.BlockSpec(memory_space=pltpu.VMEM)
        cache = jax.ShapeDtypeStruct((B, T, DH), BF16)
        o, lse, k_new, v_new = pl.pallas_call(
            attention_kernel,
            out_shape=(pltpu.VMEM((B * H, DH), F32), pltpu.VMEM((NC * H, DH), F32), cache, cache),
            in_specs=[pl.BlockSpec(memory_space=pltpu.SMEM), hbm, hbm, hbm, vm, vm, hbm, vm, hbm, vm],
            out_specs=(vm, vm, hbm, hbm),
            scratch_shapes=[
                pltpu.VMEM((B, D), BF16), pltpu.VMEM((B, D), BF16), pltpu.VMEM((D, H * DH), BF16), pltpu.VMEM((D, 2 * DH), BF16),
                pltpu.VMEM((B * H, DH), F32), pltpu.VMEM((2 * B, DH), F32),
                pltpu.VMEM((B, T, DH), BF16), pltpu.VMEM((B, T, DH), BF16),
                pltpu.SemaphoreType.DMA((NQ + 2,)), pltpu.SemaphoreType.DMA((NC,)), pltpu.SemaphoreType.DMA((NC,)),
                pltpu.SemaphoreType.DMA((2 * NC,)),
            ],
            compiler_params=pltpu.CompilerParams(vmem_limit_bytes=60 * MIB),
            name="attention",
        )(cache_lens, hidden, k_cache, v_cache, ln_gain[None], ln_bias[None], w_query, b_query[None], w_kv, b_kv[None])
        sem = pltpu.SemaphoreType.DMA
        y = pl.pallas_call(
            combine_kernel,
            out_shape=pltpu.VMEM((B, D), F32),
            in_specs=[vm, vm, hbm],
            out_specs=vm,
            scratch_shapes=[
                pltpu.VMEM((H * DH, D), BF16),
                pltpu.VMEM((NC, 2 * S * H, DH), F32), pltpu.VMEM((NC, H, DH), F32),
                pltpu.VMEM((NC, 2 * S * H, DH), F32), pltpu.VMEM((NC, H, DH), F32),
                pltpu.VMEM((NC, S * H, DH), F32), pltpu.VMEM((NC, H, DH), F32),
                pltpu.VMEM((S * H, DH), F32),
                pltpu.VMEM((NC, S, D), F32), pltpu.VMEM((NC, HALF, D), F32),
                sem, sem((NC, 2)), sem((NC, 2)), sem((NC, 2)), sem((NC, 2)), sem((NC,)), sem((NC,)),
                sem((NC, 4)), sem((NC, 4)), sem((NC, 4)), sem((NC, 4)),
            ],
            compiler_params=pltpu.CompilerParams(vmem_limit_bytes=36 * MIB, collective_id=0, has_side_effects=True),
            name="combine",
        )(o, lse, w_out)
        out_hidden = (hidden.astype(F32) + y + b_out).astype(BF16)
        return out_hidden, k_new, v_new

    cache_spec = P("dp", "sq", None)
    row_spec = P("dp", None)
    in_specs = (row_spec, P("dp"), cache_spec, cache_spec, P(None), P(None), P(None, "tp"), P("tp"), P(None, None), P(None), P("tp", None), P(None))
    out_specs = (row_spec, cache_spec, cache_spec)
    return jax.shard_map(local_step, mesh=mesh, in_specs=in_specs, out_specs=out_specs, check_vma=False)
```

```python
import functools
import math

import jax
import jax.numpy as jnp
from jax import lax
from jax.experimental import pallas as pl
from jax.experimental.pallas import tpu as pltpu
from jax.sharding import PartitionSpec as P

MESH = pl.DeviceIdType.MESH
F32 = jnp.float32
BF16 = jnp.bfloat16
NEG = -1e30
B = 256
D = 4096
H = 16
DH = 128
T = 256
NC = 4
CS = B // NC
S = CS // 4
HALF = S // 2
QB = 512
NQ = H * DH // QB
QSCALE = DH ** -0.5 * math.log2(math.e)
GROUP = 8
MIB = 1024 * 1024


def attention_kernel(lens, hid_hbm, k_hbm, v_hbm, gain_ref, bias_ref, wq_hbm, bq_ref, wkv_hbm, bkv_ref,
                     o_ref, lse_ref, ko_hbm, vo_hbm,
                     hid, h, wq, wkv, q3, kv, kbuf, vbuf, s_a, s_b, p_a, p_b, wsem, ksem, vsem, osem):
    first = lax.axis_index("sq") * T
    load_h = pltpu.make_async_copy(hid_hbm, hid, wsem.at[NQ])
    load_h.start()
    load_wq = []
    for j in range(NQ):
        cols = pl.ds(j * QB, QB)
        load_wq.append(pltpu.make_async_copy(wq_hbm.at[:, cols], wq.at[:, cols], wsem.at[j]))
    load_wkv = pltpu.make_async_copy(wkv_hbm, wkv, wsem.at[NQ + 1])
    load_wkv.start()
    for c in load_wq:
        c.start()
    load_k, load_v = [], []
    for k in range(NC):
        rows = pl.ds(k * CS, CS)
        load_k.append(pltpu.make_async_copy(k_hbm.at[rows], kbuf.at[rows], ksem.at[k]))
        load_v.append(pltpu.make_async_copy(v_hbm.at[rows], vbuf.at[rows], vsem.at[k]))
        load_k[-1].start()
        load_v[-1].start()
    load_h.wait()

    def norm_rows(i, _):
        rows = pl.ds(pl.multiple_of(i * 16, 16), 16)
        x = hid[rows, :].astype(F32)
        mean = jnp.sum(x, axis=-1, keepdims=True) * (1.0 / D)
        cen = x - mean
        var = jnp.sum(cen * cen, axis=-1, keepdims=True) * (1.0 / D)
        y = cen * lax.rsqrt(var + 1e-5)
        h[rows, :] = (y * gain_ref[...] + bias_ref[...]).astype(BF16)
        return 0

    lax.fori_loop(0, B // 16, norm_rows, 0, unroll=2)
    load_wkv.wait()
    new_kv = (jnp.dot(h[...], wkv[...], preferred_element_type=F32) + bkv_ref[...]).astype(BF16).astype(F32)
    kv[0:B, :] = new_kv[:, :DH]
    kv[B:2 * B, :] = new_kv[:, DH:]
    for j in range(NQ):
        load_wq[j].wait()
        cols = pl.ds(j * QB, QB)
        q = jnp.dot(h[...], wq[:, cols], preferred_element_type=F32) + bq_ref[:, cols]
        q = q.astype(BF16).astype(F32)
        for n in range(QB // DH):
            q3[pl.ds(j * (QB // DH) + n, B, stride=H), :] = q[:, n * DH:(n + 1) * DH]

    sub = lax.broadcasted_iota(jnp.int32, (16, DH), 0)
    lane = lax.broadcasted_iota(jnp.int32, (H, DH), 1)
    pos = lax.broadcasted_iota(jnp.int32, (H, T), 1)
    zero = jnp.zeros((H, DH), BF16)

    def insert(b, _):
        row = lens[b] - first
        start = pl.multiple_of((jnp.clip(row, 0, T - 1) // 16) * 16, 16)
        hit = sub == row - start
        for buf, c in ((kbuf, 0), (vbuf, 1)):
            new = kv[pl.ds(c * B + b, 1), :]
            old = buf[b, pl.ds(start, 16), :].astype(F32)
            buf[b, pl.ds(start, 16), :] = jnp.where(hit, new, old).astype(BF16)
        return 0

    def score(i, s_out):
        for u in range(0, GROUP, 2):
            b = i * GROUP + u
            q0 = q3[pl.ds(pl.multiple_of(b * H, H), H), :].astype(BF16)
            q1 = q3[pl.ds(pl.multiple_of(b * H + H, H), H), :].astype(BF16)
            lhs = jnp.concatenate([jnp.concatenate([q0, zero], 1), jnp.concatenate([zero, q1], 1)], 0)
            keys = jnp.concatenate([kbuf[b], kbuf[b + 1]], 1)
            s_out[u * H:(u + 2) * H, :] = lax.dot_general(lhs, keys, (((1,), (1,)), ((), ())), preferred_element_type=F32)

    def soften(i, s_in, p_out, k):
        lses = lse_ref[pl.ds(k * H, H), :]
        for u in range(GROUP):
            b = i * GROUP + u
            se = jnp.where(pos <= lens[b] - first, s_in[u * H:(u + 1) * H, :] * QSCALE, NEG)
            m = jnp.max(se, axis=1, keepdims=True)
            p = jnp.exp2(se - m)
            l = jnp.sum(p, axis=1, keepdims=True)
            p_out[u * H:(u + 1) * H, :] = (p * (1.0 / l)).astype(BF16)
            lses = jnp.where(lane == b - k * CS, m + jnp.log2(l), lses)
        lse_ref[pl.ds(k * H, H), :] = lses

    def weigh(i, p_in):
        for u in range(0, GROUP, 2):
            b = i * GROUP + u
            vals = jnp.concatenate([vbuf[b], vbuf[b + 1]], 1)
            o = jnp.dot(p_in[u * H:(u + 2) * H, :], vals, preferred_element_type=F32)
            for e in range(2):
                o_ref[pl.ds(pl.multiple_of((b + e) * H, H), H), :] = o[e * H:(e + 1) * H, e * DH:(e + 1) * DH]

    def attend(k):
        lo, hi = k * CS // GROUP, (k + 1) * CS // GROUP
        score(lo, s_a)
        score(lo + 1, s_b)
        soften(lo, s_a, p_a, k)

        def body(t, _):
            i = lo + 2 + 2 * t
            score(i, s_a)
            soften(i - 1, s_b, p_b, k)
            weigh(i - 2, p_a)
            score(i + 1, s_b)
            soften(i, s_a, p_a, k)
            weigh(i - 1, p_b)
            return 0

        lax.fori_loop(0, (hi - lo - 2) // 2, body, 0)
        soften(hi - 1, s_b, p_b, k)
        weigh(hi - 2, p_a)
        weigh(hi - 1, p_b)

    stores = []
    for k in range(NC):
        load_k[k].wait()
        load_v[k].wait()
        lse_ref[pl.ds(k * H, H), :] = jnp.zeros((H, DH), F32)
        lax.fori_loop(k * CS, (k + 1) * CS, insert, 0, unroll=4)
        attend(k)
        rows = pl.ds(k * CS, CS)
        for e, (buf, out) in enumerate(((kbuf, ko_hbm), (vbuf, vo_hbm))):
            st = pltpu.make_async_copy(buf.at[rows], out.at[rows], osem.at[2 * k + e])
            st.start()
            stores.append(st)
    for st in stores:
        st.wait()


def column(tile, j):
    return tile[:, j:j + 1]


def merge(la, lb):
    top = jnp.maximum(la, lb)
    wa, wb = jnp.exp2(la - top), jnp.exp2(lb - top)
    tot = wa + wb
    return wa / tot, wb / tot, top + jnp.log2(tot)


def combine_kernel(o_ref, lse_ref, wo_hbm, y_ref,
                   wo, o_core, l_core, o_mix, l_mix, o_x, l_x, a3, part, p_y,
                   wsem, a0s, a0r, a1s, a1r, bs, br, cs, cr, ds, dr):
    sq, tp = lax.axis_index("sq"), lax.axis_index("tp")
    x, c = sq // 2, sq % 2
    mate = {"sq": x * 2 + 1 - c}
    over_x = {"sq": (1 - x) * 2 + c}
    over_y = {"tp": 1 - tp}
    load = pltpu.make_async_copy(wo_hbm, wo, wsem)
    load.start()
    bar = pltpu.get_barrier_semaphore()
    for dev in (mate, over_x, over_y):
        pl.semaphore_signal(bar, inc=1, device_id=dev, device_id_type=MESH)
    pl.semaphore_wait(bar, 3)

    def send(src, dst, ssem, rsem, dev):
        cp = pltpu.make_async_remote_copy(src, dst, ssem, rsem, device_id=dev, device_id_type=MESH)
        cp.start()
        return cp

    W = 2 * S * H
    sent = []
    hop0, hop1, hopb, hopc, hopd = [], [], [], [], []
    for k in range(NC):
        other = pl.multiple_of(k * CS * H + (1 - c) * W, W)
        hop0.append((send(o_ref.at[pl.ds(other, W)], o_core.at[k], a0s.at[k, 0], a0r.at[k, 0], mate),
                     send(lse_ref.at[pl.ds(k * H, H)], l_core.at[k], a0s.at[k, 1], a0r.at[k, 1], mate)))
    for k in range(NC):
        for cp in hop0[k]:
            cp.wait_recv()
        shift = lax.rem(DH - c * 2 * S, DH)
        fa, fb, lm = merge(pltpu.roll(lse_ref[pl.ds(k * H, H), :], shift, 1), pltpu.roll(l_core[k], shift, 1))
        l_mix[k] = lm
        mine = k * CS * H + c * W
        for j in range(2 * S):
            oa = o_ref[pl.ds(pl.multiple_of(mine + j * H, H), H), :]
            ob = o_core[k, j * H:(j + 1) * H, :]
            o_mix[k, j * H:(j + 1) * H, :] = column(fa, j) * oa + column(fb, j) * ob
        far = pl.multiple_of((1 - x) * S * H, S * H)
        hop1.append((send(o_mix.at[k, pl.ds(far, S * H)], o_x.at[k], a1s.at[k, 0], a1r.at[k, 0], over_x),
                     send(l_mix.at[k], l_x.at[k], a1s.at[k, 1], a1r.at[k, 1], over_x)))

    def project(k):
        for cp in hop1[k]:
            cp.wait_recv()
        shift = lax.rem(DH - x * S, DH)
        fa, fb, _ = merge(pltpu.roll(l_mix[k], shift, 1), pltpu.roll(l_x[k], shift, 1))
        near = x * S * H
        for j in range(S):
            oa = o_mix[k, pl.ds(pl.multiple_of(near + j * H, H), H), :]
            ob = o_x[k, j * H:(j + 1) * H, :]
            a3[j * H:(j + 1) * H, :] = column(fa, j) * oa + column(fb, j) * ob
        a = jnp.concatenate([a3[pl.ds(n, S, stride=H), :].astype(BF16) for n in range(H)], 1)
        if k == 0:
            load.wait()

        def cols(i, _):
            cc = pl.ds(pl.multiple_of(i * 1024, 1024), 1024)
            part[k, :, cc] = jnp.dot(a, wo[:, cc], preferred_element_type=F32)
            return 0

        lax.fori_loop(0, D // 1024, cols, 0)
        far = pl.multiple_of((1 - tp) * HALF, HALF)
        hopb.append(send(part.at[k, pl.ds(far, HALF)], p_y.at[k], bs.at[k], br.at[k], over_y))

    def rows_of(k, xx, yy):
        return pl.ds(pl.multiple_of(k * CS + (c * 2 + xx) * S + yy * HALF, HALF), HALF)

    def finish(k):
        hopb[k].wait_recv()
        rows = rows_of(k, x, tp)
        y_ref[rows, :] = part[k, pl.ds(pl.multiple_of(tp * HALF, HALF), HALF), :] + p_y[k]
        hopc.append((send(y_ref.at[rows], y_ref.at[rows], cs.at[k, 0], cr.at[k, 0], over_x),
                     send(y_ref.at[rows], y_ref.at[rows], cs.at[k, 1], cr.at[k, 1], over_y)))
        hopd.append([send(y_ref.at[rows], y_ref.at[rows], ds.at[k, 0], dr.at[k, 0], mate)])

    def relay(k):
        hopc[k][0].wait_recv()
        rows, lo, hi = rows_of(k, 1 - x, tp), pl.ds(0, D // 2), pl.ds(D // 2, D // 2)
        d1 = send(y_ref.at[rows, lo], y_ref.at[rows, lo], cs.at[k, 2], cr.at[k, 2], over_y)
        hopd[k].append(send(y_ref.at[rows], y_ref.at[rows], ds.at[k, 1], dr.at[k, 1], mate))
        hopc[k][1].wait_recv()
        rows = rows_of(k, x, 1 - tp)
        d2 = send(y_ref.at[rows, hi], y_ref.at[rows, hi], cs.at[k, 3], cr.at[k, 3], over_x)
        hopd[k].append(send(y_ref.at[rows], y_ref.at[rows], ds.at[k, 2], dr.at[k, 2], mate))
        hopc[k] = hopc[k] + (d1, d2)

    def last(k):
        hopc[k][2].wait_recv()
        hopc[k][3].wait_recv()
        rows = rows_of(k, 1 - x, 1 - tp)
        hopd[k].append(send(y_ref.at[rows], y_ref.at[rows], ds.at[k, 3], dr.at[k, 3], mate))

    for step, k in ((project, 0), (project, 1), (finish, 0), (project, 2), (finish, 1), (project, 3), (relay, 0), (finish, 2),
                    (relay, 1), (last, 0), (finish, 3), (relay, 2), (last, 1), (relay, 3), (last, 2), (last, 3)):
        step(k)
    for k in range(NC):
        for cp in hopd[k]:
            cp.wait_recv()
    for k in range(NC):
        for cp in hop0[k] + hop1[k] + (hopb[k],) + hopc[k] + tuple(hopd[k]):
            cp.wait_send()


def solution(mesh):
    def local_step(hidden, cache_lens, k_cache, v_cache, ln_gain, ln_bias, w_query, b_query, w_kv, b_kv, w_out, b_out):
        hbm = pl.BlockSpec(memory_space=pltpu.HBM)
        vm = pl.BlockSpec(memory_space=pltpu.VMEM)
        cache = jax.ShapeDtypeStruct((B, T, DH), BF16)
        o, lse, k_new, v_new = pl.pallas_call(
            attention_kernel,
            out_shape=(pltpu.VMEM((B * H, DH), F32), pltpu.VMEM((NC * H, DH), F32), cache, cache),
            in_specs=[pl.BlockSpec(memory_space=pltpu.SMEM), hbm, hbm, hbm, vm, vm, hbm, vm, hbm, vm],
            out_specs=(vm, vm, hbm, hbm),
            scratch_shapes=[
                pltpu.VMEM((B, D), BF16), pltpu.VMEM((B, D), BF16), pltpu.VMEM((D, H * DH), BF16), pltpu.VMEM((D, 2 * DH), BF16),
                pltpu.VMEM((B * H, DH), F32), pltpu.VMEM((2 * B, DH), F32),
                pltpu.VMEM((B, T, DH), BF16), pltpu.VMEM((B, T, DH), BF16),
                pltpu.VMEM((GROUP * H, T), F32), pltpu.VMEM((GROUP * H, T), F32),
                pltpu.VMEM((GROUP * H, T), BF16), pltpu.VMEM((GROUP * H, T), BF16),
                pltpu.SemaphoreType.DMA((NQ + 2,)), pltpu.SemaphoreType.DMA((NC,)), pltpu.SemaphoreType.DMA((NC,)),
                pltpu.SemaphoreType.DMA((2 * NC,)),
            ],
            compiler_params=pltpu.CompilerParams(vmem_limit_bytes=60 * MIB),
            name="attention",
        )(cache_lens, hidden, k_cache, v_cache, ln_gain[None], ln_bias[None], w_query, b_query[None], w_kv, b_kv[None])
        sem = pltpu.SemaphoreType.DMA
        y = pl.pallas_call(
            combine_kernel,
            out_shape=pltpu.VMEM((B, D), F32),
            in_specs=[vm, vm, hbm],
            out_specs=vm,
            scratch_shapes=[
                pltpu.VMEM((H * DH, D), BF16),
                pltpu.VMEM((NC, 2 * S * H, DH), F32), pltpu.VMEM((NC, H, DH), F32),
                pltpu.VMEM((NC, 2 * S * H, DH), F32), pltpu.VMEM((NC, H, DH), F32),
                pltpu.VMEM((NC, S * H, DH), F32), pltpu.VMEM((NC, H, DH), F32),
                pltpu.VMEM((S * H, DH), F32),
                pltpu.VMEM((NC, S, D), F32), pltpu.VMEM((NC, HALF, D), F32),
                sem, sem((NC, 2)), sem((NC, 2)), sem((NC, 2)), sem((NC, 2)), sem((NC,)), sem((NC,)),
                sem((NC, 4)), sem((NC, 4)), sem((NC, 4)), sem((NC, 4)),
            ],
            compiler_params=pltpu.CompilerParams(vmem_limit_bytes=36 * MIB, collective_id=0, has_side_effects=True),
            name="combine",
        )(o, lse, w_out)
        out_hidden = (hidden.astype(F32) + y + b_out).astype(BF16)
        return out_hidden, k_new, v_new

    cache_spec = P("dp", "sq", None)
    row_spec = P("dp", None)
    in_specs = (row_spec, P("dp"), cache_spec, cache_spec, P(None), P(None), P(None, "tp"), P("tp"), P(None, None), P(None), P("tp", None), P(None))
    out_specs = (row_spec, cache_spec, cache_spec)
    return jax.shard_map(local_step, mesh=mesh, in_specs=in_specs, out_specs=out_specs, check_vma=False)
```

```python
import functools
import math

import jax
import jax.numpy as jnp
from jax import lax
from jax.experimental import pallas as pl
from jax.experimental.pallas import tpu as pltpu
from jax.sharding import PartitionSpec as P

MESH = pl.DeviceIdType.MESH
F32 = jnp.float32
BF16 = jnp.bfloat16
NEG = -1e30
B = 256
D = 4096
H = 16
DH = 128
T = 256
NC = 4
CS = B // NC
S = CS // 4
HALF = S // 2
QB = 512
NQ = H * DH // QB
QSCALE = DH ** -0.5 * math.log2(math.e)
GROUP = 8
MIB = 1024 * 1024
MLIM = 27
VIA_Y = 768
SCHEDULE = [(s[0], int(s[1])) for s in "a1 s1 a2 m1 s2 p0 m2 a3 s3 p1 m3 f0 p2 f1 r0 p3 f2 r1 l0 f3 r2 l1 r3 l2 l3".split()]


def attention_stages(lens, first, q3, kbuf, vbuf, base, vbase, kv, o_ref, lse_ref, bufs):
    lane = lax.broadcasted_iota(jnp.int32, (H, DH), 1)
    pos = lax.broadcasted_iota(jnp.int32, (H, T), 1)
    zero = jnp.zeros((H, DH), BF16)
    s_a, s_b, p_a, p_b, r_a, r_b, n_a, n_b = bufs

    def score(i, s_out):
        for u in range(0, GROUP, 2):
            b = i * GROUP + u
            q0 = q3[pl.ds(pl.multiple_of(b * H, H), H), :].astype(BF16)
            q1 = q3[pl.ds(pl.multiple_of(b * H + H, H), H), :].astype(BF16)
            lhs = jnp.concatenate([jnp.concatenate([q0, zero], 1), jnp.concatenate([zero, q1], 1)], 0)
            keys = jnp.concatenate([kbuf[b - base], kbuf[b + 1 - base]], 1)
            s_out[u * H:(u + 2) * H, :] = lax.dot_general(lhs, keys, (((1,), (1,)), ((), ())), preferred_element_type=F32)

    def soften(i, s_in, p_out, r_out, n_out, k):
        lses = lse_ref[pl.ds(k * H, H), :]
        for u in range(GROUP):
            b = i * GROUP + u
            row = lens[b] - first
            here = jnp.logical_and(row >= 0, row < T)
            k_new = kv[pl.ds(b, 1), :]
            v_new = kv[pl.ds(B + b, 1), :]
            q_row = q3[pl.ds(pl.multiple_of(b * H, H), H), :]
            s_new = jnp.where(here, jnp.sum(q_row * k_new, axis=1, keepdims=True) * QSCALE, NEG)
            se = jnp.where(pos < row, s_in[u * H:(u + 1) * H, :] * QSCALE, NEG)
            m = jnp.maximum(jnp.max(se, axis=1, keepdims=True), s_new)
            p = jnp.exp2(se - m)
            p_new = jnp.exp2(s_new - m)
            l = jnp.sum(p, axis=1, keepdims=True) + p_new
            r = 1.0 / l
            p_out[u * H:(u + 1) * H, :] = p.astype(BF16)
            r_out[u * H:(u + 1) * H, :] = jnp.broadcast_to(r, (H, DH))
            n_out[u * H:(u + 1) * H, :] = (p_new * r) * v_new
            lses = jnp.where(lane == b - k * CS, m + jnp.log2(l), lses)
        lse_ref[pl.ds(k * H, H), :] = lses

    def weigh(i, p_in, r_in, n_in):
        for u in range(0, GROUP, 2):
            b = i * GROUP + u
            vals = jnp.concatenate([vbuf[b - vbase], vbuf[b + 1 - vbase]], 1)
            o = jnp.dot(p_in[u * H:(u + 2) * H, :], vals, preferred_element_type=F32)
            for e in range(2):
                part = slice((u + e) * H, (u + e + 1) * H)
                o_ref[pl.ds(pl.multiple_of((b + e) * H, H), H), :] = (
                    o[e * H:(e + 1) * H, e * DH:(e + 1) * DH] * r_in[part, :] + n_in[part, :])

    def attend(k):
        lse_ref[pl.ds(k * H, H), :] = jnp.zeros((H, DH), F32)
        lo, hi = k * CS // GROUP, (k + 1) * CS // GROUP
        score(lo, s_a)
        score(lo + 1, s_b)
        soften(lo, s_a, p_a, r_a, n_a, k)

        def body(t, _):
            i = lo + 2 + 2 * t
            score(i, s_a)
            soften(i - 1, s_b, p_b, r_b, n_b, k)
            weigh(i - 2, p_a, r_a, n_a)
            score(i + 1, s_b)
            soften(i, s_a, p_a, r_a, n_a, k)
            weigh(i - 1, p_b, r_b, n_b)
            return 0

        lax.fori_loop(0, (hi - lo - 2) // 2, body, 0)
        soften(hi - 1, s_b, p_b, r_b, n_b, k)
        weigh(hi - 2, p_a, r_a, n_a)
        weigh(hi - 1, p_b, r_b, n_b)

    return attend


STAGE_BUFS = [pltpu.VMEM((GROUP * H, T), F32)] * 2 + [pltpu.VMEM((GROUP * H, T), BF16)] * 2 + [pltpu.VMEM((GROUP * H, DH), F32)] * 4


def insert_rows(lens, first, kv, pairs, lo, hi, base):
    sub = lax.broadcasted_iota(jnp.int32, (16, DH), 0)

    def insert(b, _):
        row = lens[b] - first
        start = pl.multiple_of((jnp.clip(row, 0, T - 1) // 16) * 16, 16)
        hit = sub == row - start
        for c, buf in enumerate(pairs):
            new = kv[pl.ds(c * B + b, 1), :]
            old = buf[b - base, pl.ds(start, 16), :].astype(F32)
            buf[b - base, pl.ds(start, 16), :] = jnp.where(hit, new, old).astype(BF16)
        return 0

    lax.fori_loop(lo, hi, insert, 0, unroll=4)


def first_kernel(lens, hid_hbm, k_hbm, v_hbm, gain_ref, bias_ref, wq_hbm, bq_ref, wkv_hbm, bkv_ref,
                 q3, kv, o_ref, lse_ref, ko_hbm, vo_hbm,
                 hid, h, wq, wkv, kbuf, vbuf, b0, b1, b2, b3, b4, b5, b6, b7, wsem, csem):
    first = lax.axis_index("sq") * T
    load_h = pltpu.make_async_copy(hid_hbm, hid, wsem.at[NQ])
    load_h.start()
    load_wkv = pltpu.make_async_copy(wkv_hbm, wkv, wsem.at[NQ + 1])
    load_wkv.start()
    load_wq = []
    for j in range(NQ):
        cols = pl.ds(j * QB, QB)
        load_wq.append(pltpu.make_async_copy(wq_hbm.at[:, cols], wq.at[:, cols], wsem.at[j]))
        load_wq[-1].start()
    loads = [pltpu.make_async_copy(src.at[pl.ds(0, CS)], dst, csem.at[e]) for e, (src, dst) in enumerate(((k_hbm, kbuf), (v_hbm, vbuf)))]
    for c in loads:
        c.start()
    load_h.wait()

    def norm_rows(i, _):
        rows = pl.ds(pl.multiple_of(i * 16, 16), 16)
        x = hid[rows, :].astype(F32)
        mean = jnp.sum(x, axis=-1, keepdims=True) * (1.0 / D)
        cen = x - mean
        var = jnp.sum(cen * cen, axis=-1, keepdims=True) * (1.0 / D)
        y = cen * lax.rsqrt(var + 1e-5)
        h[rows, :] = (y * gain_ref[...] + bias_ref[...]).astype(BF16)
        return 0

    lax.fori_loop(0, B // 16, norm_rows, 0, unroll=2)
    load_wkv.wait()
    new_kv = (jnp.dot(h[...], wkv[...], preferred_element_type=F32) + bkv_ref[...]).astype(BF16).astype(F32)
    kv[0:B, :] = new_kv[:, :DH]
    kv[B:2 * B, :] = new_kv[:, DH:]
    for j in range(NQ):
        load_wq[j].wait()
        cols = pl.ds(j * QB, QB)
        q = jnp.dot(h[...], wq[:, cols], preferred_element_type=F32) + bq_ref[:, cols]
        q = q.astype(BF16).astype(F32)
        for n in range(QB // DH):
            q3[pl.ds(j * (QB // DH) + n, B, stride=H), :] = q[:, n * DH:(n + 1) * DH]
    for c in loads:
        c.wait()
    insert_rows(lens, first, kv, (kbuf, vbuf), 0, CS, 0)
    stores = [pltpu.make_async_copy(src, dst.at[pl.ds(0, CS)], csem.at[2 + e]) for e, (src, dst) in enumerate(((kbuf, ko_hbm), (vbuf, vo_hbm)))]
    for c in stores:
        c.start()
    attention_stages(lens, first, q3, kbuf, vbuf, 0, 0, kv, o_ref, lse_ref, (b0, b1, b2, b3, b4, b5, b6, b7))(0)
    for c in stores:
        c.wait()


def column(tile, j):
    return tile[:, j:j + 1]


def merge(la, lb):
    top = jnp.maximum(la, lb)
    wa, wb = jnp.exp2(la - top), jnp.exp2(lb - top)
    tot = wa + wb
    return wa / tot, wb / tot, top + jnp.log2(tot)


def exchange_kernel(lens, q3, kv, o_first, lse_first, k_hbm, v_hbm, wo_hbm, y_ref, held,
                    wo, o_ref, lse_ref, b0, b1, b2, b3, b4, b5, b6, b7, o_core, l_core, o_mix, l_mix, o_x, l_x, a3, part, p_y,
                    wsem, csem, a0s, a0r, a1s, a1r, bs, br, cs, cr, ds, dr):
    sq, tp = lax.axis_index("sq"), lax.axis_index("tp")
    x, c = sq // 2, sq % 2
    mate = {"sq": x * 2 + 1 - c}
    over_x = {"sq": (1 - x) * 2 + c}
    over_y = {"tp": 1 - tp}
    loads = {}

    def fetch(k):
        rows = pl.ds(k * CS, CS)
        loads[k] = [pltpu.make_async_copy(src.at[rows], held.at[pl.ds((k - 1) * CS + e * (B - CS), CS)], csem.at[2 * k + e - 2])
                    for e, src in enumerate((k_hbm, v_hbm))]
        for cp in loads[k]:
            cp.start()

    fetch(1)
    fetch(2)
    load = pltpu.make_async_copy(wo_hbm, wo, wsem)
    load.start()
    fetch(3)
    bar = pltpu.get_barrier_semaphore()
    for dev in (mate, over_x, over_y):
        pl.semaphore_signal(bar, inc=1, device_id=dev, device_id_type=MESH)
    pl.semaphore_wait(bar, 3)

    def send(src, dst, ssem, rsem, dev):
        cp = pltpu.make_async_remote_copy(src, dst, ssem, rsem, device_id=dev, device_id_type=MESH)
        cp.start()
        return cp

    W = 2 * S * H
    hop0, hop1, hopb, hopc, hopd = {}, {}, {}, {}, {}
    stages = attention_stages(lens, sq * T, q3, held, held, CS, CS - (B - CS), kv, o_ref, lse_ref, (b0, b1, b2, b3, b4, b5, b6, b7))

    def attend(k):
        for cp in loads[k]:
            cp.wait()
        stages(k)

    def source(k):
        return (o_first, lse_first) if k == 0 else (o_ref, lse_ref)

    def share(k):
        o_k, l_k = source(k)
        other = pl.multiple_of(k * CS * H + (1 - c) * W, W)
        hop0[k] = (send(o_k.at[pl.ds(other, W)], o_core.at[k], a0s.at[k, 0], a0r.at[k, 0], mate),
                   send(l_k.at[pl.ds(k * H, H)], l_core.at[k], a0s.at[k, 1], a0r.at[k, 1], mate))

    def mix(k):
        o_k, l_k = source(k)
        for cp in hop0[k]:
            cp.wait_recv()
        shift = lax.rem(DH - c * 2 * S, DH)
        fa, fb, lm = merge(pltpu.roll(l_k[pl.ds(k * H, H), :], shift, 1), pltpu.roll(l_core[k], shift, 1))
        l_mix[k] = lm
        mine = k * CS * H + c * W
        for j in range(2 * S):
            oa = o_k[pl.ds(pl.multiple_of(mine + j * H, H), H), :]
            ob = o_core[k, j * H:(j + 1) * H, :]
            o_mix[k, j * H:(j + 1) * H, :] = column(fa, j) * oa + column(fb, j) * ob
        far = pl.multiple_of((1 - x) * S * H, S * H)
        hop1[k] = (send(o_mix.at[k, pl.ds(far, S * H)], o_x.at[k], a1s.at[k, 0], a1r.at[k, 0], over_x),
                   send(l_mix.at[k], l_x.at[k], a1s.at[k, 1], a1r.at[k, 1], over_x))

    def project(k):
        for cp in hop1[k]:
            cp.wait_recv()
        shift = lax.rem(DH - x * S, DH)
        fa, fb, _ = merge(pltpu.roll(l_mix[k], shift, 1), pltpu.roll(l_x[k], shift, 1))
        near = x * S * H
        for j in range(S):
            oa = o_mix[k, pl.ds(pl.multiple_of(near + j * H, H), H), :]
            ob = o_x[k, j * H:(j + 1) * H, :]
            a3[j * H:(j + 1) * H, :] = column(fa, j) * oa + column(fb, j) * ob
        a = jnp.concatenate([a3[pl.ds(n, S, stride=H), :].astype(BF16) for n in range(H)], 1)
        if k == 0:
            load.wait()

        def cols(i, _):
            cc = pl.ds(pl.multiple_of(i * 1024, 1024), 1024)
            part[k, :, cc] = jnp.dot(a, wo[:, cc], preferred_element_type=F32)
            return 0

        lax.fori_loop(0, D // 1024, cols, 0)
        far = pl.multiple_of((1 - tp) * HALF, HALF)
        hopb[k] = send(part.at[k, pl.ds(far, HALF)], p_y.at[k], bs.at[k], br.at[k], over_y)

    def rows_of(k, xx, yy):
        return pl.ds(pl.multiple_of(k * CS + (c * 2 + xx) * S + yy * HALF, HALF), HALF)

    def finish(k):
        hopb[k].wait_recv()
        rows = rows_of(k, x, tp)
        y_ref[rows, :] = part[k, pl.ds(pl.multiple_of(tp * HALF, HALF), HALF), :] + p_y[k]
        hopc[k] = [send(y_ref.at[rows], y_ref.at[rows], cs.at[k, 0], cr.at[k, 0], over_x),
                   send(y_ref.at[rows], y_ref.at[rows], cs.at[k, 1], cr.at[k, 1], over_y)]
        hopd[k] = [send(y_ref.at[rows], y_ref.at[rows], ds.at[k, 0], dr.at[k, 0], mate)]

    lo, hi = pl.ds(0, VIA_Y), pl.ds(VIA_Y, D - VIA_Y)

    def relay(k):
        hopc[k][1].wait_recv()
        rows = rows_of(k, x, 1 - tp)
        d2 = send(y_ref.at[rows, hi], y_ref.at[rows, hi], cs.at[k, 3], cr.at[k, 3], over_x)
        hopd[k].append(send(y_ref.at[rows], y_ref.at[rows], ds.at[k, 2], dr.at[k, 2], mate))
        hopc[k][0].wait_recv()
        rows = rows_of(k, 1 - x, tp)
        d1 = send(y_ref.at[rows, lo], y_ref.at[rows, lo], cs.at[k, 2], cr.at[k, 2], over_y)
        hopd[k].append(send(y_ref.at[rows], y_ref.at[rows], ds.at[k, 1], dr.at[k, 1], mate))
        hopc[k] += [d1, d2]

    def last(k):
        hopc[k][2].wait_recv()
        hopc[k][3].wait_recv()
        rows = rows_of(k, 1 - x, 1 - tp)
        hopd[k].append(send(y_ref.at[rows], y_ref.at[rows], ds.at[k, 3], dr.at[k, 3], mate))

    share(0)
    mix(0)
    for step, k in SCHEDULE:
        {"a": attend, "s": share, "m": mix, "p": project, "f": finish, "r": relay, "l": last}[step](k)
    for k in range(NC):
        for cp in hopd[k]:
            cp.wait_recv()
    for k in range(NC):
        for cp in [*hop0[k], *hop1[k], hopb[k], *hopc[k], *hopd[k]]:
            cp.wait_send()


def last_kernel(lens, kv, y_in, hid, bo_ref, held, k_part, v_part, ko_hbm, vo_hbm, out_hbm, ktile, vtile, out, sem, tsem):
    first = lax.axis_index("sq") * T
    sub = lax.broadcasted_iota(jnp.int32, (16, DH), 0)
    sides = ((0, ktile, ko_hbm), (B - CS, vtile, vo_hbm))
    copies = []
    for k in range(1, NC):
        for e, (src, _, dst) in enumerate(sides):
            copies.append(pltpu.make_async_copy(held.at[pl.ds(src + (k - 1) * CS, CS)], dst.at[pl.ds(k * CS, CS)], sem.at[2 * k + e - 2]))
            copies[-1].start()

    def rows(i, _):
        r = pl.ds(pl.multiple_of(i * 16, 16), 16)
        out[r, :] = (hid[r, :].astype(F32) + y_in[r, :] + bo_ref[...]).astype(BF16)
        return 0

    lax.fori_loop(0, B // 16, rows, 0, unroll=2)
    store_out = pltpu.make_async_copy(out, out_hbm, sem.at[2 * NC - 2])
    store_out.start()

    def spot(b):
        row = lens[b] - first
        start = pl.multiple_of((jnp.clip(row, 0, T - 1) // 16) * 16, 16)
        return row, start, jnp.logical_and(row >= 0, row < T)

    def build(b, _):
        row, start, _ = spot(b)
        hit = sub == row - start
        for c, (src, tile, _) in enumerate(sides):
            new = kv[pl.ds(c * B + b, 1), :]
            old = held[b - CS + src, pl.ds(start, 16), :].astype(F32)
            tile[b - CS] = jnp.where(hit, new, old).astype(BF16)
        return 0

    lax.fori_loop(CS, B, build, 0, unroll=4)

    def tile_copy(b, start, side):
        return pltpu.make_async_copy(side[1].at[b - CS], side[2].at[b, pl.ds(start, 16), :], tsem)

    def put(b, _):
        _, start, own = spot(b)

        @pl.when(own)
        def _():
            for side in sides:
                tile_copy(b, start, side).start()
        return 0

    def drain(b, _):
        _, start, own = spot(b)

        @pl.when(own)
        def _():
            for side in sides:
                tile_copy(b, start, side).wait()
        return 0

    for k in range(1, NC):
        copies[2 * k - 2].wait()
        copies[2 * k - 1].wait()
        lax.fori_loop(k * CS, (k + 1) * CS, put, 0)
    store_out.wait()
    lax.fori_loop(CS, B, drain, 0)


def solution(mesh):
    def local_step(hidden, cache_lens, k_cache, v_cache, ln_gain, ln_bias, w_query, b_query, w_kv, b_kv, w_out, b_out):
        hbm = pl.BlockSpec(memory_space=pltpu.HBM)
        vm = pl.BlockSpec(memory_space=pltpu.VMEM)
        smem = pl.BlockSpec(memory_space=pltpu.SMEM)
        sem = pltpu.SemaphoreType.DMA

        def pin(*arrays):
            return [pltpu.with_memory_space_constraint(a, pltpu.VMEM) for a in arrays]

        def far(*arrays):
            return [pltpu.with_memory_space_constraint(a, pltpu.HBM) for a in arrays]

        cache = jax.ShapeDtypeStruct((B, T, DH), BF16)
        q3, kv, o0, lse0, k_part, v_part = pl.pallas_call(
            first_kernel,
            out_shape=(pltpu.VMEM((B * H, DH), F32), pltpu.VMEM((2 * B, DH), F32), pltpu.VMEM((CS * H, DH), F32), pltpu.VMEM((H, DH), F32), cache, cache),
            in_specs=[smem, hbm, hbm, hbm, vm, vm, hbm, vm, hbm, vm],
            out_specs=(vm, vm, vm, vm, hbm, hbm),
            scratch_shapes=[
                pltpu.VMEM((B, D), BF16), pltpu.VMEM((B, D), BF16), pltpu.VMEM((D, H * DH), BF16), pltpu.VMEM((D, 2 * DH), BF16),
                pltpu.VMEM((CS, T, DH), BF16), pltpu.VMEM((CS, T, DH), BF16), *STAGE_BUFS, sem((NQ + 2,)), sem((4,)),
            ],
            compiler_params=pltpu.CompilerParams(vmem_limit_bytes=33 * MIB),
            name="first",
        )(*far(cache_lens, hidden, k_cache, v_cache, ln_gain[None], ln_bias[None], w_query, b_query[None], w_kv, b_kv[None]))
        held = pltpu.VMEM((2 * (B - CS), T, DH), BF16)
        y, kv_held = pl.pallas_call(
            exchange_kernel,
            out_shape=(pltpu.VMEM((B, D), F32), held),
            in_specs=[smem, vm, vm, vm, vm, hbm, hbm, hbm],
            out_specs=(vm, vm),
            scratch_shapes=[
                pltpu.VMEM((H * DH, D), BF16), pltpu.VMEM((B * H, DH), F32), pltpu.VMEM((NC * H, DH), F32), *STAGE_BUFS,
                pltpu.VMEM((NC, 2 * S * H, DH), F32), pltpu.VMEM((NC, H, DH), F32),
                pltpu.VMEM((NC, 2 * S * H, DH), F32), pltpu.VMEM((NC, H, DH), F32),
                pltpu.VMEM((NC, S * H, DH), F32), pltpu.VMEM((NC, H, DH), F32),
                pltpu.VMEM((S * H, DH), F32),
                pltpu.VMEM((NC, S, D), F32), pltpu.VMEM((NC, HALF, D), F32),
                sem, sem((2 * NC - 2,)), sem((NC, 2)), sem((NC, 2)), sem((NC, 2)), sem((NC, 2)), sem((NC,)), sem((NC,)),
                sem((NC, 4)), sem((NC, 4)), sem((NC, 4)), sem((NC, 4)),
            ],
            compiler_params=pltpu.CompilerParams(vmem_limit_bytes=MLIM * MIB, collective_id=0, has_side_effects=True),
            name="exchange",
        )(*far(cache_lens), *pin(q3, kv, o0, lse0), *far(k_cache, v_cache, w_out))
        k_new, v_new, out_hidden = pl.pallas_call(
            last_kernel,
            out_shape=(cache, cache, jax.ShapeDtypeStruct((B, D), BF16)),
            in_specs=[smem, vm, vm, vm, vm, vm, hbm, hbm],
            out_specs=(hbm, hbm, hbm),
            input_output_aliases={6: 0, 7: 1},
            scratch_shapes=[pltpu.VMEM((B - CS, 16, DH), BF16), pltpu.VMEM((B - CS, 16, DH), BF16), pltpu.VMEM((B, D), BF16), sem((2 * NC - 1,)), sem],
            compiler_params=pltpu.CompilerParams(vmem_limit_bytes=6 * MIB),
            name="last",
        )(*far(cache_lens), *pin(kv, y), hidden, b_out[None], *pin(kv_held), k_part, v_part)
        return out_hidden, k_new, v_new

    cache_spec = P("dp", "sq", None)
    row_spec = P("dp", None)
    in_specs = (row_spec, P("dp"), cache_spec, cache_spec, P(None), P(None), P(None, "tp"), P("tp"), P(None, None), P(None), P("tp", None), P(None))
    out_specs = (row_spec, cache_spec, cache_spec)
    return jax.shard_map(local_step, mesh=mesh, in_specs=in_specs, out_specs=out_specs, check_vma=False)
```

```python
import functools
import math

import jax
import jax.numpy as jnp
from jax import lax
from jax.experimental import pallas as pl
from jax.experimental.pallas import tpu as pltpu
from jax.sharding import PartitionSpec as P

MESH = pl.DeviceIdType.MESH
F32 = jnp.float32
BF16 = jnp.bfloat16
NEG = -1e30
B = 256
D = 4096
H = 16
DH = 128
T = 256
AB = 64
NC = 8
CS = B // NC
S = CS // 4
R = 2 * S
DC = D // 2
DY = DC // 2
QB = 512
NQ = H * DH // QB
QSCALE = DH ** -0.5 * math.log2(math.e)
GROUP = 8
MIB = 1024 * 1024
VIA_Y = 128
SCHEDULE = [(s[0], int(s[1])) for s in "s0 s1 m0 a2 m1 s2 s3 a4 s4 s5 m2 m3 q0 m4 q1 m5 p0 p1 q2 a6 f0 q3 s6 s7 q4 f1 p2 m6 m7 p3 r0 p4 f2 q5 q6 q7 f3 r1 p5 f4 r2 p6 l0 l1 r3 p7 f5 r4 f6 f7 l2 r5 l3 l4 r6 r7 l5 l6 l7".split()]
def attention_stages(lens, first, q3, kbuf, vbuf, base, vbase, kv, o_ref, lse_ref, bufs):
    lane = lax.broadcasted_iota(jnp.int32, (H, DH), 1)
    pos = lax.broadcasted_iota(jnp.int32, (H, T), 1)
    zero = jnp.zeros((H, DH), BF16)
    s_a, s_b, p_a, p_b, r_a, r_b, n_a, n_b = bufs

    def score(i, s_out):
        for u in range(0, GROUP, 2):
            b = i * GROUP + u
            q0 = q3[pl.ds(pl.multiple_of(b * H, H), H), :].astype(BF16)
            q1 = q3[pl.ds(pl.multiple_of(b * H + H, H), H), :].astype(BF16)
            lhs = jnp.concatenate([jnp.concatenate([q0, zero], 1), jnp.concatenate([zero, q1], 1)], 0)
            keys = jnp.concatenate([kbuf[b - base], kbuf[b + 1 - base]], 1)
            s_out[u * H:(u + 2) * H, :] = lax.dot_general(lhs, keys, (((1,), (1,)), ((), ())), preferred_element_type=F32)

    def soften(i, s_in, p_out, r_out, n_out):
        chunk = lax.div(i * GROUP, CS)
        tile = pl.ds(pl.multiple_of(chunk * H, H), H)
        at = i * GROUP - chunk * CS
        lses = lse_ref[tile, :]
        for u in range(GROUP):
            b = i * GROUP + u
            row = lens[b] - first
            here = jnp.logical_and(row >= 0, row < T)
            k_new = kv[pl.ds(b, 1), :]
            v_new = kv[pl.ds(B + b, 1), :]
            q_row = q3[pl.ds(pl.multiple_of(b * H, H), H), :]
            s_new = jnp.where(here, jnp.sum(q_row * k_new, axis=1, keepdims=True) * QSCALE, NEG)
            se = jnp.where(pos < row, s_in[u * H:(u + 1) * H, :] * QSCALE, NEG)
            m = jnp.maximum(jnp.max(se, axis=1, keepdims=True), s_new)
            p = jnp.exp2(se - m)
            p_new = jnp.exp2(s_new - m)
            l = jnp.sum(p, axis=1, keepdims=True) + p_new
            r = 1.0 / l
            p_out[u * H:(u + 1) * H, :] = p.astype(BF16)
            r_out[u * H:(u + 1) * H, :] = jnp.broadcast_to(r, (H, DH))
            n_out[u * H:(u + 1) * H, :] = (p_new * r) * v_new
            lses = jnp.where(lane == at + u, m + jnp.log2(l), lses)
        lse_ref[tile, :] = lses

    def weigh(i, p_in, r_in, n_in):
        for u in range(0, GROUP, 2):
            b = i * GROUP + u
            vals = jnp.concatenate([vbuf[b - vbase], vbuf[b + 1 - vbase]], 1)
            o = jnp.dot(p_in[u * H:(u + 2) * H, :], vals, preferred_element_type=F32)
            for e in range(2):
                part = slice((u + e) * H, (u + e + 1) * H)
                o_ref[pl.ds(pl.multiple_of((b + e) * H, H), H), :] = (
                    o[e * H:(e + 1) * H, e * DH:(e + 1) * DH] * r_in[part, :] + n_in[part, :])

    def attend(k):
        tiles = slice(k * AB // CS * H, (k + 1) * AB // CS * H)
        lse_ref[tiles, :] = jnp.zeros((AB // CS * H, DH), F32)
        lo, hi = k * AB // GROUP, (k + 1) * AB // GROUP
        score(lo, s_a)
        score(lo + 1, s_b)
        soften(lo, s_a, p_a, r_a, n_a)

        def body(t, _):
            i = lo + 2 + 2 * t
            score(i, s_a)
            soften(i - 1, s_b, p_b, r_b, n_b)
            weigh(i - 2, p_a, r_a, n_a)
            score(i + 1, s_b)
            soften(i, s_a, p_a, r_a, n_a)
            weigh(i - 1, p_b, r_b, n_b)
            return 0

        lax.fori_loop(0, (hi - lo - 2) // 2, body, 0)
        soften(hi - 1, s_b, p_b, r_b, n_b)
        weigh(hi - 2, p_a, r_a, n_a)
        weigh(hi - 1, p_b, r_b, n_b)

    return attend


STAGE_BUFS = [pltpu.VMEM((GROUP * H, T), F32)] * 2 + [pltpu.VMEM((GROUP * H, T), BF16)] * 2 + [pltpu.VMEM((GROUP * H, DH), F32)] * 4


def insert_rows(lens, first, kv, pairs, lo, hi, base):
    sub = lax.broadcasted_iota(jnp.int32, (16, DH), 0)

    def insert(b, _):
        row = lens[b] - first
        start = pl.multiple_of((jnp.clip(row, 0, T - 1) // 16) * 16, 16)
        hit = sub == row - start
        for c, buf in enumerate(pairs):
            new = kv[pl.ds(c * B + b, 1), :]
            old = buf[b - base, pl.ds(start, 16), :].astype(F32)
            buf[b - base, pl.ds(start, 16), :] = jnp.where(hit, new, old).astype(BF16)
        return 0

    lax.fori_loop(lo, hi, insert, 0, unroll=4)


def first_kernel(lens, hid_hbm, k_hbm, v_hbm, gain_ref, bias_ref, wq_hbm, bq_ref, wkv_hbm, bkv_ref,
                 q3, kv, o_ref, lse_ref, ko_hbm, vo_hbm,
                 hid, h, wq, wkv, kbuf, vbuf, b0, b1, b2, b3, b4, b5, b6, b7, wsem, csem):
    first = lax.axis_index("sq") * T
    load_h = []
    for e in range(2):
        rows = pl.ds(e * (B // 2), B // 2)
        load_h.append(pltpu.make_async_copy(hid_hbm.at[rows], hid.at[rows], wsem.at[NQ + e]))
        load_h[-1].start()
    load_wkv = pltpu.make_async_copy(wkv_hbm, wkv, wsem.at[NQ + 2])
    load_wkv.start()
    load_wq = []
    for j in range(NQ):
        cols = pl.ds(j * QB, QB)
        load_wq.append(pltpu.make_async_copy(wq_hbm.at[:, cols], wq.at[:, cols], wsem.at[j]))
        load_wq[-1].start()
    loads = [pltpu.make_async_copy(src.at[pl.ds(0, AB)], dst, csem.at[e]) for e, (src, dst) in enumerate(((k_hbm, kbuf), (v_hbm, vbuf)))]
    for c in loads:
        c.start()

    def norm_rows(i, _):
        rows = pl.ds(pl.multiple_of(i * 16, 16), 16)
        x = hid[rows, :].astype(F32)
        mean = jnp.sum(x, axis=-1, keepdims=True) * (1.0 / D)
        cen = x - mean
        var = jnp.sum(cen * cen, axis=-1, keepdims=True) * (1.0 / D)
        y = cen * lax.rsqrt(var + 1e-5)
        h[rows, :] = (y * gain_ref[...] + bias_ref[...]).astype(BF16)
        return 0

    for e in range(2):
        load_h[e].wait()
        lax.fori_loop(e * (B // 32), (e + 1) * (B // 32), norm_rows, 0, unroll=2)
    load_wkv.wait()
    new_kv = (jnp.dot(h[...], wkv[...], preferred_element_type=F32) + bkv_ref[...]).astype(BF16).astype(F32)
    kv[0:B, :] = new_kv[:, :DH]
    kv[B:2 * B, :] = new_kv[:, DH:]
    for j in range(NQ):
        load_wq[j].wait()
        cols = pl.ds(j * QB, QB)
        q = jnp.dot(h[...], wq[:, cols], preferred_element_type=F32) + bq_ref[:, cols]
        q = q.astype(BF16).astype(F32)
        for n in range(QB // DH):
            q3[pl.ds(j * (QB // DH) + n, B, stride=H), :] = q[:, n * DH:(n + 1) * DH]
    for c in loads:
        c.wait()
    insert_rows(lens, first, kv, (kbuf, vbuf), 0, AB, 0)
    stores = [pltpu.make_async_copy(src, dst.at[pl.ds(0, AB)], csem.at[2 + e]) for e, (src, dst) in enumerate(((kbuf, ko_hbm), (vbuf, vo_hbm)))]
    for c in stores:
        c.start()
    attention_stages(lens, first, q3, kbuf, vbuf, 0, 0, kv, o_ref, lse_ref, (b0, b1, b2, b3, b4, b5, b6, b7))(0)
    for c in stores:
        c.wait()


def column(tile, j):
    return tile[:, j:j + 1]


def merge(la, lb):
    top = jnp.maximum(la, lb)
    wa, wb = jnp.exp2(la - top), jnp.exp2(lb - top)
    tot = wa + wb
    return wa / tot, wb / tot, top + jnp.log2(tot)


def exchange_kernel(lens, q3, kv, o_first, lse_first, k_hbm, v_hbm, wo_hbm, y_ref, held,
                    wo, o_ref, lse_ref, b0, b1, b2, b3, b4, b5, b6, b7, o_core, l_core, o_mix, l_mix, o_x, l_x, a_all, part, p_y,
                    wsem, csem, a0s, a0r, a1s, a1r, a2s, a2r, bs, br, cs, cr, ds, dr):
    sq, tp = lax.axis_index("sq"), lax.axis_index("tp")
    x, c = sq // 2, sq % 2
    mate = {"sq": x * 2 + 1 - c}
    over_x = {"sq": (1 - x) * 2 + c}
    over_y = {"tp": 1 - tp}
    loads = {}

    def fetch(k):
        rows = pl.ds(k * AB, AB)
        loads[k] = [pltpu.make_async_copy(src.at[rows], held.at[pl.ds((k - 1) * AB + e * (B - AB), AB)], csem.at[2 * k + e - 2])
                    for e, src in enumerate((k_hbm, v_hbm))]
        for cp in loads[k]:
            cp.start()

    fetch(1)
    fetch(2)
    load = pltpu.make_async_copy(wo_hbm.at[:, pl.ds(pl.multiple_of(c * DC, DC), DC)], wo, wsem)
    load.start()
    fetch(3)
    bar = pltpu.get_barrier_semaphore()
    for dev in (mate, over_x, over_y):
        pl.semaphore_signal(bar, inc=1, device_id=dev, device_id_type=MESH)
    pl.semaphore_wait(bar, 3)

    def send(src, dst, ssem, rsem, dev):
        cp = pltpu.make_async_remote_copy(src, dst, ssem, rsem, device_id=dev, device_id_type=MESH)
        cp.start()
        return cp

    W = S * H
    hop0, hop1, hop2, hopb, hopc, hopd = {}, {}, {}, {}, {}, {}
    stages = attention_stages(lens, sq * T, q3, held, held, AB, AB - (B - AB), kv, o_ref, lse_ref, (b0, b1, b2, b3, b4, b5, b6, b7))
    ready = []

    def attend(k):
        block = k * CS // AB
        for cp in loads[block]:
            cp.wait()
        stages(block)

    def source(k):
        return (o_first, lse_first) if k * CS < AB else (o_ref, lse_ref)

    def rows_of_o(k, xx, cc):
        return pl.ds(pl.multiple_of((k * 4 + xx * 2 + cc) * W, W), W)

    def share(k):
        o_k, l_k = source(k)
        hop0[k] = [send(o_k.at[rows_of_o(k, xx, 1 - c)], o_core.at[k, xx], a0s.at[k, xx], a0r.at[k, xx], mate) for xx in range(2)]
        hop0[k].append(send(l_k.at[pl.ds(k * H, H)], l_core.at[k], a0s.at[k, 2], a0r.at[k, 2], mate))

    def mix(k):
        o_k, l_k = source(k)
        for cp in hop0[k]:
            cp.wait_recv()
        shift = lax.rem(DH - c * S, DH)
        fa, fb, lm = merge(pltpu.roll(l_k[pl.ds(k * H, H), :], shift, 1), pltpu.roll(l_core[k], shift, 1))
        l_mix[k] = lm
        for xx in range(2):
            mine = (k * 4 + xx * 2 + c) * W
            for j in range(S):
                oa = o_k[pl.ds(pl.multiple_of(mine + j * H, H), H), :]
                ob = o_core[k, xx, j * H:(j + 1) * H, :]
                at = xx * R + j
                o_mix[k, xx, j * H:(j + 1) * H, :] = column(fa, at) * oa + column(fb, at) * ob
        hop1[k] = [send(o_mix.at[k, 1 - x], o_x.at[k], a1s.at[k, 0], a1r.at[k, 0], over_x),
                   send(l_mix.at[k], l_x.at[k], a1s.at[k, 1], a1r.at[k, 1], over_x)]

    def quarter(k):
        for cp in hop1[k]:
            cp.wait_recv()
        shift = lax.rem(DH - x * R, DH)
        fa, fb, _ = merge(pltpu.roll(l_mix[k], shift, 1), pltpu.roll(l_x[k], shift, 1))
        for j in range(S):
            oa = o_mix[k, x, j * H:(j + 1) * H, :]
            ob = o_x[k, j * H:(j + 1) * H, :]
            a_all[k, pl.ds(pl.multiple_of(c * W + j * H, H), H), :] = column(fa, j) * oa + column(fb, j) * ob
        own = pl.ds(pl.multiple_of(c * W, W), W)
        hop2[k] = send(a_all.at[k, own], a_all.at[k, own], a2s.at[k], a2r.at[k], mate)

    def project(k):
        hop2[k].wait_recv()
        a = jnp.concatenate([a_all[k, pl.ds(n, R, stride=H), :].astype(BF16) for n in range(H)], 1)
        if not ready:
            load.wait()
            ready.append(1)
        part[k] = jnp.dot(a, wo[...], preferred_element_type=F32)
        hopb[k] = send(part.at[k, :, pl.ds(pl.multiple_of((1 - tp) * DY, DY), DY)], p_y.at[k], bs.at[k], br.at[k], over_y)

    def piece(k, xx, yy, lo=0, width=DY):
        return (pl.ds(pl.multiple_of(k * CS + xx * R, R), R), pl.ds(pl.multiple_of(c * DC + yy * DY + lo, 128), width))

    def pass_on(at, ssem, rsem, dev):
        return send(y_ref.at[at], y_ref.at[at], ssem, rsem, dev)

    def finish(k):
        hopb[k].wait_recv()
        at = piece(k, x, tp)
        y_ref[at] = part[k, :, pl.ds(pl.multiple_of(tp * DY, DY), DY)] + p_y[k]
        hopc[k] = [pass_on(at, cs.at[k, 0], cr.at[k, 0], over_x), pass_on(at, cs.at[k, 1], cr.at[k, 1], over_y)]
        hopd[k] = [pass_on(at, ds.at[k, 0], dr.at[k, 0], mate)]

    def relay(k):
        hopc[k][1].wait_recv()
        hopc[k].append(pass_on(piece(k, x, 1 - tp, VIA_Y, DY - VIA_Y), cs.at[k, 2], cr.at[k, 2], over_x))
        hopd[k].append(pass_on(piece(k, x, 1 - tp), ds.at[k, 1], dr.at[k, 1], mate))
        hopc[k][0].wait_recv()
        hopc[k].append(pass_on(piece(k, 1 - x, tp, 0, VIA_Y), cs.at[k, 3], cr.at[k, 3], over_y))
        hopd[k].append(pass_on(piece(k, 1 - x, tp), ds.at[k, 2], dr.at[k, 2], mate))

    def last(k):
        hopc[k][2].wait_recv()
        hopc[k][3].wait_recv()
        hopd[k].append(pass_on(piece(k, 1 - x, 1 - tp), ds.at[k, 3], dr.at[k, 3], mate))

    for step, k in SCHEDULE:
        {"a": attend, "s": share, "m": mix, "q": quarter, "p": project, "f": finish, "r": relay, "l": last}[step](k)
    for k in range(NC):
        for cp in hopd[k]:
            cp.wait_recv()
    for k in range(NC):
        for cp in [*hop0[k], *hop1[k], hop2[k], hopb[k], *hopc[k], *hopd[k]]:
            cp.wait_send()


def last_kernel(lens, kv, y_in, hid, bo_ref, held, k_part, v_part, ko_hbm, vo_hbm, out_hbm, ktile, vtile, out, sem, osem, tsem):
    first = lax.axis_index("sq") * T
    sub = lax.broadcasted_iota(jnp.int32, (16, DH), 0)
    sides = ((0, ktile, ko_hbm), (B - AB, vtile, vo_hbm))
    blocks = range(1, B // AB)
    copies = {}
    for k in blocks:
        for e, (src, _, dst) in enumerate(sides):
            copies[k, e] = pltpu.make_async_copy(held.at[pl.ds(src + (k - 1) * AB, AB)], dst.at[pl.ds(k * AB, AB)], sem.at[2 * k + e - 2])
            copies[k, e].start()

    def rows(i, _):
        r = pl.ds(pl.multiple_of(i * 16, 16), 16)
        out[r, :] = (hid[r, :].astype(F32) + y_in[r, :] + bo_ref[...]).astype(BF16)
        return 0

    lax.fori_loop(0, B // 16, rows, 0, unroll=2)
    store_out = pltpu.make_async_copy(out, out_hbm, osem)
    store_out.start()

    def spot(b):
        row = lens[b] - first
        start = pl.multiple_of((jnp.clip(row, 0, T - 1) // 16) * 16, 16)
        return row, start

    def build(b, _):
        row, start = spot(b)
        hit = sub == row - start
        for c, (src, tile, _) in enumerate(sides):
            new = kv[pl.ds(c * B + b, 1), :]
            old = held[b - AB + src, pl.ds(start, 16), :].astype(F32)
            tile[b - AB] = jnp.where(hit, new, old).astype(BF16)
        return 0

    lax.fori_loop(AB, B, build, 0, unroll=4)

    def put(b, _):
        _, start = spot(b)
        for e, (_, tile, dst) in enumerate(sides):
            pltpu.make_async_copy(tile.at[b - AB], dst.at[b, pl.ds(start, 16), :], tsem.at[e]).start()
        return 0

    for k in blocks:
        for e in range(2):
            copies[k, e].wait()
        lax.fori_loop(k * AB, (k + 1) * AB, put, 0, unroll=4)
    store_out.wait()
    for e, (_, tile, dst) in enumerate(sides):
        pltpu.make_async_copy(tile, dst.at[pl.ds(0, B - AB), pl.ds(0, 16), :], tsem.at[e]).wait()


def solution(mesh):
    def local_step(hidden, cache_lens, k_cache, v_cache, ln_gain, ln_bias, w_query, b_query, w_kv, b_kv, w_out, b_out):
        hbm = pl.BlockSpec(memory_space=pltpu.HBM)
        vm = pl.BlockSpec(memory_space=pltpu.VMEM)
        smem = pl.BlockSpec(memory_space=pltpu.SMEM)
        sem = pltpu.SemaphoreType.DMA

        def pin(*arrays):
            return [pltpu.with_memory_space_constraint(a, pltpu.VMEM) for a in arrays]

        def far(*arrays):
            return [pltpu.with_memory_space_constraint(a, pltpu.HBM) for a in arrays]

        cache = jax.ShapeDtypeStruct((B, T, DH), BF16)
        q3, kv, o0, lse0, k_part, v_part = pl.pallas_call(
            first_kernel,
            out_shape=(pltpu.VMEM((B * H, DH), F32), pltpu.VMEM((2 * B, DH), F32), pltpu.VMEM((AB * H, DH), F32), pltpu.VMEM((AB // CS * H, DH), F32), cache, cache),
            in_specs=[smem, hbm, hbm, hbm, vm, vm, hbm, vm, hbm, vm],
            out_specs=(vm, vm, vm, vm, hbm, hbm),
            scratch_shapes=[
                pltpu.VMEM((B, D), BF16), pltpu.VMEM((B, D), BF16), pltpu.VMEM((D, H * DH), BF16), pltpu.VMEM((D, 2 * DH), BF16),
                pltpu.VMEM((AB, T, DH), BF16), pltpu.VMEM((AB, T, DH), BF16), *STAGE_BUFS, sem((NQ + 3,)), sem((4,)),
            ],
            compiler_params=pltpu.CompilerParams(vmem_limit_bytes=33 * MIB),
            name="first",
        )(*far(cache_lens, hidden, k_cache, v_cache, ln_gain[None], ln_bias[None], w_query, b_query[None], w_kv, b_kv[None]))
        held = pltpu.VMEM((2 * (B - AB), T, DH), BF16)
        y, kv_held = pl.pallas_call(
            exchange_kernel,
            out_shape=(pltpu.VMEM((B, D), F32), held),
            in_specs=[smem, vm, vm, vm, vm, hbm, hbm, hbm],
            out_specs=(vm, vm),
            scratch_shapes=[
                pltpu.VMEM((H * DH, DC), BF16), pltpu.VMEM((B * H, DH), F32), pltpu.VMEM((NC * H, DH), F32), *STAGE_BUFS,
                pltpu.VMEM((NC, 2, S * H, DH), F32), pltpu.VMEM((NC, H, DH), F32),
                pltpu.VMEM((NC, 2, S * H, DH), F32), pltpu.VMEM((NC, H, DH), F32),
                pltpu.VMEM((NC, S * H, DH), F32), pltpu.VMEM((NC, H, DH), F32),
                pltpu.VMEM((NC, R * H, DH), F32), pltpu.VMEM((NC, R, DC), F32), pltpu.VMEM((NC, R, DY), F32),
                sem, sem((2 * (B // AB) - 2,)), sem((NC, 3)), sem((NC, 3)), sem((NC, 2)), sem((NC, 2)), sem((NC,)), sem((NC,)),
                sem((NC,)), sem((NC,)), sem((NC, 4)), sem((NC, 4)), sem((NC, 4)), sem((NC, 4)),
            ],
            compiler_params=pltpu.CompilerParams(vmem_limit_bytes=24 * MIB, collective_id=0, has_side_effects=True),
            name="exchange",
        )(*far(cache_lens), *pin(q3, kv, o0, lse0), *far(k_cache, v_cache, w_out))
        k_new, v_new, out_hidden = pl.pallas_call(
            last_kernel,
            out_shape=(cache, cache, jax.ShapeDtypeStruct((B, D), BF16)),
            in_specs=[smem, vm, vm, vm, vm, vm, hbm, hbm],
            out_specs=(hbm, hbm, hbm),
            input_output_aliases={6: 0, 7: 1},
            scratch_shapes=[pltpu.VMEM((B - AB, 16, DH), BF16), pltpu.VMEM((B - AB, 16, DH), BF16), pltpu.VMEM((B, D), BF16),
                            sem((2 * (B // AB) - 2,)), sem, sem((2,))],
            compiler_params=pltpu.CompilerParams(vmem_limit_bytes=6 * MIB),
            name="last",
        )(*far(cache_lens), *pin(kv, y), hidden, b_out[None], *pin(kv_held), k_part, v_part)
        return out_hidden, k_new, v_new

    cache_spec = P("dp", "sq", None)
    row_spec = P("dp", None)
    in_specs = (row_spec, P("dp"), cache_spec, cache_spec, P(None), P(None), P(None, "tp"), P("tp"), P(None, None), P(None), P("tp", None), P(None))
    out_specs = (row_spec, cache_spec, cache_spec)
    return jax.shard_map(local_step, mesh=mesh, in_specs=in_specs, out_specs=out_specs, check_vma=False)
```

```python
import functools
import math

import jax
import jax.numpy as jnp
from jax import lax
from jax.experimental import pallas as pl
from jax.experimental.pallas import tpu as pltpu
from jax.sharding import PartitionSpec as P

MESH = pl.DeviceIdType.MESH
F32 = jnp.float32
BF16 = jnp.bfloat16
NEG = -1e30
B = 256
D = 4096
H = 16
DH = 128
T = 256
AB = 64
NC = 8
CS = B // NC
S = CS // 4
R = 2 * S
DC = D // 2
DY = DC // 2
QB = 512
NQ = H * DH // QB
QSCALE = DH ** -0.5 * math.log2(math.e)
GROUP = 8
MIB = 1024 * 1024
VIA_Y = 128
SCHEDULE = [(s[0], int(s[1])) for s in "s0 s1 m0 a2 m1 s2 s3 a4 s4 s5 m2 m3 q0 m4 q1 m5 p0 p1 q2 a6 f0 q3 s6 s7 q4 f1 p2 m6 m7 p3 r0 p4 f2 q5 q6 q7 f3 r1 p5 f4 r2 p6 l0 l1 r3 p7 f5 r4 f6 f7 l2 r5 l3 l4 r6 r7 l5 l6 l7".split()]
def attention_stages(lens, first, q3, kbuf, vbuf, base, vbase, kv, o_ref, lse_ref, bufs):
    lane = lax.broadcasted_iota(jnp.int32, (H, DH), 1)
    pos = lax.broadcasted_iota(jnp.int32, (H, T), 1)
    zero = jnp.zeros((H, DH), BF16)
    s_a, s_b, p_a, p_b, r_a, r_b, n_a, n_b = bufs

    def score(i, s_out):
        for u in range(0, GROUP, 2):
            b = i * GROUP + u
            q0 = q3[pl.ds(pl.multiple_of(b * H, H), H), :].astype(BF16)
            q1 = q3[pl.ds(pl.multiple_of(b * H + H, H), H), :].astype(BF16)
            lhs = jnp.concatenate([jnp.concatenate([q0, zero], 1), jnp.concatenate([zero, q1], 1)], 0)
            keys = jnp.concatenate([kbuf[b - base], kbuf[b + 1 - base]], 1)
            s_out[u * H:(u + 2) * H, :] = lax.dot_general(lhs, keys, (((1,), (1,)), ((), ())), preferred_element_type=F32)

    def soften(i, s_in, p_out, r_out, n_out):
        chunk = lax.div(i * GROUP, CS)
        tile = pl.ds(pl.multiple_of(chunk * H, H), H)
        at = i * GROUP - chunk * CS
        lses = lse_ref[tile, :]
        for u in range(GROUP):
            b = i * GROUP + u
            row = lens[b] - first
            here = jnp.logical_and(row >= 0, row < T)
            k_new = kv[pl.ds(b, 1), :]
            v_new = kv[pl.ds(B + b, 1), :]
            q_row = q3[pl.ds(pl.multiple_of(b * H, H), H), :]
            s_new = jnp.where(here, jnp.sum(q_row * k_new, axis=1, keepdims=True) * QSCALE, NEG)
            se = jnp.where(pos < row, s_in[u * H:(u + 1) * H, :] * QSCALE, NEG)
            m = jnp.maximum(jnp.max(se, axis=1, keepdims=True), s_new)
            p = jnp.exp2(se - m)
            p_new = jnp.exp2(s_new - m)
            l = jnp.sum(p, axis=1, keepdims=True) + p_new
            r = 1.0 / l
            p_out[u * H:(u + 1) * H, :] = p.astype(BF16)
            r_out[u * H:(u + 1) * H, :] = jnp.broadcast_to(r, (H, DH))
            n_out[u * H:(u + 1) * H, :] = (p_new * r) * v_new
            lses = jnp.where(lane == at + u, m + jnp.log2(l), lses)
        lse_ref[tile, :] = lses

    def weigh(i, p_in, r_in, n_in):
        for u in range(0, GROUP, 2):
            b = i * GROUP + u
            vals = jnp.concatenate([vbuf[b - vbase], vbuf[b + 1 - vbase]], 1)
            o = jnp.dot(p_in[u * H:(u + 2) * H, :], vals, preferred_element_type=F32)
            for e in range(2):
                part = slice((u + e) * H, (u + e + 1) * H)
                o_ref[pl.ds(pl.multiple_of((b + e) * H, H), H), :] = (
                    o[e * H:(e + 1) * H, e * DH:(e + 1) * DH] * r_in[part, :] + n_in[part, :])

    def attend(k):
        tiles = slice(k * AB // CS * H, (k + 1) * AB // CS * H)
        lse_ref[tiles, :] = jnp.zeros((AB // CS * H, DH), F32)
        lo, hi = k * AB // GROUP, (k + 1) * AB // GROUP
        score(lo, s_a)
        score(lo + 1, s_b)
        soften(lo, s_a, p_a, r_a, n_a)

        def body(t, _):
            i = lo + 2 + 2 * t
            score(i, s_a)
            soften(i - 1, s_b, p_b, r_b, n_b)
            weigh(i - 2, p_a, r_a, n_a)
            score(i + 1, s_b)
            soften(i, s_a, p_a, r_a, n_a)
            weigh(i - 1, p_b, r_b, n_b)
            return 0

        lax.fori_loop(0, (hi - lo - 2) // 2, body, 0)
        soften(hi - 1, s_b, p_b, r_b, n_b)
        weigh(hi - 2, p_a, r_a, n_a)
        weigh(hi - 1, p_b, r_b, n_b)

    return attend


STAGE_BUFS = [pltpu.VMEM((GROUP * H, T), F32)] * 2 + [pltpu.VMEM((GROUP * H, T), BF16)] * 2 + [pltpu.VMEM((GROUP * H, DH), F32)] * 4


def insert_rows(lens, first, kv, pairs, lo, hi, base):
    sub = lax.broadcasted_iota(jnp.int32, (16, DH), 0)

    def insert(b, _):
        row = lens[b] - first
        start = pl.multiple_of((jnp.clip(row, 0, T - 1) // 16) * 16, 16)
        hit = sub == row - start
        for c, buf in enumerate(pairs):
            new = kv[pl.ds(c * B + b, 1), :]
            old = buf[b - base, pl.ds(start, 16), :].astype(F32)
            buf[b - base, pl.ds(start, 16), :] = jnp.where(hit, new, old).astype(BF16)
        return 0

    lax.fori_loop(lo, hi, insert, 0, unroll=4)


def first_kernel(lens_hbm, hid_hbm, k_hbm, v_hbm, gain_hbm, bias_hbm, wq_hbm, bq_hbm, wkv_hbm, bkv_hbm,
                 q3, kv, o_ref, lse_ref, ko_hbm, vo_hbm,
                 lens, gain_ref, bias_ref, bq_ref, bkv_ref, hid, h, wq, wkv, kbuf, vbuf, b0, b1, b2, b3, b4, b5, b6, b7, wsem, csem, ssem):
    first = lax.axis_index("sq") * T
    small = [pltpu.make_async_copy(src, dst, ssem.at[e]) for e, (src, dst) in enumerate((
        (gain_hbm, gain_ref), (bias_hbm, bias_ref), (bkv_hbm, bkv_ref), (bq_hbm, bq_ref), (lens_hbm, lens)))]
    load_h = []
    for e in range(2):
        rows = pl.ds(e * (B // 2), B // 2)
        load_h.append(pltpu.make_async_copy(hid_hbm.at[rows], hid.at[rows], wsem.at[NQ + e]))
        load_h[-1].start()
        if e == 0:
            for cp in small:
                cp.start()
    load_wkv = pltpu.make_async_copy(wkv_hbm, wkv, wsem.at[NQ + 2])
    load_wkv.start()
    load_wq = []
    for j in range(NQ):
        cols = pl.ds(j * QB, QB)
        load_wq.append(pltpu.make_async_copy(wq_hbm.at[:, cols], wq.at[:, cols], wsem.at[j]))
    loads = [pltpu.make_async_copy(src.at[pl.ds(0, AB)], dst, csem.at[e]) for e, (src, dst) in enumerate(((k_hbm, kbuf), (v_hbm, vbuf)))]
    for cp in [*load_wq[:-1], *loads, load_wq[-1]]:
        cp.start()
    small[0].wait()
    small[1].wait()

    def norm_rows(i, _):
        rows = pl.ds(pl.multiple_of(i * 16, 16), 16)
        x = hid[rows, :].astype(F32)
        mean = jnp.sum(x, axis=-1, keepdims=True) * (1.0 / D)
        cen = x - mean
        var = jnp.sum(cen * cen, axis=-1, keepdims=True) * (1.0 / D)
        y = cen * lax.rsqrt(var + 1e-5)
        h[rows, :] = (y * gain_ref[...] + bias_ref[...]).astype(BF16)
        return 0

    for e in range(2):
        load_h[e].wait()
        lax.fori_loop(e * (B // 32), (e + 1) * (B // 32), norm_rows, 0, unroll=2)
    load_wkv.wait()
    for cp in small[2:]:
        cp.wait()
    load_wq[0].wait()
    new_kv = (jnp.dot(h[...], wkv[...], preferred_element_type=F32) + bkv_ref[...]).astype(BF16).astype(F32)
    kv[0:B, :] = new_kv[:, :DH]
    kv[B:2 * B, :] = new_kv[:, DH:]
    stores = [pltpu.make_async_copy(src, dst.at[pl.ds(0, AB)], csem.at[2 + e]) for e, (src, dst) in enumerate(((kbuf, ko_hbm), (vbuf, vo_hbm)))]
    for j in range(NQ):
        cols = pl.ds(j * QB, QB)
        q = jnp.dot(h[...], wq[:, cols], preferred_element_type=F32) + bq_ref[:, cols]
        q = q.astype(BF16).astype(F32)
        if j < NQ - 2:
            load_wq[j + 1].wait()
        for n in range(QB // DH):
            q3[pl.ds(j * (QB // DH) + n, B, stride=H), :] = q[:, n * DH:(n + 1) * DH]
        if j == NQ - 2:
            for c in loads:
                c.wait()
            insert_rows(lens, first, kv, (kbuf, vbuf), 0, AB, 0)
            for c in stores:
                c.start()
            load_wq[j + 1].wait()
    attention_stages(lens, first, q3, kbuf, vbuf, 0, 0, kv, o_ref, lse_ref, (b0, b1, b2, b3, b4, b5, b6, b7))(0)
    for c in stores:
        c.wait()


def column(tile, j):
    return tile[:, j:j + 1]


def merge(la, lb):
    top = jnp.maximum(la, lb)
    wa, wb = jnp.exp2(la - top), jnp.exp2(lb - top)
    tot = wa + wb
    return wa / tot, wb / tot, top + jnp.log2(tot)


def exchange_kernel(lens_hbm, q3, kv, o_first, lse_first, k_hbm, v_hbm, wo_hbm, y_ref, held,
                    lens, wo, o_ref, lse_ref, b0, b1, b2, b3, b4, b5, b6, b7, o_core, l_core, o_mix, l_mix, l_half, o_x, l_x, a_all, part, p_y,
                    wsem, csem, nsem, a0s, a0r, a1s, a1r, a2s, a2r, bs, br, cs, cr, ds, dr):
    sq, tp = lax.axis_index("sq"), lax.axis_index("tp")
    x, c = sq // 2, sq % 2
    mate = {"sq": x * 2 + 1 - c}
    over_x = {"sq": (1 - x) * 2 + c}
    over_y = {"tp": 1 - tp}
    loads = {}
    bar = pltpu.get_barrier_semaphore()
    for dev in (mate, over_x, over_y):
        pl.semaphore_signal(bar, inc=1, device_id=dev, device_id_type=MESH)
    load_lens = pltpu.make_async_copy(lens_hbm, lens, nsem)
    load_lens.start()

    def fetch(k):
        rows = pl.ds(k * AB, AB)
        loads[k] = [pltpu.make_async_copy(src.at[rows], held.at[pl.ds((k - 1) * AB + e * (B - AB), AB)], csem.at[2 * k + e - 2])
                    for e, src in enumerate((k_hbm, v_hbm))]
        for cp in loads[k]:
            cp.start()

    fetch(1)
    fetch(2)
    load = pltpu.make_async_copy(wo_hbm.at[:, pl.ds(pl.multiple_of(c * DC, DC), DC)], wo, wsem)
    load.start()
    fetch(3)
    load_lens.wait()
    pl.semaphore_wait(bar, 3)

    def send(src, dst, ssem, rsem, dev):
        cp = pltpu.make_async_remote_copy(src, dst, ssem, rsem, device_id=dev, device_id_type=MESH)
        cp.start()
        return cp

    W = S * H
    hop0, hop1, hop2, hopb, hopc, hopd = {}, {}, {}, {}, {}, {}
    stages = attention_stages(lens, sq * T, q3, held, held, AB, AB - (B - AB), kv, o_ref, lse_ref, (b0, b1, b2, b3, b4, b5, b6, b7))
    ready = []
    lane8 = lax.broadcasted_iota(jnp.int32, (H // 2, DH), 1)

    def attend(k):
        block = k * CS // AB
        for cp in loads[block]:
            cp.wait()
        stages(block)

    def source(k):
        return (o_first, lse_first) if k * CS < AB else (o_ref, lse_ref)

    def rows_of_o(k, xx, cc):
        return pl.ds(pl.multiple_of((k * 4 + xx * 2 + cc) * W, W), W)

    def share(k):
        o_k, l_k = source(k)
        hop0[k] = [send(o_k.at[rows_of_o(k, xx, 1 - c)], o_core.at[k, xx], a0s.at[k, xx], a0r.at[k, xx], mate) for xx in range(2)]
        hop0[k].append(send(l_k.at[pl.ds(k * H, H)], l_core.at[k], a0s.at[k, 2], a0r.at[k, 2], mate))

    def mix(k):
        o_k, l_k = source(k)
        for cp in hop0[k]:
            cp.wait_recv()
        shift = lax.rem(DH - c * S, DH)
        fa, fb, lm = merge(pltpu.roll(l_k[pl.ds(k * H, H), :], shift, 1), pltpu.roll(l_core[k], shift, 1))
        l_mix[k] = lm
        theirs = pltpu.roll(lm, lax.rem(DH - (1 - x) * R, DH), 1)
        l_half[k] = jnp.where(lane8 < S, theirs[:H // 2], pltpu.roll(theirs[H // 2:], S, 1))
        for xx in range(2):
            mine = (k * 4 + xx * 2 + c) * W
            for j in range(S):
                oa = o_k[pl.ds(pl.multiple_of(mine + j * H, H), H), :]
                ob = o_core[k, xx, j * H:(j + 1) * H, :]
                at = xx * R + j
                o_mix[k, xx, j * H:(j + 1) * H, :] = column(fa, at) * oa + column(fb, at) * ob
        hop1[k] = [send(o_mix.at[k, 1 - x], o_x.at[k], a1s.at[k, 0], a1r.at[k, 0], over_x),
                   send(l_half.at[k], l_x.at[k], a1s.at[k, 1], a1r.at[k, 1], over_x)]

    def quarter(k):
        for cp in hop1[k]:
            cp.wait_recv()
        shift = lax.rem(DH - x * R, DH)
        l_far = jnp.concatenate([l_x[k], pltpu.roll(l_x[k], DH - S, 1)], 0)
        fa, fb, _ = merge(pltpu.roll(l_mix[k], shift, 1), l_far)
        for j in range(S):
            oa = o_mix[k, x, j * H:(j + 1) * H, :]
            ob = o_x[k, j * H:(j + 1) * H, :]
            a_all[k, pl.ds(pl.multiple_of(c * W + j * H, H), H), :] = column(fa, j) * oa + column(fb, j) * ob
        own = pl.ds(pl.multiple_of(c * W, W), W)
        hop2[k] = send(a_all.at[k, own], a_all.at[k, own], a2s.at[k], a2r.at[k], mate)

    def project(k):
        hop2[k].wait_recv()
        a = jnp.concatenate([a_all[k, pl.ds(n, R, stride=H), :].astype(BF16) for n in range(H)], 1)
        if not ready:
            load.wait()
            ready.append(1)
        part[k] = jnp.dot(a, wo[...], preferred_element_type=F32)
        hopb[k] = send(part.at[k, :, pl.ds(pl.multiple_of((1 - tp) * DY, DY), DY)], p_y.at[k], bs.at[k], br.at[k], over_y)

    def piece(k, xx, yy, lo=0, width=DY):
        return (pl.ds(pl.multiple_of(k * CS + xx * R, R), R), pl.ds(pl.multiple_of(c * DC + yy * DY + lo, 128), width))

    def pass_on(at, ssem, rsem, dev):
        return send(y_ref.at[at], y_ref.at[at], ssem, rsem, dev)

    def finish(k):
        hopb[k].wait_recv()
        at = piece(k, x, tp)
        y_ref[at] = part[k, :, pl.ds(pl.multiple_of(tp * DY, DY), DY)] + p_y[k]
        hopc[k] = [pass_on(at, cs.at[k, 0], cr.at[k, 0], over_x), pass_on(at, cs.at[k, 1], cr.at[k, 1], over_y)]
        hopd[k] = [pass_on(at, ds.at[k, 0], dr.at[k, 0], mate)]

    def relay(k):
        hopc[k][1].wait_recv()
        hopc[k].append(pass_on(piece(k, x, 1 - tp, VIA_Y, DY - VIA_Y), cs.at[k, 2], cr.at[k, 2], over_x))
        hopd[k].append(pass_on(piece(k, x, 1 - tp), ds.at[k, 1], dr.at[k, 1], mate))
        hopc[k][0].wait_recv()
        hopc[k].append(pass_on(piece(k, 1 - x, tp, 0, VIA_Y), cs.at[k, 3], cr.at[k, 3], over_y))
        hopd[k].append(pass_on(piece(k, 1 - x, tp), ds.at[k, 2], dr.at[k, 2], mate))

    def last(k):
        hopc[k][2].wait_recv()
        hopc[k][3].wait_recv()
        hopd[k].append(pass_on(piece(k, 1 - x, 1 - tp), ds.at[k, 3], dr.at[k, 3], mate))

    for step, k in SCHEDULE:
        {"a": attend, "s": share, "m": mix, "q": quarter, "p": project, "f": finish, "r": relay, "l": last}[step](k)
    for k in range(NC):
        for cp in hopd[k]:
            cp.wait_recv()
    for k in range(NC):
        for cp in [*hop0[k], *hop1[k], hop2[k], hopb[k], *hopc[k], *hopd[k]]:
            cp.wait_send()


def last_kernel(lens_hbm, kv, y_in, hid, bo_ref, held_in, k_part, v_part, ko_hbm, vo_hbm, out_hbm, held, lens, out, sem, osem):
    load_lens = pltpu.make_async_copy(lens_hbm, lens, osem)
    load_lens.start()

    def rows(i, _):
        r = pl.ds(pl.multiple_of(i * 16, 16), 16)
        out[r, :] = (hid[r, :].astype(F32) + y_in[r, :] + bo_ref[...]).astype(BF16)
        return 0

    lax.fori_loop(0, B // 32, rows, 0, unroll=2)
    load_lens.wait()
    first = lax.axis_index("sq") * T
    n = B - AB
    copies = []

    def put(k):
        insert_rows(lens, first, kv, (held.at[pl.ds(0, n)], held.at[pl.ds(n, n)]), k * AB, (k + 1) * AB, AB)
        for e, dst in enumerate((ko_hbm, vo_hbm)):
            copies.append(pltpu.make_async_copy(held.at[pl.ds(e * n + (k - 1) * AB, AB)], dst.at[pl.ds(k * AB, AB)], sem.at[2 * k + e - 2]))
            copies[-1].start()

    put(1)
    lax.fori_loop(B // 32, B // 16, rows, 0, unroll=2)
    copies.append(pltpu.make_async_copy(out, out_hbm, osem))
    copies[-1].start()
    for k in range(2, B // AB):
        put(k)
    for cp in copies:
        cp.wait()


def solution(mesh):
    def local_step(hidden, cache_lens, k_cache, v_cache, ln_gain, ln_bias, w_query, b_query, w_kv, b_kv, w_out, b_out):
        hbm = pl.BlockSpec(memory_space=pltpu.HBM)
        vm = pl.BlockSpec(memory_space=pltpu.VMEM)
        smem = pl.BlockSpec(memory_space=pltpu.SMEM)
        sem = pltpu.SemaphoreType.DMA

        def pin(*arrays):
            return [pltpu.with_memory_space_constraint(a, pltpu.VMEM) for a in arrays]

        def far(*arrays):
            return [pltpu.with_memory_space_constraint(a, pltpu.HBM) for a in arrays]

        cache = jax.ShapeDtypeStruct((B, T, DH), BF16)
        q3, kv, o0, lse0, k_part, v_part = pl.pallas_call(
            first_kernel,
            out_shape=(pltpu.VMEM((B * H, DH), F32), pltpu.VMEM((2 * B, DH), F32), pltpu.VMEM((AB * H, DH), F32), pltpu.VMEM((AB // CS * H, DH), F32), cache, cache),
            in_specs=[hbm] * 10,
            out_specs=(vm, vm, vm, vm, hbm, hbm),
            scratch_shapes=[
                pltpu.SMEM((B,), jnp.int32), pltpu.VMEM((1, D), F32), pltpu.VMEM((1, D), F32), pltpu.VMEM((1, H * DH), F32), pltpu.VMEM((1, 2 * DH), F32),
                pltpu.VMEM((B, D), BF16), pltpu.VMEM((B, D), BF16), pltpu.VMEM((D, H * DH), BF16), pltpu.VMEM((D, 2 * DH), BF16),
                pltpu.VMEM((AB, T, DH), BF16), pltpu.VMEM((AB, T, DH), BF16), *STAGE_BUFS, sem((NQ + 3,)), sem((4,)), sem((5,)),
            ],
            compiler_params=pltpu.CompilerParams(vmem_limit_bytes=33 * MIB),
            name="first",
        )(*far(cache_lens, hidden, k_cache, v_cache, ln_gain[None], ln_bias[None], w_query, b_query[None], w_kv, b_kv[None]))
        held = pltpu.VMEM((2 * (B - AB), T, DH), BF16)
        y, kv_held = pl.pallas_call(
            exchange_kernel,
            out_shape=(pltpu.VMEM((B, D), F32), held),
            in_specs=[hbm, vm, vm, vm, vm, hbm, hbm, hbm],
            out_specs=(vm, vm),
            scratch_shapes=[
                pltpu.SMEM((B,), jnp.int32),
                pltpu.VMEM((H * DH, DC), BF16), pltpu.VMEM((B * H, DH), F32), pltpu.VMEM((NC * H, DH), F32), *STAGE_BUFS,
                pltpu.VMEM((NC, 2, S * H, DH), F32), pltpu.VMEM((NC, H, DH), F32),
                pltpu.VMEM((NC, 2, S * H, DH), F32), pltpu.VMEM((NC, H, DH), F32), pltpu.VMEM((NC, H // 2, DH), F32),
                pltpu.VMEM((NC, S * H, DH), F32), pltpu.VMEM((NC, H // 2, DH), F32),
                pltpu.VMEM((NC, R * H, DH), F32), pltpu.VMEM((NC, R, DC), F32), pltpu.VMEM((NC, R, DY), F32),
                sem, sem((2 * (B // AB) - 2,)), sem, sem((NC, 3)), sem((NC, 3)), sem((NC, 2)), sem((NC, 2)), sem((NC,)), sem((NC,)),
                sem((NC,)), sem((NC,)), sem((NC, 4)), sem((NC, 4)), sem((NC, 4)), sem((NC, 4)),
            ],
            compiler_params=pltpu.CompilerParams(vmem_limit_bytes=24 * MIB, collective_id=0, has_side_effects=True),
            name="exchange",
        )(*far(cache_lens), *pin(q3, kv, o0, lse0), *far(k_cache, v_cache, w_out))
        k_new, v_new, out_hidden, _ = pl.pallas_call(
            last_kernel,
            out_shape=(cache, cache, jax.ShapeDtypeStruct((B, D), BF16), held),
            in_specs=[hbm, vm, vm, vm, vm, vm, hbm, hbm],
            out_specs=(hbm, hbm, hbm, vm),
            input_output_aliases={5: 3, 6: 0, 7: 1},
            scratch_shapes=[pltpu.SMEM((B,), jnp.int32), pltpu.VMEM((B, D), BF16), sem((2 * (B // AB) - 2,)), sem],
            compiler_params=pltpu.CompilerParams(vmem_limit_bytes=6 * MIB),
            name="last",
        )(*far(cache_lens), *pin(kv, y), hidden, b_out[None], *pin(kv_held), k_part, v_part)
        return out_hidden, k_new, v_new

    cache_spec = P("dp", "sq", None)
    row_spec = P("dp", None)
    in_specs = (row_spec, P("dp"), cache_spec, cache_spec, P(None), P(None), P(None, "tp"), P("tp"), P(None, None), P(None), P("tp", None), P(None))
    out_specs = (row_spec, cache_spec, cache_spec)
    return jax.shard_map(local_step, mesh=mesh, in_specs=in_specs, out_specs=out_specs, check_vma=False)
```

```python
import functools
import math

import jax
import jax.numpy as jnp
from jax import lax
from jax.experimental import pallas as pl
from jax.experimental.pallas import tpu as pltpu
from jax.sharding import PartitionSpec as P

MESH = pl.DeviceIdType.MESH
F32 = jnp.float32
BF16 = jnp.bfloat16
NEG = -1e30
B = 256
D = 4096
H = 16
DH = 128
T = 256
AB = 64
NC = 8
CS = B // NC
S = CS // 4
R = 2 * S
DC = D // 2
DY = DC // 2
QB = 512
HC = H // 2
NQ = HC * DH // QB
QSCALE = DH ** -0.5 * math.log2(math.e)
GROUP = 8
MIB = 1024 * 1024
MLIM = 24 * MIB
VIA_Y = 256
SCHEDULE = [(s[0], int(s[1])) for s in (
    "a0", "s0", "s1", "a2", "m0", "s2", "m1", "a4", "m2", "q0", "s5", "a6", "m5", "s3", "q1", "s7", "s4", "p0", "q2", "s6", "m3", "p1", "m4", "p2", "m6", "q5", "f0", "q3", "m7", "q4", "f1", "p3", "p4", "q6", "r0", "p5", "q7", "f2", "p6", "r1", "p7", "f4", "f3", "f5", "l0", "f6", "f7", "r2", "r3", "r4", "r5", "r6", "r7", "l1", "l2", "l3", "l4", "l5", "l6", "l7")]
def attention_stages(lens, first, q2, held, kv, o_ref, lse_ref, bufs):
    lane = lax.broadcasted_iota(jnp.int32, (H, DH), 1)
    pos = lax.broadcasted_iota(jnp.int32, (H, T), 1)
    zero = jnp.zeros((H, DH), BF16)
    s_a, s_b, p_a, p_b, r_a, r_b, n_a, n_b = bufs

    def query(b):
        rows = pl.ds(pl.multiple_of(b * HC, HC), HC)
        return jnp.concatenate([q2[0, rows, :], q2[1, rows, :]], 0)

    def score(i, s_out):
        for u in range(0, GROUP, 2):
            b = i * GROUP + u
            q0 = query(b).astype(BF16)
            q1 = query(b + 1).astype(BF16)
            lhs = jnp.concatenate([jnp.concatenate([q0, zero], 1), jnp.concatenate([zero, q1], 1)], 0)
            keys = jnp.concatenate([held[b], held[b + 1]], 1)
            s_out[u * H:(u + 2) * H, :] = lax.dot_general(lhs, keys, (((1,), (1,)), ((), ())), preferred_element_type=F32)

    def soften(i, s_in, p_out, r_out, n_out):
        chunk = lax.div(i * GROUP, CS)
        tile = pl.ds(pl.multiple_of(chunk * H, H), H)
        at = i * GROUP - chunk * CS
        lses = lse_ref[tile, :]
        for u in range(GROUP):
            b = i * GROUP + u
            row = lens[b] - first
            here = jnp.logical_and(row >= 0, row < T)
            k_new = kv[pl.ds(b, 1), :]
            v_new = kv[pl.ds(B + b, 1), :]
            q_row = query(b)
            s_new = jnp.where(here, jnp.sum(q_row * k_new, axis=1, keepdims=True) * QSCALE, NEG)
            se = jnp.where(pos < row, s_in[u * H:(u + 1) * H, :] * QSCALE, NEG)
            m = jnp.maximum(jnp.max(se, axis=1, keepdims=True), s_new)
            p = jnp.exp2(se - m)
            p_new = jnp.exp2(s_new - m)
            l = jnp.sum(p, axis=1, keepdims=True) + p_new
            r = 1.0 / l
            p_out[u * H:(u + 1) * H, :] = p.astype(BF16)
            r_out[u * H:(u + 1) * H, :] = jnp.broadcast_to(r, (H, DH))
            n_out[u * H:(u + 1) * H, :] = (p_new * r) * v_new
            lses = jnp.where(lane == at + u, m + jnp.log2(l), lses)
        lse_ref[tile, :] = lses

    def weigh(i, p_in, r_in, n_in):
        for u in range(0, GROUP, 2):
            b = i * GROUP + u
            vals = jnp.concatenate([held[B + b], held[B + b + 1]], 1)
            o = jnp.dot(p_in[u * H:(u + 2) * H, :], vals, preferred_element_type=F32)
            for e in range(2):
                part = slice((u + e) * H, (u + e + 1) * H)
                o_ref[pl.ds(pl.multiple_of((b + e) * H, H), H), :] = (
                    o[e * H:(e + 1) * H, e * DH:(e + 1) * DH] * r_in[part, :] + n_in[part, :])

    def attend(k):
        tiles = slice(k * AB // CS * H, (k + 1) * AB // CS * H)
        lse_ref[tiles, :] = jnp.zeros((AB // CS * H, DH), F32)
        lo, hi = k * AB // GROUP, (k + 1) * AB // GROUP
        score(lo, s_a)
        score(lo + 1, s_b)
        soften(lo, s_a, p_a, r_a, n_a)

        def body(t, _):
            i = lo + 2 + 2 * t
            score(i, s_a)
            soften(i - 1, s_b, p_b, r_b, n_b)
            weigh(i - 2, p_a, r_a, n_a)
            score(i + 1, s_b)
            soften(i, s_a, p_a, r_a, n_a)
            weigh(i - 1, p_b, r_b, n_b)
            return 0

        lax.fori_loop(0, (hi - lo - 2) // 2, body, 0)
        soften(hi - 1, s_b, p_b, r_b, n_b)
        weigh(hi - 2, p_a, r_a, n_a)
        weigh(hi - 1, p_b, r_b, n_b)

    return attend


STAGE_BUFS = [pltpu.VMEM((GROUP * H, T), F32)] * 2 + [pltpu.VMEM((GROUP * H, T), BF16)] * 2 + [pltpu.VMEM((GROUP * H, DH), F32)] * 4


def insert_rows(lens, first, kv, held, lo, hi):
    sub = lax.broadcasted_iota(jnp.int32, (16, DH), 0)

    def insert(b, _):
        row = lens[b] - first
        start = pl.multiple_of((jnp.clip(row, 0, T - 1) // 16) * 16, 16)
        hit = sub == row - start
        for c in range(2):
            new = kv[pl.ds(c * B + b, 1), :]
            old = held[c * B + b, pl.ds(start, 16), :].astype(F32)
            held[c * B + b, pl.ds(start, 16), :] = jnp.where(hit, new, old).astype(BF16)
        return 0

    lax.fori_loop(lo, hi, insert, 0, unroll=4)


def column(tile, j):
    return tile[:, j:j + 1]


def merge(la, lb):
    top = jnp.maximum(la, lb)
    wa, wb = jnp.exp2(la - top), jnp.exp2(lb - top)
    tot = wa + wb
    return wa / tot, wb / tot, top + jnp.log2(tot)


def step_kernel(lens_hbm, hid_hbm, k_hbm, v_hbm, gain_hbm, bias_hbm, wq_hbm, bq_hbm, wkv_hbm, bkv_hbm, wo_hbm,
                y_ref, held, kv,
                lens, gain_ref, bias_ref, bq_ref, bkv_ref, h, w, wkv, q2, o_ref, lse_ref, b0, b1, b2, b3, b4, b5, b6, b7,
                o_core, l_core, o_mix, l_mix, l_half, o_x, l_x, a_all, part, p_y,
                hsem, ssem, wsem, csem, qs, qr, a0s, a0r, a1s, a1r, a2s, a2r, bs, br, cs, cr, ds, dr):
    sq, tp = lax.axis_index("sq"), lax.axis_index("tp")
    x, c = sq // 2, sq % 2
    mate = {"sq": x * 2 + 1 - c}
    over_x = {"sq": (1 - x) * 2 + c}
    over_y = {"tp": 1 - tp}
    bar = pltpu.get_barrier_semaphore()
    for dev in (mate, over_x, over_y):
        pl.semaphore_signal(bar, inc=1, device_id=dev, device_id_type=MESH)
    halves = [pl.ds(e * (B // 2), B // 2) for e in range(2)]
    load_h = [pltpu.make_async_copy(hid_hbm.at[halves[e]], h.at[halves[e]], hsem.at[e]) for e in range(2)]
    own_q = HC * DH
    small = [pltpu.make_async_copy(src, dst, ssem.at[e]) for e, (src, dst) in enumerate((
        (gain_hbm, gain_ref), (bias_hbm, bias_ref), (bkv_hbm, bkv_ref),
        (bq_hbm.at[:, pl.ds(pl.multiple_of(c * own_q, own_q), own_q)], bq_ref), (lens_hbm, lens)))]
    load_wkv = pltpu.make_async_copy(wkv_hbm, wkv, hsem.at[2])
    load_wq = [pltpu.make_async_copy(wq_hbm.at[:, pl.ds(pl.multiple_of(c * own_q + j * QB, QB), QB)], w.at[:, pl.ds(j * QB, QB)], wsem.at[j])
               for j in range(NQ)]
    for cp in [load_h[0], *small, load_h[1], load_wkv, *load_wq]:
        cp.start()
    loads = {}

    def fetch(k):
        loads[k] = [pltpu.make_async_copy(src.at[pl.ds(k * AB, AB)], held.at[pl.ds(e * B + k * AB, AB)], csem.at[2 * k + e])
                    for e, src in enumerate((k_hbm, v_hbm))]
        for cp in loads[k]:
            cp.start()

    fetch(0)
    fetch(1)
    small[0].wait()
    small[1].wait()

    def norm_rows(i, _):
        rows = pl.ds(pl.multiple_of(i * 16, 16), 16)
        wide = h[rows, :].astype(F32)
        mean = jnp.sum(wide, axis=-1, keepdims=True) * (1.0 / D)
        cen = wide - mean
        var = jnp.sum(cen * cen, axis=-1, keepdims=True) * (1.0 / D)
        h[rows, :] = (cen * lax.rsqrt(var + 1e-5) * gain_ref[...] + bias_ref[...]).astype(BF16)
        return 0

    for e in range(2):
        load_h[e].wait()
        lax.fori_loop(e * (B // 32), (e + 1) * (B // 32), norm_rows, 0, unroll=2)
    load_wkv.wait()
    for cp in small[2:]:
        cp.wait()
    load_wq[0].wait()
    new_kv = (jnp.dot(h[...], wkv[...], preferred_element_type=F32) + bkv_ref[...]).astype(BF16).astype(F32)
    kv[0:B, :] = new_kv[:, :DH]
    kv[B:2 * B, :] = new_kv[:, DH:]
    for j in range(NQ):
        cols = pl.ds(j * QB, QB)
        q = jnp.dot(h[...], w[:, cols], preferred_element_type=F32) + bq_ref[:, cols]
        q = q.astype(BF16).astype(F32)
        if j < NQ - 1:
            load_wq[j + 1].wait()
        for n in range(QB // DH):
            q2[c, pl.ds(j * (QB // DH) + n, B, stride=HC), :] = q[:, n * DH:(n + 1) * DH]
    load_wo = []
    for e in range(2):
        cols = pl.ds(pl.multiple_of(c * DC + e * DY, DY), DY)
        load_wo.append(pltpu.make_async_copy(wo_hbm.at[:, cols], w.at[pl.ds(e * H * DH, H * DH)], wsem.at[NQ + e]))
        load_wo[-1].start()
    fetch(2)
    fetch(3)
    pl.semaphore_wait(bar, 3)

    def send(src, dst, ssem, rsem, dev):
        cp = pltpu.make_async_remote_copy(src, dst, ssem, rsem, device_id=dev, device_id_type=MESH)
        cp.start()
        return cp

    W = S * H
    Q = AB * HC
    swap = [send(q2.at[c, pl.ds(k * Q, Q)], q2.at[c, pl.ds(k * Q, Q)], qs.at[k], qr.at[k], mate) for k in range(B // AB)]
    hop0, hop1, hop2, hopb, hopc, hopd = {}, {}, {}, {}, {}, {}
    stages = attention_stages(lens, sq * T, q2, held, kv, o_ref, lse_ref, (b0, b1, b2, b3, b4, b5, b6, b7))
    ready = []
    lane8 = lax.broadcasted_iota(jnp.int32, (H // 2, DH), 1)

    def attend(k):
        block = k * CS // AB
        swap[block].wait_recv()
        for cp in loads[block]:
            cp.wait()
        stages(block)

    def rows_of_o(k, xx, cc):
        return pl.ds(pl.multiple_of((k * 4 + xx * 2 + cc) * W, W), W)

    def share(k):
        hop0[k] = [send(o_ref.at[rows_of_o(k, xx, 1 - c)], o_core.at[k, xx], a0s.at[k, xx], a0r.at[k, xx], mate) for xx in range(2)]
        hop0[k].append(send(lse_ref.at[pl.ds(k * H, H)], l_core.at[k], a0s.at[k, 2], a0r.at[k, 2], mate))

    def mix(k):
        for cp in hop0[k]:
            cp.wait_recv()
        shift = lax.rem(DH - c * S, DH)
        fa, fb, lm = merge(pltpu.roll(lse_ref[pl.ds(k * H, H), :], shift, 1), pltpu.roll(l_core[k], shift, 1))
        l_mix[k] = lm
        theirs = pltpu.roll(lm, lax.rem(DH - (1 - x) * R, DH), 1)
        l_half[k] = jnp.where(lane8 < S, theirs[:H // 2], pltpu.roll(theirs[H // 2:], S, 1))
        for xx in range(2):
            mine = (k * 4 + xx * 2 + c) * W
            for j in range(S):
                oa = o_ref[pl.ds(pl.multiple_of(mine + j * H, H), H), :]
                ob = o_core[k, xx, j * H:(j + 1) * H, :]
                at = xx * R + j
                o_mix[k, xx, j * H:(j + 1) * H, :] = column(fa, at) * oa + column(fb, at) * ob
        hop1[k] = [send(o_mix.at[k, 1 - x], o_x.at[k], a1s.at[k, 0], a1r.at[k, 0], over_x),
                   send(l_half.at[k], l_x.at[k], a1s.at[k, 1], a1r.at[k, 1], over_x)]

    def quarter(k):
        for cp in hop1[k]:
            cp.wait_recv()
        shift = lax.rem(DH - x * R, DH)
        l_far = jnp.concatenate([l_x[k], pltpu.roll(l_x[k], DH - S, 1)], 0)
        fa, fb, _ = merge(pltpu.roll(l_mix[k], shift, 1), l_far)
        for j in range(S):
            oa = o_mix[k, x, j * H:(j + 1) * H, :]
            ob = o_x[k, j * H:(j + 1) * H, :]
            a_all[k, pl.ds(pl.multiple_of(c * W + j * H, H), H), :] = column(fa, j) * oa + column(fb, j) * ob
        own = pl.ds(pl.multiple_of(c * W, W), W)
        hop2[k] = send(a_all.at[k, own], a_all.at[k, own], a2s.at[k], a2r.at[k], mate)

    def project(k):
        hop2[k].wait_recv()
        a = jnp.concatenate([a_all[k, pl.ds(n, R, stride=H), :].astype(BF16) for n in range(H)], 1)
        if not ready:
            for cp in load_wo:
                cp.wait()
            ready.append(1)
        for e in range(2):
            part[k, :, e * DY:(e + 1) * DY] = jnp.dot(a, w[e * H * DH:(e + 1) * H * DH, :], preferred_element_type=F32)
        hopb[k] = send(part.at[k, :, pl.ds(pl.multiple_of((1 - tp) * DY, DY), DY)], p_y.at[k], bs.at[k], br.at[k], over_y)

    def piece(k, xx, yy, lo=0, width=DY):
        return (pl.ds(pl.multiple_of(k * CS + xx * R, R), R), pl.ds(pl.multiple_of(c * DC + yy * DY + lo, 128), width))

    def pass_on(at, ssem, rsem, dev):
        return send(y_ref.at[at], y_ref.at[at], ssem, rsem, dev)

    def finish(k):
        hopb[k].wait_recv()
        at = piece(k, x, tp)
        y_ref[at] = part[k, :, pl.ds(pl.multiple_of(tp * DY, DY), DY)] + p_y[k]
        hopc[k] = [pass_on(at, cs.at[k, 0], cr.at[k, 0], over_x), pass_on(at, cs.at[k, 1], cr.at[k, 1], over_y)]
        hopd[k] = [pass_on(at, ds.at[k, 0], dr.at[k, 0], mate)]

    def relay(k):
        hopc[k][1].wait_recv()
        hopc[k].append(pass_on(piece(k, x, 1 - tp, VIA_Y, DY - VIA_Y), cs.at[k, 2], cr.at[k, 2], over_x))
        hopd[k].append(pass_on(piece(k, x, 1 - tp), ds.at[k, 1], dr.at[k, 1], mate))
        hopc[k][0].wait_recv()
        hopc[k].append(pass_on(piece(k, 1 - x, tp, 0, VIA_Y), cs.at[k, 3], cr.at[k, 3], over_y))
        hopd[k].append(pass_on(piece(k, 1 - x, tp), ds.at[k, 2], dr.at[k, 2], mate))

    def last(k):
        hopc[k][2].wait_recv()
        hopc[k][3].wait_recv()
        hopd[k].append(pass_on(piece(k, 1 - x, 1 - tp), ds.at[k, 3], dr.at[k, 3], mate))

    for step, k in SCHEDULE:
        {"a": attend, "s": share, "m": mix, "q": quarter, "p": project, "f": finish, "r": relay, "l": last}[step](k)
    for k in range(NC):
        for cp in hopd[k]:
            cp.wait_recv()
    for cp in swap:
        cp.wait_send()
    for k in range(NC):
        for cp in [*hop0[k], *hop1[k], hop2[k], hopb[k], *hopc[k], *hopd[k]]:
            cp.wait_send()


def last_kernel(lens_hbm, kv, y_in, hid_hbm, bo_hbm, held_in, ko_hbm, vo_hbm, out_hbm, held, lens, hid, bo_ref, out, sem, isem, osem):
    load = [pltpu.make_async_copy(src, dst, isem.at[e]) for e, (src, dst) in enumerate(((lens_hbm, lens), (bo_hbm, bo_ref), (hid_hbm, hid)))]
    for cp in load:
        cp.start()

    def rows(i, _):
        r = pl.ds(pl.multiple_of(i * 16, 16), 16)
        out[r, :] = (hid[r, :].astype(F32) + y_in[r, :] + bo_ref[...]).astype(BF16)
        return 0

    first = lax.axis_index("sq") * T
    copies = []

    def put(k):
        insert_rows(lens, first, kv, held, k * AB, (k + 1) * AB)
        for e, dst in enumerate((ko_hbm, vo_hbm)):
            copies.append(pltpu.make_async_copy(held.at[pl.ds(e * B + k * AB, AB)], dst.at[pl.ds(k * AB, AB)], sem.at[2 * k + e]))
            copies[-1].start()

    load[0].wait()
    put(0)
    load[1].wait()
    load[2].wait()
    lax.fori_loop(0, B // 16, rows, 0, unroll=2)
    copies.append(pltpu.make_async_copy(out, out_hbm, osem))
    copies[-1].start()
    for k in range(1, B // AB):
        put(k)
    for cp in copies:
        cp.wait()


def solution(mesh):
    def local_step(hidden, cache_lens, k_cache, v_cache, ln_gain, ln_bias, w_query, b_query, w_kv, b_kv, w_out, b_out):
        hbm = pl.BlockSpec(memory_space=pltpu.HBM)
        vm = pl.BlockSpec(memory_space=pltpu.VMEM)
        sem = pltpu.SemaphoreType.DMA

        def pin(*arrays):
            return [pltpu.with_memory_space_constraint(a, pltpu.VMEM) for a in arrays]

        def far(*arrays):
            return [pltpu.with_memory_space_constraint(a, pltpu.HBM) for a in arrays]

        held = pltpu.VMEM((2 * B, T, DH), BF16)
        y, kv_held, kv = pl.pallas_call(
            step_kernel,
            out_shape=(pltpu.VMEM((B, D), F32), held, pltpu.VMEM((2 * B, DH), F32)),
            in_specs=[hbm] * 11,
            out_specs=(vm, vm, vm),
            scratch_shapes=[
                pltpu.SMEM((B,), jnp.int32), pltpu.VMEM((1, D), F32), pltpu.VMEM((1, D), F32), pltpu.VMEM((1, HC * DH), F32), pltpu.VMEM((1, 2 * DH), F32),
                pltpu.VMEM((B, D), BF16), pltpu.VMEM((D, HC * DH), BF16), pltpu.VMEM((D, 2 * DH), BF16), pltpu.VMEM((2, B * HC, DH), F32),
                pltpu.VMEM((B * H, DH), F32), pltpu.VMEM((NC * H, DH), F32), *STAGE_BUFS,
                pltpu.VMEM((NC, 2, S * H, DH), F32), pltpu.VMEM((NC, H, DH), F32),
                pltpu.VMEM((NC, 2, S * H, DH), F32), pltpu.VMEM((NC, H, DH), F32), pltpu.VMEM((NC, H // 2, DH), F32),
                pltpu.VMEM((NC, S * H, DH), F32), pltpu.VMEM((NC, H // 2, DH), F32),
                pltpu.VMEM((NC, R * H, DH), F32), pltpu.VMEM((NC, R, DC), F32), pltpu.VMEM((NC, R, DY), F32),
                sem((3,)), sem((5,)), sem((NQ + 2,)), sem((2 * (B // AB),)), sem((B // AB,)), sem((B // AB,)),
                sem((NC, 3)), sem((NC, 3)), sem((NC, 2)), sem((NC, 2)), sem((NC,)), sem((NC,)),
                sem((NC,)), sem((NC,)), sem((NC, 4)), sem((NC, 4)), sem((NC, 4)), sem((NC, 4)),
            ],
            compiler_params=pltpu.CompilerParams(vmem_limit_bytes=MLIM, collective_id=0, has_side_effects=True),
            name="step",
        )(*far(cache_lens, hidden, k_cache, v_cache, ln_gain[None], ln_bias[None], w_query, b_query[None], w_kv, b_kv[None], w_out))
        cache = jax.ShapeDtypeStruct((B, T, DH), BF16)
        k_new, v_new, out_hidden, _ = pl.pallas_call(
            last_kernel,
            out_shape=(cache, cache, jax.ShapeDtypeStruct((B, D), BF16), held),
            in_specs=[hbm, vm, vm, hbm, hbm, vm],
            out_specs=(hbm, hbm, hbm, vm),
            input_output_aliases={5: 3},
            scratch_shapes=[pltpu.SMEM((B,), jnp.int32), pltpu.VMEM((B, D), BF16), pltpu.VMEM((1, D), F32), pltpu.VMEM((B, D), BF16),
                            sem((2 * (B // AB),)), sem((3,)), sem],
            compiler_params=pltpu.CompilerParams(vmem_limit_bytes=24 * MIB),
            name="last",
        )(*far(cache_lens), *pin(kv, y), *far(hidden, b_out[None]), *pin(kv_held))
        return out_hidden, k_new, v_new

    cache_spec = P("dp", "sq", None)
    row_spec = P("dp", None)
    in_specs = (row_spec, P("dp"), cache_spec, cache_spec, P(None), P(None), P(None, "tp"), P("tp"), P(None, None), P(None), P("tp", None), P(None))
    out_specs = (row_spec, cache_spec, cache_spec)
    return jax.shard_map(local_step, mesh=mesh, in_specs=in_specs, out_specs=out_specs, check_vma=False)
```

```python
import functools
import math

import jax
import jax.numpy as jnp
from jax import lax
from jax.experimental import pallas as pl
from jax.experimental.pallas import tpu as pltpu
from jax.sharding import PartitionSpec as P

MESH = pl.DeviceIdType.MESH
F32 = jnp.float32
BF16 = jnp.bfloat16
NEG = -1e30
B = 256
D = 4096
H = 16
DH = 128
T = 256
AB = 64
NC = 8
CS = B // NC
S = CS // 4
R = 2 * S
DC = D // 2
DY = DC // 2
QB = 512
HC = H // 2
NQ = HC * DH // QB
QSCALE = DH ** -0.5 * math.log2(math.e)
GROUP = 8
MIB = 1024 * 1024
MLIM = 24 * MIB
VIA_Y = 384
SCHEDULE = [(s[0], int(s[1])) for s in (
    "a0", "s0", "s1", "a2", "s3", "s2", "m1", "m0", "a4", "m2", "s4", "a6", "s5", "q0", "m4", "s6", "q1", "m3", "s7", "q2", "p0", "p1", "p2", "m5", "q3", "m6", "f0", "m7", "f1", "q4", "p3", "q5", "f2", "p4", "q6", "p5", "f3", "q7", "p6", "r1", "p7", "f5", "f4", "f6", "r0", "l1", "f7", "r5", "r3", "r4", "r2", "r6", "r7", "l5", "l4", "l3", "l0", "l2", "l6", "l7")]
def attention_stages(lens, first, q2, held, kv, o_ref, lse_ref, bufs):
    lane = lax.broadcasted_iota(jnp.int32, (H, DH), 1)
    pos = lax.broadcasted_iota(jnp.int32, (H, T), 1)
    zero = jnp.zeros((H, DH), BF16)
    s_a, s_b, p_a, p_b, r_a, r_b, n_a, n_b = bufs

    def query(b):
        rows = pl.ds(pl.multiple_of(b * HC, HC), HC)
        return jnp.concatenate([q2[0, rows, :], q2[1, rows, :]], 0)

    def score(i, s_out):
        for u in range(0, GROUP, 2):
            b = i * GROUP + u
            q0 = query(b).astype(BF16)
            q1 = query(b + 1).astype(BF16)
            lhs = jnp.concatenate([jnp.concatenate([q0, zero], 1), jnp.concatenate([zero, q1], 1)], 0)
            keys = jnp.concatenate([held[b], held[b + 1]], 1)
            s_out[u * H:(u + 2) * H, :] = lax.dot_general(lhs, keys, (((1,), (1,)), ((), ())), preferred_element_type=F32)

    def soften(i, s_in, p_out, r_out, n_out):
        chunk = lax.div(i * GROUP, CS)
        tile = pl.ds(pl.multiple_of(chunk * H, H), H)
        at = i * GROUP - chunk * CS
        lses = lse_ref[tile, :]
        for u in range(GROUP):
            b = i * GROUP + u
            row = lens[b] - first
            here = jnp.logical_and(row >= 0, row < T)
            k_new = kv[pl.ds(b, 1), :]
            v_new = kv[pl.ds(B + b, 1), :]
            q_row = query(b)
            s_new = jnp.where(here, jnp.sum(q_row * k_new, axis=1, keepdims=True) * QSCALE, NEG)
            se = jnp.where(pos < row, s_in[u * H:(u + 1) * H, :] * QSCALE, NEG)
            m = jnp.maximum(jnp.max(se, axis=1, keepdims=True), s_new)
            p = jnp.exp2(se - m)
            p_new = jnp.exp2(s_new - m)
            l = jnp.sum(p, axis=1, keepdims=True) + p_new
            r = 1.0 / l
            p_out[u * H:(u + 1) * H, :] = p.astype(BF16)
            r_out[u * H:(u + 1) * H, :] = jnp.broadcast_to(r, (H, DH))
            n_out[u * H:(u + 1) * H, :] = (p_new * r) * v_new
            lses = jnp.where(lane == at + u, m + jnp.log2(l), lses)
        lse_ref[tile, :] = lses

    def weigh(i, p_in, r_in, n_in):
        for u in range(0, GROUP, 2):
            b = i * GROUP + u
            vals = jnp.concatenate([held[B + b], held[B + b + 1]], 1)
            o = jnp.dot(p_in[u * H:(u + 2) * H, :], vals, preferred_element_type=F32)
            for e in range(2):
                part = slice((u + e) * H, (u + e + 1) * H)
                o_ref[pl.ds(pl.multiple_of((b + e) * H, H), H), :] = (
                    o[e * H:(e + 1) * H, e * DH:(e + 1) * DH] * r_in[part, :] + n_in[part, :])

    def attend(k):
        tiles = slice(k * AB // CS * H, (k + 1) * AB // CS * H)
        lse_ref[tiles, :] = jnp.zeros((AB // CS * H, DH), F32)
        lo, hi = k * AB // GROUP, (k + 1) * AB // GROUP
        score(lo, s_a)
        score(lo + 1, s_b)
        soften(lo, s_a, p_a, r_a, n_a)

        def body(t):
            i = lo + 2 + 2 * t
            score(i, s_a)
            soften(i - 1, s_b, p_b, r_b, n_b)
            weigh(i - 2, p_a, r_a, n_a)
            score(i + 1, s_b)
            soften(i, s_a, p_a, r_a, n_a)
            weigh(i - 1, p_b, r_b, n_b)

        for t in range((hi - lo - 2) // 2):
            body(t)
        soften(hi - 1, s_b, p_b, r_b, n_b)
        weigh(hi - 2, p_a, r_a, n_a)
        weigh(hi - 1, p_b, r_b, n_b)

    return attend


STAGE_BUFS = [pltpu.VMEM((GROUP * H, T), F32)] * 2 + [pltpu.VMEM((GROUP * H, T), BF16)] * 2 + [pltpu.VMEM((GROUP * H, DH), F32)] * 4


def insert_rows(lens, first, kv, held, lo, hi):
    sub = lax.broadcasted_iota(jnp.int32, (16, DH), 0)

    def insert(b, _):
        row = lens[b] - first
        start = pl.multiple_of((jnp.clip(row, 0, T - 1) // 16) * 16, 16)
        hit = sub == row - start
        for c in range(2):
            new = kv[pl.ds(c * B + b, 1), :]
            old = held[c * B + b, pl.ds(start, 16), :].astype(F32)
            held[c * B + b, pl.ds(start, 16), :] = jnp.where(hit, new, old).astype(BF16)
        return 0

    lax.fori_loop(lo, hi, insert, 0, unroll=4)


def column(tile, j):
    return tile[:, j:j + 1]


def merge(la, lb):
    top = jnp.maximum(la, lb)
    wa, wb = jnp.exp2(la - top), jnp.exp2(lb - top)
    tot = wa + wb
    return wa / tot, wb / tot, top + jnp.log2(tot)


def step_kernel(lens_hbm, hid_hbm, k_hbm, v_hbm, gain_hbm, bias_hbm, wq_hbm, bq_hbm, wkv_hbm, bkv_hbm, wo_hbm,
                y_ref, held, kv,
                lens, gain_ref, bias_ref, bq_ref, bkv_ref, h, mean_ref, rstd_ref, w, wkv, q2, o_ref, lse_ref, b0, b1, b2, b3, b4, b5, b6, b7,
                o_core, l_core, o_mix, l_mix, l_half, o_x, l_x, a_all, part, p_y,
                hsem, ssem, wsem, csem, qs, qr, a0s, a0r, a1s, a1r, a2s, a2r, bs, br, cs, cr, ds, dr):
    sq, tp = lax.axis_index("sq"), lax.axis_index("tp")
    x, c = sq // 2, sq % 2
    mate = {"sq": x * 2 + 1 - c}
    over_x = {"sq": (1 - x) * 2 + c}
    over_y = {"tp": 1 - tp}
    bar = pltpu.get_barrier_semaphore()
    for dev in (mate, over_x, over_y):
        pl.semaphore_signal(bar, inc=1, device_id=dev, device_id_type=MESH)
    halves = [pl.ds(e * (B // 2), B // 2) for e in range(2)]
    load_h = [pltpu.make_async_copy(hid_hbm.at[halves[e]], h.at[halves[e]], hsem.at[e]) for e in range(2)]
    own_q = HC * DH
    small = [pltpu.make_async_copy(src, dst, ssem.at[e]) for e, (src, dst) in enumerate((
        (gain_hbm, gain_ref), (bias_hbm, bias_ref), (bkv_hbm, bkv_ref),
        (bq_hbm.at[:, pl.ds(pl.multiple_of(c * own_q, own_q), own_q)], bq_ref), (lens_hbm, lens)))]
    load_wkv = pltpu.make_async_copy(wkv_hbm, wkv, hsem.at[2])
    load_wq = [pltpu.make_async_copy(wq_hbm.at[:, pl.ds(pl.multiple_of(c * own_q + j * QB, QB), QB)], w.at[:, pl.ds(j * QB, QB)], wsem.at[j])
               for j in range(NQ)]
    for cp in [load_h[0], *small, load_h[1], load_wkv, *load_wq]:
        cp.start()
    loads = {}

    def fetch(k):
        loads[k] = [pltpu.make_async_copy(src.at[pl.ds(k * AB, AB)], held.at[pl.ds(e * B + k * AB, AB)], csem.at[2 * k + e])
                    for e, src in enumerate((k_hbm, v_hbm))]
        for cp in loads[k]:
            cp.start()

    fetch(0)
    fetch(1)
    small[0].wait()
    small[1].wait()

    def spread(tile):
        return jnp.concatenate([tile] * (D // DH), 1)

    def block(i):
        return pl.ds(pl.multiple_of(i * 16, 16), 16)

    def means(i, _):
        total = jnp.sum(h[block(i), :].astype(F32), axis=-1, keepdims=True)
        mean_ref[block(i), :] = jnp.broadcast_to(total * (1.0 / D), (16, DH))
        return 0

    def scales(i, _):
        cen = h[block(i), :].astype(F32) - spread(mean_ref[block(i), :])
        var = jnp.sum(cen * cen, axis=-1, keepdims=True) * (1.0 / D)
        rstd_ref[block(i), :] = jnp.broadcast_to(lax.rsqrt(var + 1e-5), (16, DH))
        return 0

    def normed(i, _):
        y = (h[block(i), :].astype(F32) - spread(mean_ref[block(i), :])) * spread(rstd_ref[block(i), :])
        h[block(i), :] = (y * gain_ref[...] + bias_ref[...]).astype(BF16)
        return 0

    for e in range(2):
        load_h[e].wait()
        lo, hi = e * (B // 32), (e + 1) * (B // 32)
        lax.fori_loop(lo, hi, means, 0, unroll=4)
        lax.fori_loop(lo, hi, scales, 0, unroll=4)
        lax.fori_loop(lo, hi, normed, 0, unroll=2)
    load_wkv.wait()
    for cp in small[2:]:
        cp.wait()
    load_wq[0].wait()
    new_kv = (jnp.dot(h[...], wkv[...], preferred_element_type=F32) + bkv_ref[...]).astype(BF16).astype(F32)
    kv[0:B, :] = new_kv[:, :DH]
    kv[B:2 * B, :] = new_kv[:, DH:]
    for j in range(NQ):
        cols = pl.ds(j * QB, QB)
        q = jnp.dot(h[...], w[:, cols], preferred_element_type=F32) + bq_ref[:, cols]
        q = q.astype(BF16).astype(F32)
        if j < NQ - 1:
            load_wq[j + 1].wait()
        for n in range(QB // DH):
            q2[c, pl.ds(j * (QB // DH) + n, B, stride=HC), :] = q[:, n * DH:(n + 1) * DH]
    load_wo = []
    for e in range(2):
        cols = pl.ds(pl.multiple_of(c * DC + e * DY, DY), DY)
        load_wo.append(pltpu.make_async_copy(wo_hbm.at[:, cols], w.at[pl.ds(e * H * DH, H * DH)], wsem.at[NQ + e]))
        load_wo[-1].start()
    fetch(2)
    fetch(3)
    pl.semaphore_wait(bar, 3)

    def send(src, dst, ssem, rsem, dev):
        cp = pltpu.make_async_remote_copy(src, dst, ssem, rsem, device_id=dev, device_id_type=MESH)
        cp.start()
        return cp

    W = S * H
    Q = AB * HC
    swap = [send(q2.at[c, pl.ds(k * Q, Q)], q2.at[c, pl.ds(k * Q, Q)], qs.at[k], qr.at[k], mate) for k in range(B // AB)]
    hop0, hop1, hop2, hopb, hopc, hopd = {}, {}, {}, {}, {}, {}
    stages = attention_stages(lens, sq * T, q2, held, kv, o_ref, lse_ref, (b0, b1, b2, b3, b4, b5, b6, b7))
    ready = []
    lane8 = lax.broadcasted_iota(jnp.int32, (H // 2, DH), 1)

    def attend(k):
        block = k * CS // AB
        swap[block].wait_recv()
        for cp in loads[block]:
            cp.wait()
        stages(block)

    def rows_of_o(k, xx, cc):
        return pl.ds(pl.multiple_of((k * 4 + xx * 2 + cc) * W, W), W)

    def share(k):
        hop0[k] = [send(o_ref.at[rows_of_o(k, xx, 1 - c)], o_core.at[k, xx], a0s.at[k, xx], a0r.at[k, xx], mate) for xx in range(2)]
        hop0[k].append(send(lse_ref.at[pl.ds(k * H, H)], l_core.at[k], a0s.at[k, 2], a0r.at[k, 2], mate))

    def mix(k):
        for cp in hop0[k]:
            cp.wait_recv()
        shift = lax.rem(DH - c * S, DH)
        fa, fb, lm = merge(pltpu.roll(lse_ref[pl.ds(k * H, H), :], shift, 1), pltpu.roll(l_core[k], shift, 1))
        l_mix[k] = lm
        theirs = pltpu.roll(lm, lax.rem(DH - (1 - x) * R, DH), 1)
        l_half[k] = jnp.where(lane8 < S, theirs[:H // 2], pltpu.roll(theirs[H // 2:], S, 1))
        for xx in range(2):
            mine = (k * 4 + xx * 2 + c) * W
            for j in range(S):
                oa = o_ref[pl.ds(pl.multiple_of(mine + j * H, H), H), :]
                ob = o_core[k, xx, j * H:(j + 1) * H, :]
                at = xx * R + j
                o_mix[k, xx, j * H:(j + 1) * H, :] = column(fa, at) * oa + column(fb, at) * ob
        hop1[k] = [send(o_mix.at[k, 1 - x], o_x.at[k], a1s.at[k, 0], a1r.at[k, 0], over_x),
                   send(l_half.at[k], l_x.at[k], a1s.at[k, 1], a1r.at[k, 1], over_x)]

    def quarter(k):
        for cp in hop1[k]:
            cp.wait_recv()
        shift = lax.rem(DH - x * R, DH)
        l_far = jnp.concatenate([l_x[k], pltpu.roll(l_x[k], DH - S, 1)], 0)
        fa, fb, _ = merge(pltpu.roll(l_mix[k], shift, 1), l_far)
        for j in range(S):
            oa = o_mix[k, x, j * H:(j + 1) * H, :]
            ob = o_x[k, j * H:(j + 1) * H, :]
            a_all[k, pl.ds(pl.multiple_of(c * W + j * H, H), H), :] = column(fa, j) * oa + column(fb, j) * ob
        own = pl.ds(pl.multiple_of(c * W, W), W)
        hop2[k] = send(a_all.at[k, own], a_all.at[k, own], a2s.at[k], a2r.at[k], mate)

    def project(k):
        hop2[k].wait_recv()
        a = jnp.concatenate([a_all[k, pl.ds(n, R, stride=H), :].astype(BF16) for n in range(H)], 1)
        if not ready:
            for cp in load_wo:
                cp.wait()
            ready.append(1)
        for e in range(2):
            part[k, :, e * DY:(e + 1) * DY] = jnp.dot(a, w[e * H * DH:(e + 1) * H * DH, :], preferred_element_type=F32)
        hopb[k] = send(part.at[k, :, pl.ds(pl.multiple_of((1 - tp) * DY, DY), DY)], p_y.at[k], bs.at[k], br.at[k], over_y)

    def piece(k, xx, yy, lo=0, width=DY):
        return (pl.ds(pl.multiple_of(k * CS + xx * R, R), R), pl.ds(pl.multiple_of(c * DC + yy * DY + lo, 128), width))

    def pass_on(at, ssem, rsem, dev):
        return send(y_ref.at[at], y_ref.at[at], ssem, rsem, dev)

    def finish(k):
        hopb[k].wait_recv()
        at = piece(k, x, tp)
        y_ref[at] = part[k, :, pl.ds(pl.multiple_of(tp * DY, DY), DY)] + p_y[k]
        hopc[k] = [pass_on(at, cs.at[k, 0], cr.at[k, 0], over_x), pass_on(at, cs.at[k, 1], cr.at[k, 1], over_y)]
        hopd[k] = [pass_on(at, ds.at[k, 0], dr.at[k, 0], mate)]

    def relay(k):
        hopc[k][1].wait_recv()
        hopc[k].append(pass_on(piece(k, x, 1 - tp, VIA_Y, DY - VIA_Y), cs.at[k, 2], cr.at[k, 2], over_x))
        hopd[k].append(pass_on(piece(k, x, 1 - tp), ds.at[k, 1], dr.at[k, 1], mate))
        hopc[k][0].wait_recv()
        hopc[k].append(pass_on(piece(k, 1 - x, tp, 0, VIA_Y), cs.at[k, 3], cr.at[k, 3], over_y))
        hopd[k].append(pass_on(piece(k, 1 - x, tp), ds.at[k, 2], dr.at[k, 2], mate))

    def last(k):
        hopc[k][2].wait_recv()
        hopc[k][3].wait_recv()
        hopd[k].append(pass_on(piece(k, 1 - x, 1 - tp), ds.at[k, 3], dr.at[k, 3], mate))

    for step, k in SCHEDULE:
        {"a": attend, "s": share, "m": mix, "q": quarter, "p": project, "f": finish, "r": relay, "l": last}[step](k)
    for k in range(NC):
        for cp in hopd[k]:
            cp.wait_recv()
    for cp in swap:
        cp.wait_send()
    for k in range(NC):
        for cp in [*hop0[k], *hop1[k], hop2[k], hopb[k], *hopc[k], *hopd[k]]:
            cp.wait_send()


def last_kernel(lens_hbm, kv, y_in, hid_hbm, bo_hbm, held_in, ko_hbm, vo_hbm, out_hbm, held, lens, hid, bo_ref, out, sem, isem, osem):
    load = [pltpu.make_async_copy(src, dst, isem.at[e]) for e, (src, dst) in enumerate(((lens_hbm, lens), (bo_hbm, bo_ref), (hid_hbm, hid)))]
    for cp in load:
        cp.start()

    def rows(i, _):
        r = pl.ds(pl.multiple_of(i * 16, 16), 16)
        out[r, :] = (hid[r, :].astype(F32) + y_in[r, :] + bo_ref[...]).astype(BF16)
        return 0

    first = lax.axis_index("sq") * T
    copies = []

    def put(lo, hi):
        insert_rows(lens, first, kv, held, lo, hi)
        for e, dst in enumerate((ko_hbm, vo_hbm)):
            copies.append(pltpu.make_async_copy(held.at[pl.ds(e * B + lo, hi - lo)], dst.at[pl.ds(lo, hi - lo)], sem.at[len(copies)]))
            copies[-1].start()

    load[0].wait()
    put(0, 16)
    put(16, 32)
    put(32, 64)
    put(64, 128)
    load[1].wait()
    load[2].wait()
    lax.fori_loop(0, B // 16, rows, 0, unroll=2)
    store_out = pltpu.make_async_copy(out, out_hbm, osem)
    store_out.start()
    put(128, 192)
    put(192, 256)
    store_out.wait()
    for cp in copies:
        cp.wait()


def solution(mesh):
    def local_step(hidden, cache_lens, k_cache, v_cache, ln_gain, ln_bias, w_query, b_query, w_kv, b_kv, w_out, b_out):
        hbm = pl.BlockSpec(memory_space=pltpu.HBM)
        vm = pl.BlockSpec(memory_space=pltpu.VMEM)
        sem = pltpu.SemaphoreType.DMA

        def pin(*arrays):
            return [pltpu.with_memory_space_constraint(a, pltpu.VMEM) for a in arrays]

        def far(*arrays):
            return [pltpu.with_memory_space_constraint(a, pltpu.HBM) for a in arrays]

        held = pltpu.VMEM((2 * B, T, DH), BF16)
        y, kv_held, kv = pl.pallas_call(
            step_kernel,
            out_shape=(pltpu.VMEM((B, D), F32), held, pltpu.VMEM((2 * B, DH), F32)),
            in_specs=[hbm] * 11,
            out_specs=(vm, vm, vm),
            scratch_shapes=[
                pltpu.SMEM((B,), jnp.int32), pltpu.VMEM((1, D), F32), pltpu.VMEM((1, D), F32), pltpu.VMEM((1, HC * DH), F32), pltpu.VMEM((1, 2 * DH), F32),
                pltpu.VMEM((B, D), BF16), pltpu.VMEM((B, DH), F32), pltpu.VMEM((B, DH), F32), pltpu.VMEM((D, HC * DH), BF16), pltpu.VMEM((D, 2 * DH), BF16), pltpu.VMEM((2, B * HC, DH), F32),
                pltpu.VMEM((B * H, DH), F32), pltpu.VMEM((NC * H, DH), F32), *STAGE_BUFS,
                pltpu.VMEM((NC, 2, S * H, DH), F32), pltpu.VMEM((NC, H, DH), F32),
                pltpu.VMEM((NC, 2, S * H, DH), F32), pltpu.VMEM((NC, H, DH), F32), pltpu.VMEM((NC, H // 2, DH), F32),
                pltpu.VMEM((NC, S * H, DH), F32), pltpu.VMEM((NC, H // 2, DH), F32),
                pltpu.VMEM((NC, R * H, DH), F32), pltpu.VMEM((NC, R, DC), F32), pltpu.VMEM((NC, R, DY), F32),
                sem((3,)), sem((5,)), sem((NQ + 2,)), sem((2 * (B // AB),)), sem((B // AB,)), sem((B // AB,)),
                sem((NC, 3)), sem((NC, 3)), sem((NC, 2)), sem((NC, 2)), sem((NC,)), sem((NC,)),
                sem((NC,)), sem((NC,)), sem((NC, 4)), sem((NC, 4)), sem((NC, 4)), sem((NC, 4)),
            ],
            compiler_params=pltpu.CompilerParams(vmem_limit_bytes=MLIM, collective_id=0, has_side_effects=True),
            name="step",
        )(*far(cache_lens, hidden, k_cache, v_cache, ln_gain[None], ln_bias[None], w_query, b_query[None], w_kv, b_kv[None], w_out))
        cache = jax.ShapeDtypeStruct((B, T, DH), BF16)
        k_new, v_new, out_hidden, _ = pl.pallas_call(
            last_kernel,
            out_shape=(cache, cache, jax.ShapeDtypeStruct((B, D), BF16), held),
            in_specs=[hbm, vm, vm, hbm, hbm, vm],
            out_specs=(hbm, hbm, hbm, vm),
            input_output_aliases={5: 3},
            scratch_shapes=[pltpu.SMEM((B,), jnp.int32), pltpu.VMEM((B, D), BF16), pltpu.VMEM((1, D), F32), pltpu.VMEM((B, D), BF16),
                            sem((12,)), sem((3,)), sem],
            compiler_params=pltpu.CompilerParams(vmem_limit_bytes=24 * MIB),
            name="last",
        )(*far(cache_lens), *pin(kv, y), *far(hidden, b_out[None]), *pin(kv_held))
        return out_hidden, k_new, v_new

    cache_spec = P("dp", "sq", None)
    row_spec = P("dp", None)
    in_specs = (row_spec, P("dp"), cache_spec, cache_spec, P(None), P(None), P(None, "tp"), P("tp"), P(None, None), P(None), P("tp", None), P(None))
    out_specs = (row_spec, cache_spec, cache_spec)
    return jax.shard_map(local_step, mesh=mesh, in_specs=in_specs, out_specs=out_specs, check_vma=False)
```

```python
import functools
import math

import jax
import jax.numpy as jnp
from jax import lax
from jax.experimental import pallas as pl
from jax.experimental.pallas import tpu as pltpu
from jax.sharding import PartitionSpec as P

MESH = pl.DeviceIdType.MESH
F32 = jnp.float32
BF16 = jnp.bfloat16
NEG = -1e30
B = 256
D = 4096
H = 16
DH = 128
T = 256
AB = 64
NC = 8
CS = B // NC
S = CS // 4
R = 2 * S
DC = D // 2
DY = DC // 2
QB = 512
NQ = H * DH // QB
QSCALE = DH ** -0.5 * math.log2(math.e)
GROUP = 8
MIB = 1024 * 1024
VIA_Y = 128
SCHEDULE = [(s[0], int(s[1])) for s in (
    "s0", "s1", "m0", "a2", "m1", "s2", "s3", "a4", "s4", "s5", "m2", "m3", "q0", "m4", "q1", "m5", "p0", "p1", "q2", "a6", "f0", "q3", "s6", "s7", "q4", "f1", "p2", "m6", "m7", "p3", "r0", "p4", "f2", "q5", "q6", "q7", "f3", "r1", "p5", "f4", "r2", "p6", "l0", "l1", "r3", "p7", "f5", "r4", "f6", "f7", "l2", "r5", "l3", "l4", "r6", "r7", "l5", "l6", "l7")]

def attention_stages(lens, first, q3, kbuf, vbuf, base, vbase, kv, o_ref, lse_ref, bufs):
    lane = lax.broadcasted_iota(jnp.int32, (H, DH), 1)
    pos = lax.broadcasted_iota(jnp.int32, (H, T), 1)
    zero = jnp.zeros((H, DH), BF16)
    s_a, s_b, p_a, p_b, r_a, r_b, n_a, n_b = bufs

    def score(i, s_out):
        for u in range(0, GROUP, 2):
            b = i * GROUP + u
            q0 = q3[pl.ds(pl.multiple_of(b * H, H), H), :].astype(BF16)
            q1 = q3[pl.ds(pl.multiple_of(b * H + H, H), H), :].astype(BF16)
            lhs = jnp.concatenate([jnp.concatenate([q0, zero], 1), jnp.concatenate([zero, q1], 1)], 0)
            keys = jnp.concatenate([kbuf[b - base], kbuf[b + 1 - base]], 1)
            s_out[u * H:(u + 2) * H, :] = lax.dot_general(lhs, keys, (((1,), (1,)), ((), ())), preferred_element_type=F32)

    def soften(i, s_in, p_out, r_out, n_out):
        chunk = lax.div(i * GROUP, CS)
        tile = pl.ds(pl.multiple_of(chunk * H, H), H)
        at = i * GROUP - chunk * CS
        lses = lse_ref[tile, :]
        for u in range(GROUP):
            b = i * GROUP + u
            row = lens[b] - first
            here = jnp.logical_and(row >= 0, row < T)
            k_new = kv[pl.ds(b, 1), :]
            v_new = kv[pl.ds(B + b, 1), :]
            q_row = q3[pl.ds(pl.multiple_of(b * H, H), H), :]
            s_new = jnp.where(here, jnp.sum(q_row * k_new, axis=1, keepdims=True) * QSCALE, NEG)
            se = jnp.where(pos < row, s_in[u * H:(u + 1) * H, :] * QSCALE, NEG)
            m = jnp.maximum(jnp.max(se, axis=1, keepdims=True), s_new)
            p = jnp.exp2(se - m)
            p_new = jnp.exp2(s_new - m)
            l = jnp.sum(p, axis=1, keepdims=True) + p_new
            r = 1.0 / l
            p_out[u * H:(u + 1) * H, :] = p.astype(BF16)
            r_out[u * H:(u + 1) * H, :] = jnp.broadcast_to(r, (H, DH))
            n_out[u * H:(u + 1) * H, :] = (p_new * r) * v_new
            lses = jnp.where(lane == at + u, m + jnp.log2(l), lses)
        lse_ref[tile, :] = lses

    def weigh(i, p_in, r_in, n_in):
        for u in range(0, GROUP, 2):
            b = i * GROUP + u
            vals = jnp.concatenate([vbuf[b - vbase], vbuf[b + 1 - vbase]], 1)
            o = jnp.dot(p_in[u * H:(u + 2) * H, :], vals, preferred_element_type=F32)
            for e in range(2):
                part = slice((u + e) * H, (u + e + 1) * H)
                o_ref[pl.ds(pl.multiple_of((b + e) * H, H), H), :] = (
                    o[e * H:(e + 1) * H, e * DH:(e + 1) * DH] * r_in[part, :] + n_in[part, :])

    def attend(k):
        tiles = slice(k * AB // CS * H, (k + 1) * AB // CS * H)
        lse_ref[tiles, :] = jnp.zeros((AB // CS * H, DH), F32)
        lo, hi = k * AB // GROUP, (k + 1) * AB // GROUP
        score(lo, s_a)
        score(lo + 1, s_b)
        soften(lo, s_a, p_a, r_a, n_a)

        def body(t):
            i = lo + 2 + 2 * t
            score(i, s_a)
            soften(i - 1, s_b, p_b, r_b, n_b)
            weigh(i - 2, p_a, r_a, n_a)
            score(i + 1, s_b)
            soften(i, s_a, p_a, r_a, n_a)
            weigh(i - 1, p_b, r_b, n_b)

        for t in range((hi - lo - 2) // 2):
            body(t)
        soften(hi - 1, s_b, p_b, r_b, n_b)
        weigh(hi - 2, p_a, r_a, n_a)
        weigh(hi - 1, p_b, r_b, n_b)

    return attend


STAGE_BUFS = [pltpu.VMEM((GROUP * H, T), F32)] * 2 + [pltpu.VMEM((GROUP * H, T), BF16)] * 2 + [pltpu.VMEM((GROUP * H, DH), F32)] * 4


def insert_rows(lens, first, kv, pairs, lo, hi, base):
    sub = lax.broadcasted_iota(jnp.int32, (16, DH), 0)

    def insert(b, _):
        row = lens[b] - first
        start = pl.multiple_of((jnp.clip(row, 0, T - 1) // 16) * 16, 16)
        hit = sub == row - start
        for c, buf in enumerate(pairs):
            new = kv[pl.ds(c * B + b, 1), :]
            old = buf[b - base, pl.ds(start, 16), :].astype(F32)
            buf[b - base, pl.ds(start, 16), :] = jnp.where(hit, new, old).astype(BF16)
        return 0

    lax.fori_loop(lo, hi, insert, 0, unroll=4)


def first_kernel(lens_hbm, hid_hbm, k_hbm, v_hbm, gain_hbm, bias_hbm, wq_hbm, bq_hbm, wkv_hbm, bkv_hbm,
                 q3, kv, o_ref, lse_ref, ko_hbm, vo_hbm,
                 lens, gain_ref, bias_ref, bq_ref, bkv_ref, h, mean_ref, rstd_ref, wq, wkv, kbuf, vbuf, b0, b1, b2, b3, b4, b5, b6, b7, wsem, csem, ssem):
    first = lax.axis_index("sq") * T
    small = [pltpu.make_async_copy(src, dst, ssem.at[e]) for e, (src, dst) in enumerate((
        (gain_hbm, gain_ref), (bias_hbm, bias_ref), (bkv_hbm, bkv_ref), (bq_hbm, bq_ref), (lens_hbm, lens)))]
    load_h = []
    for e in range(2):
        rows = pl.ds(e * (B // 2), B // 2)
        load_h.append(pltpu.make_async_copy(hid_hbm.at[rows], h.at[rows], wsem.at[NQ + e]))
        load_h[-1].start()
        if e == 0:
            for cp in small:
                cp.start()
    load_wkv = pltpu.make_async_copy(wkv_hbm, wkv, wsem.at[NQ + 2])
    load_wkv.start()
    load_wq = []
    for j in range(NQ):
        cols = pl.ds(j * QB, QB)
        load_wq.append(pltpu.make_async_copy(wq_hbm.at[:, cols], wq.at[:, cols], wsem.at[j]))
    loads = [pltpu.make_async_copy(src.at[pl.ds(0, AB)], dst, csem.at[e]) for e, (src, dst) in enumerate(((k_hbm, kbuf), (v_hbm, vbuf)))]
    for cp in [*load_wq[:-1], *loads, load_wq[-1]]:
        cp.start()
    small[0].wait()
    small[1].wait()

    def spread(tile):
        return jnp.concatenate([tile] * (D // DH), 1)

    def block(i):
        return pl.ds(pl.multiple_of(i * 16, 16), 16)

    def means(i, _):
        total = jnp.sum(h[block(i), :].astype(F32), axis=-1, keepdims=True)
        mean_ref[block(i), :] = jnp.broadcast_to(total * (1.0 / D), (16, DH))
        return 0

    def scales(i, _):
        cen = h[block(i), :].astype(F32) - spread(mean_ref[block(i), :])
        var = jnp.sum(cen * cen, axis=-1, keepdims=True) * (1.0 / D)
        rstd_ref[block(i), :] = jnp.broadcast_to(lax.rsqrt(var + 1e-5), (16, DH))
        return 0

    def normed(i, _):
        y = (h[block(i), :].astype(F32) - spread(mean_ref[block(i), :])) * spread(rstd_ref[block(i), :])
        h[block(i), :] = (y * gain_ref[...] + bias_ref[...]).astype(BF16)
        return 0

    for e in range(2):
        load_h[e].wait()
        lo, hi = e * (B // 32), (e + 1) * (B // 32)
        lax.fori_loop(lo, hi, means, 0, unroll=4)
        lax.fori_loop(lo, hi, scales, 0, unroll=4)
        lax.fori_loop(lo, hi, normed, 0, unroll=2)
    load_wkv.wait()
    for cp in small[2:]:
        cp.wait()
    load_wq[0].wait()
    new_kv = (jnp.dot(h[...], wkv[...], preferred_element_type=F32) + bkv_ref[...]).astype(BF16).astype(F32)
    kv[0:B, :] = new_kv[:, :DH]
    kv[B:2 * B, :] = new_kv[:, DH:]
    stores = [pltpu.make_async_copy(src, dst.at[pl.ds(0, AB)], csem.at[2 + e]) for e, (src, dst) in enumerate(((kbuf, ko_hbm), (vbuf, vo_hbm)))]
    for j in range(NQ):
        cols = pl.ds(j * QB, QB)
        q = jnp.dot(h[...], wq[:, cols], preferred_element_type=F32) + bq_ref[:, cols]
        q = q.astype(BF16).astype(F32)
        if j < NQ - 2:
            load_wq[j + 1].wait()
        for n in range(QB // DH):
            q3[pl.ds(j * (QB // DH) + n, B, stride=H), :] = q[:, n * DH:(n + 1) * DH]
        if j == NQ - 2:
            for c in loads:
                c.wait()
            insert_rows(lens, first, kv, (kbuf, vbuf), 0, AB, 0)
            for c in stores:
                c.start()
            load_wq[j + 1].wait()
    attention_stages(lens, first, q3, kbuf, vbuf, 0, 0, kv, o_ref, lse_ref, (b0, b1, b2, b3, b4, b5, b6, b7))(0)
    for c in stores:
        c.wait()


def column(tile, j):
    return tile[:, j:j + 1]


def merge(la, lb):
    top = jnp.maximum(la, lb)
    wa, wb = jnp.exp2(la - top), jnp.exp2(lb - top)
    tot = wa + wb
    return wa / tot, wb / tot, top + jnp.log2(tot)


def exchange_kernel(lens_hbm, q3, kv, o_first, lse_first, k_hbm, v_hbm, wo_hbm, y_ref, held,
                    lens, wo, o_ref, lse_ref, b0, b1, b2, b3, b4, b5, b6, b7, o_core, l_core, o_mix, l_mix, l_half, o_x, l_x, a_all, part, p_y,
                    wsem, csem, nsem, a0s, a0r, a1s, a1r, a2s, a2r, bs, br, cs, cr, ds, dr):
    sq, tp = lax.axis_index("sq"), lax.axis_index("tp")
    x, c = sq // 2, sq % 2
    mate = {"sq": x * 2 + 1 - c}
    over_x = {"sq": (1 - x) * 2 + c}
    over_y = {"tp": 1 - tp}
    loads = {}
    bar = pltpu.get_barrier_semaphore()
    for dev in (mate, over_x, over_y):
        pl.semaphore_signal(bar, inc=1, device_id=dev, device_id_type=MESH)
    load_lens = pltpu.make_async_copy(lens_hbm, lens, nsem)
    load_lens.start()

    def fetch(k):
        rows = pl.ds(k * AB, AB)
        loads[k] = [pltpu.make_async_copy(src.at[rows], held.at[pl.ds((k - 1) * AB + e * (B - AB), AB)], csem.at[2 * k + e - 2])
                    for e, src in enumerate((k_hbm, v_hbm))]
        for cp in loads[k]:
            cp.start()

    fetch(1)
    fetch(2)
    load = pltpu.make_async_copy(wo_hbm.at[:, pl.ds(pl.multiple_of(c * DC, DC), DC)], wo, wsem)
    load.start()
    fetch(3)
    load_lens.wait()
    pl.semaphore_wait(bar, 3)

    def send(src, dst, ssem, rsem, dev):
        cp = pltpu.make_async_remote_copy(src, dst, ssem, rsem, device_id=dev, device_id_type=MESH)
        cp.start()
        return cp

    W = S * H
    hop0, hop1, hop2, hopb, hopc, hopd = {}, {}, {}, {}, {}, {}
    stages = attention_stages(lens, sq * T, q3, held, held, AB, AB - (B - AB), kv, o_ref, lse_ref, (b0, b1, b2, b3, b4, b5, b6, b7))
    ready = []
    lane8 = lax.broadcasted_iota(jnp.int32, (H // 2, DH), 1)

    def attend(k):
        block = k * CS // AB
        for cp in loads[block]:
            cp.wait()
        stages(block)

    def source(k):
        return (o_first, lse_first) if k * CS < AB else (o_ref, lse_ref)

    def rows_of_o(k, xx, cc):
        return pl.ds(pl.multiple_of((k * 4 + xx * 2 + cc) * W, W), W)

    def share(k):
        o_k, l_k = source(k)
        hop0[k] = [send(o_k.at[rows_of_o(k, xx, 1 - c)], o_core.at[k, xx], a0s.at[k, xx], a0r.at[k, xx], mate) for xx in range(2)]
        hop0[k].append(send(l_k.at[pl.ds(k * H, H)], l_core.at[k], a0s.at[k, 2], a0r.at[k, 2], mate))

    def mix(k):
        o_k, l_k = source(k)
        for cp in hop0[k]:
            cp.wait_recv()
        shift = lax.rem(DH - c * S, DH)
        fa, fb, lm = merge(pltpu.roll(l_k[pl.ds(k * H, H), :], shift, 1), pltpu.roll(l_core[k], shift, 1))
        l_mix[k] = lm
        theirs = pltpu.roll(lm, lax.rem(DH - (1 - x) * R, DH), 1)
        l_half[k] = jnp.where(lane8 < S, theirs[:H // 2], pltpu.roll(theirs[H // 2:], S, 1))
        for xx in range(2):
            mine = (k * 4 + xx * 2 + c) * W
            for j in range(S):
                oa = o_k[pl.ds(pl.multiple_of(mine + j * H, H), H), :]
                ob = o_core[k, xx, j * H:(j + 1) * H, :]
                at = xx * R + j
                o_mix[k, xx, j * H:(j + 1) * H, :] = column(fa, at) * oa + column(fb, at) * ob
        hop1[k] = [send(o_mix.at[k, 1 - x], o_x.at[k], a1s.at[k, 0], a1r.at[k, 0], over_x),
                   send(l_half.at[k], l_x.at[k], a1s.at[k, 1], a1r.at[k, 1], over_x)]

    def quarter(k):
        for cp in hop1[k]:
            cp.wait_recv()
        shift = lax.rem(DH - x * R, DH)
        l_far = jnp.concatenate([l_x[k], pltpu.roll(l_x[k], DH - S, 1)], 0)
        fa, fb, _ = merge(pltpu.roll(l_mix[k], shift, 1), l_far)
        for j in range(S):
            oa = o_mix[k, x, j * H:(j + 1) * H, :]
            ob = o_x[k, j * H:(j + 1) * H, :]
            a_all[k, pl.ds(pl.multiple_of(c * W + j * H, H), H), :] = column(fa, j) * oa + column(fb, j) * ob
        own = pl.ds(pl.multiple_of(c * W, W), W)
        hop2[k] = send(a_all.at[k, own], a_all.at[k, own], a2s.at[k], a2r.at[k], mate)

    def project(k):
        hop2[k].wait_recv()
        a = jnp.concatenate([a_all[k, pl.ds(n, R, stride=H), :].astype(BF16) for n in range(H)], 1)
        if not ready:
            load.wait()
            ready.append(1)
        part[k] = jnp.dot(a, wo[...], preferred_element_type=F32)
        hopb[k] = send(part.at[k, :, pl.ds(pl.multiple_of((1 - tp) * DY, DY), DY)], p_y.at[k], bs.at[k], br.at[k], over_y)

    def piece(k, xx, yy, lo=0, width=DY):
        return (pl.ds(pl.multiple_of(k * CS + xx * R, R), R), pl.ds(pl.multiple_of(c * DC + yy * DY + lo, 128), width))

    def pass_on(at, ssem, rsem, dev):
        return send(y_ref.at[at], y_ref.at[at], ssem, rsem, dev)

    def finish(k):
        hopb[k].wait_recv()
        at = piece(k, x, tp)
        y_ref[at] = part[k, :, pl.ds(pl.multiple_of(tp * DY, DY), DY)] + p_y[k]
        hopc[k] = [pass_on(at, cs.at[k, 0], cr.at[k, 0], over_x), pass_on(at, cs.at[k, 1], cr.at[k, 1], over_y)]
        hopd[k] = [pass_on(at, ds.at[k, 0], dr.at[k, 0], mate)]

    def relay(k):
        hopc[k][1].wait_recv()
        hopc[k].append(pass_on(piece(k, x, 1 - tp, VIA_Y, DY - VIA_Y), cs.at[k, 2], cr.at[k, 2], over_x))
        hopd[k].append(pass_on(piece(k, x, 1 - tp), ds.at[k, 1], dr.at[k, 1], mate))
        hopc[k][0].wait_recv()
        hopc[k].append(pass_on(piece(k, 1 - x, tp, 0, VIA_Y), cs.at[k, 3], cr.at[k, 3], over_y))
        hopd[k].append(pass_on(piece(k, 1 - x, tp), ds.at[k, 2], dr.at[k, 2], mate))

    def last(k):
        hopc[k][2].wait_recv()
        hopc[k][3].wait_recv()
        hopd[k].append(pass_on(piece(k, 1 - x, 1 - tp), ds.at[k, 3], dr.at[k, 3], mate))

    for step, k in SCHEDULE:
        {"a": attend, "s": share, "m": mix, "q": quarter, "p": project, "f": finish, "r": relay, "l": last}[step](k)
    for k in range(NC):
        for cp in hopd[k]:
            cp.wait_recv()
    for k in range(NC):
        for cp in [*hop0[k], *hop1[k], hop2[k], hopb[k], *hopc[k], *hopd[k]]:
            cp.wait_send()


def last_kernel(lens_hbm, kv, y_in, hid, bo_ref, held_in, k_part, v_part, ko_hbm, vo_hbm, out_hbm, held, lens, out, sem, osem):
    load_lens = pltpu.make_async_copy(lens_hbm, lens, osem)
    load_lens.start()

    def rows(i, _):
        r = pl.ds(pl.multiple_of(i * 16, 16), 16)
        out[r, :] = (hid[r, :].astype(F32) + y_in[r, :] + bo_ref[...]).astype(BF16)
        return 0

    lax.fori_loop(0, B // 32, rows, 0, unroll=2)
    load_lens.wait()
    first = lax.axis_index("sq") * T
    n = B - AB
    copies = []

    def put(lo, hi):
        insert_rows(lens, first, kv, (held.at[pl.ds(0, n)], held.at[pl.ds(n, n)]), lo, hi, AB)
        for e, dst in enumerate((ko_hbm, vo_hbm)):
            copies.append(pltpu.make_async_copy(held.at[pl.ds(e * n + lo - AB, hi - lo)], dst.at[pl.ds(lo, hi - lo)], sem.at[len(copies)]))
            copies[-1].start()

    put(64, 80)
    put(80, 96)
    put(96, 128)
    lax.fori_loop(B // 32, B // 16, rows, 0, unroll=2)
    store_out = pltpu.make_async_copy(out, out_hbm, osem)
    store_out.start()
    put(128, 192)
    put(192, 256)
    store_out.wait()
    for cp in copies:
        cp.wait()


def solution(mesh):
    def local_step(hidden, cache_lens, k_cache, v_cache, ln_gain, ln_bias, w_query, b_query, w_kv, b_kv, w_out, b_out):
        hbm = pl.BlockSpec(memory_space=pltpu.HBM)
        vm = pl.BlockSpec(memory_space=pltpu.VMEM)
        smem = pl.BlockSpec(memory_space=pltpu.SMEM)
        sem = pltpu.SemaphoreType.DMA

        def pin(*arrays):
            return [pltpu.with_memory_space_constraint(a, pltpu.VMEM) for a in arrays]

        def far(*arrays):
            return [pltpu.with_memory_space_constraint(a, pltpu.HBM) for a in arrays]

        cache = jax.ShapeDtypeStruct((B, T, DH), BF16)
        q3, kv, o0, lse0, k_part, v_part = pl.pallas_call(
            first_kernel,
            out_shape=(pltpu.VMEM((B * H, DH), F32), pltpu.VMEM((2 * B, DH), F32), pltpu.VMEM((AB * H, DH), F32), pltpu.VMEM((AB // CS * H, DH), F32), cache, cache),
            in_specs=[hbm] * 10,
            out_specs=(vm, vm, vm, vm, hbm, hbm),
            scratch_shapes=[
                pltpu.SMEM((B,), jnp.int32), pltpu.VMEM((1, D), F32), pltpu.VMEM((1, D), F32), pltpu.VMEM((1, H * DH), F32), pltpu.VMEM((1, 2 * DH), F32),
                pltpu.VMEM((B, D), BF16), pltpu.VMEM((B, DH), F32), pltpu.VMEM((B, DH), F32), pltpu.VMEM((D, H * DH), BF16), pltpu.VMEM((D, 2 * DH), BF16),
                pltpu.VMEM((AB, T, DH), BF16), pltpu.VMEM((AB, T, DH), BF16), *STAGE_BUFS, sem((NQ + 3,)), sem((4,)), sem((5,)),
            ],
            compiler_params=pltpu.CompilerParams(vmem_limit_bytes=33 * MIB),
            name="first",
        )(*far(cache_lens, hidden, k_cache, v_cache, ln_gain[None], ln_bias[None], w_query, b_query[None], w_kv, b_kv[None]))
        held = pltpu.VMEM((2 * (B - AB), T, DH), BF16)
        y, kv_held = pl.pallas_call(
            exchange_kernel,
            out_shape=(pltpu.VMEM((B, D), F32), held),
            in_specs=[hbm, vm, vm, vm, vm, hbm, hbm, hbm],
            out_specs=(vm, vm),
            scratch_shapes=[
                pltpu.SMEM((B,), jnp.int32),
                pltpu.VMEM((H * DH, DC), BF16), pltpu.VMEM((B * H, DH), F32), pltpu.VMEM((NC * H, DH), F32), *STAGE_BUFS,
                pltpu.VMEM((NC, 2, S * H, DH), F32), pltpu.VMEM((NC, H, DH), F32),
                pltpu.VMEM((NC, 2, S * H, DH), F32), pltpu.VMEM((NC, H, DH), F32), pltpu.VMEM((NC, H // 2, DH), F32),
                pltpu.VMEM((NC, S * H, DH), F32), pltpu.VMEM((NC, H // 2, DH), F32),
                pltpu.VMEM((NC, R * H, DH), F32), pltpu.VMEM((NC, R, DC), F32), pltpu.VMEM((NC, R, DY), F32),
                sem, sem((2 * (B // AB) - 2,)), sem, sem((NC, 3)), sem((NC, 3)), sem((NC, 2)), sem((NC, 2)), sem((NC,)), sem((NC,)),
                sem((NC,)), sem((NC,)), sem((NC, 4)), sem((NC, 4)), sem((NC, 4)), sem((NC, 4)),
            ],
            compiler_params=pltpu.CompilerParams(vmem_limit_bytes=24 * MIB, collective_id=0, has_side_effects=True),
            name="exchange",
        )(*far(cache_lens), *pin(q3, kv, o0, lse0), *far(k_cache, v_cache, w_out))
        k_new, v_new, out_hidden, _ = pl.pallas_call(
            last_kernel,
            out_shape=(cache, cache, jax.ShapeDtypeStruct((B, D), BF16), held),
            in_specs=[hbm, vm, vm, vm, vm, vm, hbm, hbm],
            out_specs=(hbm, hbm, hbm, vm),
            input_output_aliases={5: 3, 6: 0, 7: 1},
            scratch_shapes=[pltpu.SMEM((B,), jnp.int32), pltpu.VMEM((B, D), BF16), sem((10,)), sem],
            compiler_params=pltpu.CompilerParams(vmem_limit_bytes=6 * MIB),
            name="last",
        )(*far(cache_lens), *pin(kv, y), hidden, b_out[None], *pin(kv_held), k_part, v_part)
        return out_hidden, k_new, v_new

    cache_spec = P("dp", "sq", None)
    row_spec = P("dp", None)
    in_specs = (row_spec, P("dp"), cache_spec, cache_spec, P(None), P(None), P(None, "tp"), P("tp"), P(None, None), P(None), P("tp", None), P(None))
    out_specs = (row_spec, cache_spec, cache_spec)
    return jax.shard_map(local_step, mesh=mesh, in_specs=in_specs, out_specs=out_specs, check_vma=False)
```

```python
import functools
import math

import jax
import jax.numpy as jnp
from jax import lax
from jax.experimental import pallas as pl
from jax.experimental.pallas import tpu as pltpu
from jax.sharding import PartitionSpec as P

MESH = pl.DeviceIdType.MESH
F32 = jnp.float32
BF16 = jnp.bfloat16
NEG = -1e30
B = 256
D = 4096
H = 16
DH = 128
T = 256
AB = 64
NC = 4
CS = B // NC
S = CS // 4
R = 2 * S
DC = D // 2
DY = DC // 2
QB = 512
NQ = H * DH // QB
QSCALE = DH ** -0.5 * math.log2(math.e)
GROUP = 8
MIB = 1024 * 1024
VIA_Y = 384
SCHEDULE = [(s[0], int(s[1])) for s in (
    "s0", "a1", "s1", "m0", "a2", "s2", "m1", "m2", "q0", "a3", "s3", "q1", "p0", "m3", "p1", "q2", "f0", "q3", "p2", "p3", "f1", "f2", "f3", "r0", "r1", "r2", "r3", "l0", "l1", "l2", "l3")]

def attention_stages(lens, first, q3, kbuf, vbuf, base, vbase, kv, o_ref, lse_ref, bufs):
    lane = lax.broadcasted_iota(jnp.int32, (H, DH), 1)
    pos = lax.broadcasted_iota(jnp.int32, (H, T), 1)
    zero = jnp.zeros((H, DH), BF16)
    s_a, s_b, p_a, p_b, r_a, r_b, n_a, n_b = bufs

    def score(i, s_out):
        for u in range(0, GROUP, 2):
            b = i * GROUP + u
            q0 = q3[pl.ds(pl.multiple_of(b * H, H), H), :].astype(BF16)
            q1 = q3[pl.ds(pl.multiple_of(b * H + H, H), H), :].astype(BF16)
            lhs = jnp.concatenate([jnp.concatenate([q0, zero], 1), jnp.concatenate([zero, q1], 1)], 0)
            keys = jnp.concatenate([kbuf[b - base], kbuf[b + 1 - base]], 1)
            s_out[u * H:(u + 2) * H, :] = lax.dot_general(lhs, keys, (((1,), (1,)), ((), ())), preferred_element_type=F32)

    def soften(i, s_in, p_out, r_out, n_out):
        chunk = lax.div(i * GROUP, CS)
        tile = pl.ds(pl.multiple_of(chunk * H, H), H)
        at = i * GROUP - chunk * CS
        lses = lse_ref[tile, :]
        for u in range(GROUP):
            b = i * GROUP + u
            row = lens[b] - first
            here = jnp.logical_and(row >= 0, row < T)
            k_new = kv[pl.ds(b, 1), :]
            v_new = kv[pl.ds(B + b, 1), :]
            q_row = q3[pl.ds(pl.multiple_of(b * H, H), H), :]
            s_new = jnp.where(here, jnp.sum(q_row * k_new, axis=1, keepdims=True) * QSCALE, NEG)
            se = jnp.where(pos < row, s_in[u * H:(u + 1) * H, :] * QSCALE, NEG)
            m = jnp.maximum(jnp.max(se, axis=1, keepdims=True), s_new)
            p = jnp.exp2(se - m)
            p_new = jnp.exp2(s_new - m)
            l = jnp.sum(p, axis=1, keepdims=True) + p_new
            r = 1.0 / l
            p_out[u * H:(u + 1) * H, :] = p.astype(BF16)
            r_out[u * H:(u + 1) * H, :] = jnp.broadcast_to(r, (H, DH))
            n_out[u * H:(u + 1) * H, :] = (p_new * r) * v_new
            lses = jnp.where(lane == at + u, m + jnp.log2(l), lses)
        lse_ref[tile, :] = lses

    def weigh(i, p_in, r_in, n_in):
        for u in range(0, GROUP, 2):
            b = i * GROUP + u
            vals = jnp.concatenate([vbuf[b - vbase], vbuf[b + 1 - vbase]], 1)
            o = jnp.dot(p_in[u * H:(u + 2) * H, :], vals, preferred_element_type=F32)
            for e in range(2):
                part = slice((u + e) * H, (u + e + 1) * H)
                o_ref[pl.ds(pl.multiple_of((b + e) * H, H), H), :] = (
                    o[e * H:(e + 1) * H, e * DH:(e + 1) * DH] * r_in[part, :] + n_in[part, :])

    def attend(k):
        tiles = slice(k * AB // CS * H, (k + 1) * AB // CS * H)
        lse_ref[tiles, :] = jnp.zeros((AB // CS * H, DH), F32)
        lo, hi = k * AB // GROUP, (k + 1) * AB // GROUP
        score(lo, s_a)
        score(lo + 1, s_b)
        soften(lo, s_a, p_a, r_a, n_a)

        def body(t):
            i = lo + 2 + 2 * t
            score(i, s_a)
            soften(i - 1, s_b, p_b, r_b, n_b)
            weigh(i - 2, p_a, r_a, n_a)
            score(i + 1, s_b)
            soften(i, s_a, p_a, r_a, n_a)
            weigh(i - 1, p_b, r_b, n_b)

        for t in range((hi - lo - 2) // 2):
            body(t)
        soften(hi - 1, s_b, p_b, r_b, n_b)
        weigh(hi - 2, p_a, r_a, n_a)
        weigh(hi - 1, p_b, r_b, n_b)

    return attend


STAGE_BUFS = [pltpu.VMEM((GROUP * H, T), F32)] * 2 + [pltpu.VMEM((GROUP * H, T), BF16)] * 2 + [pltpu.VMEM((GROUP * H, DH), F32)] * 4


def insert_rows(lens, first, kv, pairs, lo, hi, base):
    sub = lax.broadcasted_iota(jnp.int32, (16, DH), 0)

    def insert(b, _):
        row = lens[b] - first
        start = pl.multiple_of((jnp.clip(row, 0, T - 1) // 16) * 16, 16)
        hit = sub == row - start
        for c, buf in enumerate(pairs):
            new = kv[pl.ds(c * B + b, 1), :]
            old = buf[b - base, pl.ds(start, 16), :].astype(F32)
            buf[b - base, pl.ds(start, 16), :] = jnp.where(hit, new, old).astype(BF16)
        return 0

    lax.fori_loop(lo, hi, insert, 0, unroll=4)


def first_kernel(lens_hbm, hid_hbm, k_hbm, v_hbm, gain_hbm, bias_hbm, wq_hbm, bq_hbm, wkv_hbm, bkv_hbm,
                 q3, kv, o_ref, lse_ref, ko_hbm, vo_hbm,
                 lens, gain_ref, bias_ref, bq_ref, bkv_ref, h, mean_ref, rstd_ref, wq, wkv, kbuf, vbuf, b0, b1, b2, b3, b4, b5, b6, b7, wsem, csem, ssem):
    first = lax.axis_index("sq") * T
    small = [pltpu.make_async_copy(src, dst, ssem.at[e]) for e, (src, dst) in enumerate((
        (gain_hbm, gain_ref), (bias_hbm, bias_ref), (bkv_hbm, bkv_ref), (bq_hbm, bq_ref), (lens_hbm, lens)))]
    load_h = []
    for e in range(2):
        rows = pl.ds(e * (B // 2), B // 2)
        load_h.append(pltpu.make_async_copy(hid_hbm.at[rows], h.at[rows], wsem.at[NQ + e]))
        load_h[-1].start()
        if e == 0:
            for cp in small:
                cp.start()
    load_wkv = pltpu.make_async_copy(wkv_hbm, wkv, wsem.at[NQ + 2])
    load_wkv.start()
    load_wq = []
    for j in range(NQ):
        cols = pl.ds(j * QB, QB)
        load_wq.append(pltpu.make_async_copy(wq_hbm.at[:, cols], wq.at[:, cols], wsem.at[j]))
    loads = [pltpu.make_async_copy(src.at[pl.ds(0, AB)], dst, csem.at[e]) for e, (src, dst) in enumerate(((k_hbm, kbuf), (v_hbm, vbuf)))]
    for cp in [*load_wq[:-1], *loads, load_wq[-1]]:
        cp.start()
    small[0].wait()
    small[1].wait()

    def spread(tile):
        return jnp.concatenate([tile] * (D // DH), 1)

    def block(i):
        return pl.ds(pl.multiple_of(i * 16, 16), 16)

    def means(i, _):
        total = jnp.sum(h[block(i), :].astype(F32), axis=-1, keepdims=True)
        mean_ref[block(i), :] = jnp.broadcast_to(total * (1.0 / D), (16, DH))
        return 0

    def scales(i, _):
        cen = h[block(i), :].astype(F32) - spread(mean_ref[block(i), :])
        var = jnp.sum(cen * cen, axis=-1, keepdims=True) * (1.0 / D)
        rstd_ref[block(i), :] = jnp.broadcast_to(lax.rsqrt(var + 1e-5), (16, DH))
        return 0

    def normed(i, _):
        y = (h[block(i), :].astype(F32) - spread(mean_ref[block(i), :])) * spread(rstd_ref[block(i), :])
        h[block(i), :] = (y * gain_ref[...] + bias_ref[...]).astype(BF16)
        return 0

    for e in range(2):
        load_h[e].wait()
        lo, hi = e * (B // 32), (e + 1) * (B // 32)
        lax.fori_loop(lo, hi, means, 0, unroll=4)
        lax.fori_loop(lo, hi, scales, 0, unroll=4)
        lax.fori_loop(lo, hi, normed, 0, unroll=2)
    load_wkv.wait()
    for cp in small[2:]:
        cp.wait()
    load_wq[0].wait()
    new_kv = (jnp.dot(h[...], wkv[...], preferred_element_type=F32) + bkv_ref[...]).astype(BF16).astype(F32)
    kv[0:B, :] = new_kv[:, :DH]
    kv[B:2 * B, :] = new_kv[:, DH:]
    stores = [pltpu.make_async_copy(src, dst.at[pl.ds(0, AB)], csem.at[2 + e]) for e, (src, dst) in enumerate(((kbuf, ko_hbm), (vbuf, vo_hbm)))]
    for j in range(NQ):
        cols = pl.ds(j * QB, QB)
        q = jnp.dot(h[...], wq[:, cols], preferred_element_type=F32) + bq_ref[:, cols]
        q = q.astype(BF16).astype(F32)
        if j < NQ - 2:
            load_wq[j + 1].wait()
        for n in range(QB // DH):
            q3[pl.ds(j * (QB // DH) + n, B, stride=H), :] = q[:, n * DH:(n + 1) * DH]
        if j == NQ - 2:
            for c in loads:
                c.wait()
            insert_rows(lens, first, kv, (kbuf, vbuf), 0, AB, 0)
            for c in stores:
                c.start()
            load_wq[j + 1].wait()
    attention_stages(lens, first, q3, kbuf, vbuf, 0, 0, kv, o_ref, lse_ref, (b0, b1, b2, b3, b4, b5, b6, b7))(0)
    for c in stores:
        c.wait()


def column(tile, j):
    return tile[:, j:j + 1]


def merge(la, lb):
    top = jnp.maximum(la, lb)
    wa, wb = jnp.exp2(la - top), jnp.exp2(lb - top)
    tot = wa + wb
    return wa / tot, wb / tot, top + jnp.log2(tot)


def exchange_kernel(lens_hbm, q3, kv, o_first, lse_first, k_hbm, v_hbm, wo_hbm, y_ref, held,
                    lens, wo, o_ref, lse_ref, b0, b1, b2, b3, b4, b5, b6, b7, o_core, l_core, o_mix, l_mix, l_half, o_x, l_x, a_all, part, p_y,
                    wsem, csem, nsem, a0s, a0r, a1s, a1r, a2s, a2r, bs, br, cs, cr, ds, dr):
    sq, tp = lax.axis_index("sq"), lax.axis_index("tp")
    x, c = sq // 2, sq % 2
    mate = {"sq": x * 2 + 1 - c}
    over_x = {"sq": (1 - x) * 2 + c}
    over_y = {"tp": 1 - tp}
    loads = {}
    bar = pltpu.get_barrier_semaphore()
    for dev in (mate, over_x, over_y):
        pl.semaphore_signal(bar, inc=1, device_id=dev, device_id_type=MESH)
    load_lens = pltpu.make_async_copy(lens_hbm, lens, nsem)
    load_lens.start()

    def fetch(k):
        rows = pl.ds(k * AB, AB)
        loads[k] = [pltpu.make_async_copy(src.at[rows], held.at[pl.ds((k - 1) * AB + e * (B - AB), AB)], csem.at[2 * k + e - 2])
                    for e, src in enumerate((k_hbm, v_hbm))]
        for cp in loads[k]:
            cp.start()

    fetch(1)
    fetch(2)
    load = pltpu.make_async_copy(wo_hbm.at[:, pl.ds(pl.multiple_of(c * DC, DC), DC)], wo, wsem)
    load.start()
    fetch(3)
    load_lens.wait()
    pl.semaphore_wait(bar, 3)

    def send(src, dst, ssem, rsem, dev):
        cp = pltpu.make_async_remote_copy(src, dst, ssem, rsem, device_id=dev, device_id_type=MESH)
        cp.start()
        return cp

    W = S * H
    hop0, hop1, hop2, hopb, hopc, hopd = {}, {}, {}, {}, {}, {}
    stages = attention_stages(lens, sq * T, q3, held, held, AB, AB - (B - AB), kv, o_ref, lse_ref, (b0, b1, b2, b3, b4, b5, b6, b7))
    ready = []
    lane8 = lax.broadcasted_iota(jnp.int32, (H // 2, DH), 1)

    def attend(k):
        block = k * CS // AB
        for cp in loads[block]:
            cp.wait()
        stages(block)

    def source(k):
        return (o_first, lse_first) if k * CS < AB else (o_ref, lse_ref)

    def rows_of_o(k, xx, cc):
        return pl.ds(pl.multiple_of((k * 4 + xx * 2 + cc) * W, W), W)

    def share(k):
        o_k, l_k = source(k)
        hop0[k] = [send(o_k.at[rows_of_o(k, xx, 1 - c)], o_core.at[k, xx], a0s.at[k, xx], a0r.at[k, xx], mate) for xx in range(2)]
        hop0[k].append(send(l_k.at[pl.ds(k * H, H)], l_core.at[k], a0s.at[k, 2], a0r.at[k, 2], mate))

    def mix(k):
        o_k, l_k = source(k)
        for cp in hop0[k]:
            cp.wait_recv()
        shift = lax.rem(DH - c * S, DH)
        fa, fb, lm = merge(pltpu.roll(l_k[pl.ds(k * H, H), :], shift, 1), pltpu.roll(l_core[k], shift, 1))
        l_mix[k] = lm
        theirs = pltpu.roll(lm, lax.rem(DH - (1 - x) * R, DH), 1)
        l_half[k] = jnp.where(lane8 < S, theirs[:H // 2], pltpu.roll(theirs[H // 2:], S, 1))
        for xx in range(2):
            mine = (k * 4 + xx * 2 + c) * W
            for j in range(S):
                oa = o_k[pl.ds(pl.multiple_of(mine + j * H, H), H), :]
                ob = o_core[k, xx, j * H:(j + 1) * H, :]
                at = xx * R + j
                o_mix[k, xx, j * H:(j + 1) * H, :] = column(fa, at) * oa + column(fb, at) * ob
        hop1[k] = [send(o_mix.at[k, 1 - x], o_x.at[k], a1s.at[k, 0], a1r.at[k, 0], over_x),
                   send(l_half.at[k], l_x.at[k], a1s.at[k, 1], a1r.at[k, 1], over_x)]

    def quarter(k):
        for cp in hop1[k]:
            cp.wait_recv()
        shift = lax.rem(DH - x * R, DH)
        l_far = jnp.concatenate([l_x[k], pltpu.roll(l_x[k], DH - S, 1)], 0)
        fa, fb, _ = merge(pltpu.roll(l_mix[k], shift, 1), l_far)
        for j in range(S):
            oa = o_mix[k, x, j * H:(j + 1) * H, :]
            ob = o_x[k, j * H:(j + 1) * H, :]
            a_all[k, pl.ds(pl.multiple_of(c * W + j * H, H), H), :] = column(fa, j) * oa + column(fb, j) * ob
        own = pl.ds(pl.multiple_of(c * W, W), W)
        hop2[k] = send(a_all.at[k, own], a_all.at[k, own], a2s.at[k], a2r.at[k], mate)

    def project(k):
        hop2[k].wait_recv()
        a = jnp.concatenate([a_all[k, pl.ds(n, R, stride=H), :].astype(BF16) for n in range(H)], 1)
        if not ready:
            load.wait()
            ready.append(1)
        part[k] = jnp.dot(a, wo[...], preferred_element_type=F32)
        hopb[k] = send(part.at[k, :, pl.ds(pl.multiple_of((1 - tp) * DY, DY), DY)], p_y.at[k], bs.at[k], br.at[k], over_y)

    def piece(k, xx, yy, lo=0, width=DY):
        return (pl.ds(pl.multiple_of(k * CS + xx * R, R), R), pl.ds(pl.multiple_of(c * DC + yy * DY + lo, 128), width))

    def pass_on(at, ssem, rsem, dev):
        return send(y_ref.at[at], y_ref.at[at], ssem, rsem, dev)

    def finish(k):
        hopb[k].wait_recv()
        at = piece(k, x, tp)
        y_ref[at] = part[k, :, pl.ds(pl.multiple_of(tp * DY, DY), DY)] + p_y[k]
        hopc[k] = [pass_on(at, cs.at[k, 0], cr.at[k, 0], over_x), pass_on(at, cs.at[k, 1], cr.at[k, 1], over_y)]
        hopd[k] = [pass_on(at, ds.at[k, 0], dr.at[k, 0], mate)]

    def relay(k):
        hopc[k][1].wait_recv()
        hopc[k].append(pass_on(piece(k, x, 1 - tp, VIA_Y, DY - VIA_Y), cs.at[k, 2], cr.at[k, 2], over_x))
        hopd[k].append(pass_on(piece(k, x, 1 - tp), ds.at[k, 1], dr.at[k, 1], mate))
        hopc[k][0].wait_recv()
        hopc[k].append(pass_on(piece(k, 1 - x, tp, 0, VIA_Y), cs.at[k, 3], cr.at[k, 3], over_y))
        hopd[k].append(pass_on(piece(k, 1 - x, tp), ds.at[k, 2], dr.at[k, 2], mate))

    def last(k):
        hopc[k][2].wait_recv()
        hopc[k][3].wait_recv()
        hopd[k].append(pass_on(piece(k, 1 - x, 1 - tp), ds.at[k, 3], dr.at[k, 3], mate))

    for step, k in SCHEDULE:
        {"a": attend, "s": share, "m": mix, "q": quarter, "p": project, "f": finish, "r": relay, "l": last}[step](k)
    for k in range(NC):
        for cp in hopd[k]:
            cp.wait_recv()
    for k in range(NC):
        for cp in [*hop0[k], *hop1[k], hop2[k], hopb[k], *hopc[k], *hopd[k]]:
            cp.wait_send()


def last_kernel(lens_hbm, kv, y_in, hid, bo_ref, held_in, k_part, v_part, ko_hbm, vo_hbm, out_hbm, held, lens, out, sem, osem):
    load_lens = pltpu.make_async_copy(lens_hbm, lens, osem)
    load_lens.start()

    def rows(i, _):
        r = pl.ds(pl.multiple_of(i * 16, 16), 16)
        out[r, :] = (hid[r, :].astype(F32) + y_in[r, :] + bo_ref[...]).astype(BF16)
        return 0

    lax.fori_loop(0, B // 32, rows, 0, unroll=2)
    load_lens.wait()
    first = lax.axis_index("sq") * T
    n = B - AB
    copies = []

    def put(lo, hi):
        insert_rows(lens, first, kv, (held.at[pl.ds(0, n)], held.at[pl.ds(n, n)]), lo, hi, AB)
        for e, dst in enumerate((ko_hbm, vo_hbm)):
            copies.append(pltpu.make_async_copy(held.at[pl.ds(e * n + lo - AB, hi - lo)], dst.at[pl.ds(lo, hi - lo)], sem.at[len(copies)]))
            copies[-1].start()

    put(64, 80)
    put(80, 96)
    put(96, 128)
    lax.fori_loop(B // 32, B // 16, rows, 0, unroll=2)
    store_out = pltpu.make_async_copy(out, out_hbm, osem)
    store_out.start()
    put(128, 192)
    put(192, 256)
    store_out.wait()
    for cp in copies:
        cp.wait()


def solution(mesh):
    def local_step(hidden, cache_lens, k_cache, v_cache, ln_gain, ln_bias, w_query, b_query, w_kv, b_kv, w_out, b_out):
        hbm = pl.BlockSpec(memory_space=pltpu.HBM)
        vm = pl.BlockSpec(memory_space=pltpu.VMEM)
        smem = pl.BlockSpec(memory_space=pltpu.SMEM)
        sem = pltpu.SemaphoreType.DMA

        def pin(*arrays):
            return [pltpu.with_memory_space_constraint(a, pltpu.VMEM) for a in arrays]

        def far(*arrays):
            return [pltpu.with_memory_space_constraint(a, pltpu.HBM) for a in arrays]

        cache = jax.ShapeDtypeStruct((B, T, DH), BF16)
        q3, kv, o0, lse0, k_part, v_part = pl.pallas_call(
            first_kernel,
            out_shape=(pltpu.VMEM((B * H, DH), F32), pltpu.VMEM((2 * B, DH), F32), pltpu.VMEM((AB * H, DH), F32), pltpu.VMEM((AB // CS * H, DH), F32), cache, cache),
            in_specs=[hbm] * 10,
            out_specs=(vm, vm, vm, vm, hbm, hbm),
            scratch_shapes=[
                pltpu.SMEM((B,), jnp.int32), pltpu.VMEM((1, D), F32), pltpu.VMEM((1, D), F32), pltpu.VMEM((1, H * DH), F32), pltpu.VMEM((1, 2 * DH), F32),
                pltpu.VMEM((B, D), BF16), pltpu.VMEM((B, DH), F32), pltpu.VMEM((B, DH), F32), pltpu.VMEM((D, H * DH), BF16), pltpu.VMEM((D, 2 * DH), BF16),
                pltpu.VMEM((AB, T, DH), BF16), pltpu.VMEM((AB, T, DH), BF16), *STAGE_BUFS, sem((NQ + 3,)), sem((4,)), sem((5,)),
            ],
            compiler_params=pltpu.CompilerParams(vmem_limit_bytes=33 * MIB),
            name="first",
        )(*far(cache_lens, hidden, k_cache, v_cache, ln_gain[None], ln_bias[None], w_query, b_query[None], w_kv, b_kv[None]))
        held = pltpu.VMEM((2 * (B - AB), T, DH), BF16)
        y, kv_held = pl.pallas_call(
            exchange_kernel,
            out_shape=(pltpu.VMEM((B, D), F32), held),
            in_specs=[hbm, vm, vm, vm, vm, hbm, hbm, hbm],
            out_specs=(vm, vm),
            scratch_shapes=[
                pltpu.SMEM((B,), jnp.int32),
                pltpu.VMEM((H * DH, DC), BF16), pltpu.VMEM((B * H, DH), F32), pltpu.VMEM((NC * H, DH), F32), *STAGE_BUFS,
                pltpu.VMEM((NC, 2, S * H, DH), F32), pltpu.VMEM((NC, H, DH), F32),
                pltpu.VMEM((NC, 2, S * H, DH), F32), pltpu.VMEM((NC, H, DH), F32), pltpu.VMEM((NC, H // 2, DH), F32),
                pltpu.VMEM((NC, S * H, DH), F32), pltpu.VMEM((NC, H // 2, DH), F32),
                pltpu.VMEM((NC, R * H, DH), F32), pltpu.VMEM((NC, R, DC), F32), pltpu.VMEM((NC, R, DY), F32),
                sem, sem((2 * (B // AB) - 2,)), sem, sem((NC, 3)), sem((NC, 3)), sem((NC, 2)), sem((NC, 2)), sem((NC,)), sem((NC,)),
                sem((NC,)), sem((NC,)), sem((NC, 4)), sem((NC, 4)), sem((NC, 4)), sem((NC, 4)),
            ],
            compiler_params=pltpu.CompilerParams(vmem_limit_bytes=24 * MIB, collective_id=0, has_side_effects=True),
            name="exchange",
        )(*far(cache_lens), *pin(q3, kv, o0, lse0), *far(k_cache, v_cache, w_out))
        k_new, v_new, out_hidden, _ = pl.pallas_call(
            last_kernel,
            out_shape=(cache, cache, jax.ShapeDtypeStruct((B, D), BF16), held),
            in_specs=[hbm, vm, vm, vm, vm, vm, hbm, hbm],
            out_specs=(hbm, hbm, hbm, vm),
            input_output_aliases={5: 3, 6: 0, 7: 1},
            scratch_shapes=[pltpu.SMEM((B,), jnp.int32), pltpu.VMEM((B, D), BF16), sem((10,)), sem],
            compiler_params=pltpu.CompilerParams(vmem_limit_bytes=6 * MIB),
            name="last",
        )(*far(cache_lens), *pin(kv, y), hidden, b_out[None], *pin(kv_held), k_part, v_part)
        return out_hidden, k_new, v_new

    cache_spec = P("dp", "sq", None)
    row_spec = P("dp", None)
    in_specs = (row_spec, P("dp"), cache_spec, cache_spec, P(None), P(None), P(None, "tp"), P("tp"), P(None, None), P(None), P("tp", None), P(None))
    out_specs = (row_spec, cache_spec, cache_spec)
    return jax.shard_map(local_step, mesh=mesh, in_specs=in_specs, out_specs=out_specs, check_vma=False)
```

```python
import functools
import math

import jax
import jax.numpy as jnp
from jax import lax
from jax.experimental import pallas as pl
from jax.experimental.pallas import tpu as pltpu
from jax.sharding import PartitionSpec as P

MESH = pl.DeviceIdType.MESH
F32 = jnp.float32
BF16 = jnp.bfloat16
NEG = -1e30
B = 256
D = 4096
H = 16
DH = 128
T = 256
AB = 64
NC = 8
CS = B // NC
S = CS // 4
R = 2 * S
DC = D // 2
DY = DC // 2
QB = 512
NQ = H * DH // QB
QSCALE = DH ** -0.5 * math.log2(math.e)
GROUP = 8
MIB = 1024 * 1024
VIA_Y = 128
SCHEDULE = [(s[0], int(s[1])) for s in (
    "s0", "s1", "m0", "a2", "m1", "s2", "s3", "a4", "s4", "s5", "m2", "m3", "q0", "m4", "q1", "m5", "p0", "p1", "q2", "a6", "f0", "q3", "s6", "s7", "q4", "f1", "p2", "m6", "m7", "p3", "r0", "p4", "f2", "q5", "q6", "q7", "f3", "r1", "p5", "f4", "r2", "p6", "l0", "l1", "r3", "p7", "f5", "r4", "f6", "f7", "l2", "r5", "l3", "l4", "r6", "r7", "l5", "l6", "l7")]

def attention_stages(lens, first, q3, kbuf, vbuf, base, vbase, kv, o_ref, lse_ref, bufs):
    lane = lax.broadcasted_iota(jnp.int32, (H, DH), 1)
    pos = lax.broadcasted_iota(jnp.int32, (H, T), 1)
    zero = jnp.zeros((H, DH), BF16)
    s_a, s_b, p_a, p_b, r_a, r_b, n_a, n_b = bufs

    def score(i, s_out):
        for u in range(0, GROUP, 2):
            b = i * GROUP + u
            q0 = q3[pl.ds(pl.multiple_of(b * H, H), H), :].astype(BF16)
            q1 = q3[pl.ds(pl.multiple_of(b * H + H, H), H), :].astype(BF16)
            lhs = jnp.concatenate([jnp.concatenate([q0, zero], 1), jnp.concatenate([zero, q1], 1)], 0)
            keys = jnp.concatenate([kbuf[b - base], kbuf[b + 1 - base]], 1)
            s_out[u * H:(u + 2) * H, :] = lax.dot_general(lhs, keys, (((1,), (1,)), ((), ())), preferred_element_type=F32)

    def soften(i, s_in, p_out, r_out, n_out):
        chunk = lax.div(i * GROUP, CS)
        tile = pl.ds(pl.multiple_of(chunk * H, H), H)
        at = i * GROUP - chunk * CS
        lses = lse_ref[tile, :]
        for u in range(GROUP):
            b = i * GROUP + u
            row = lens[b] - first
            here = jnp.logical_and(row >= 0, row < T)
            k_new = kv[pl.ds(b, 1), :]
            v_new = kv[pl.ds(B + b, 1), :]
            q_row = q3[pl.ds(pl.multiple_of(b * H, H), H), :]
            s_new = jnp.where(here, jnp.sum(q_row * k_new, axis=1, keepdims=True) * QSCALE, NEG)
            se = jnp.where(pos < row, s_in[u * H:(u + 1) * H, :] * QSCALE, NEG)
            m = jnp.maximum(jnp.max(se, axis=1, keepdims=True), s_new)
            p = jnp.exp2(se - m)
            p_new = jnp.exp2(s_new - m)
            l = jnp.sum(p, axis=1, keepdims=True) + p_new
            r = 1.0 / l
            p_out[u * H:(u + 1) * H, :] = p.astype(BF16)
            r_out[u * H:(u + 1) * H, :] = jnp.broadcast_to(r, (H, DH))
            n_out[u * H:(u + 1) * H, :] = (p_new * r) * v_new
            lses = jnp.where(lane == at + u, m + jnp.log2(l), lses)
        lse_ref[tile, :] = lses

    def weigh(i, p_in, r_in, n_in):
        for u in range(0, GROUP, 2):
            b = i * GROUP + u
            vals = jnp.concatenate([vbuf[b - vbase], vbuf[b + 1 - vbase]], 1)
            o = jnp.dot(p_in[u * H:(u + 2) * H, :], vals, preferred_element_type=F32)
            for e in range(2):
                part = slice((u + e) * H, (u + e + 1) * H)
                o_ref[pl.ds(pl.multiple_of((b + e) * H, H), H), :] = (
                    o[e * H:(e + 1) * H, e * DH:(e + 1) * DH] * r_in[part, :] + n_in[part, :])

    def attend(k):
        tiles = slice(k * AB // CS * H, (k + 1) * AB // CS * H)
        lse_ref[tiles, :] = jnp.zeros((AB // CS * H, DH), F32)
        lo, hi = k * AB // GROUP, (k + 1) * AB // GROUP
        score(lo, s_a)
        score(lo + 1, s_b)
        soften(lo, s_a, p_a, r_a, n_a)

        def body(t):
            i = lo + 2 + 2 * t
            score(i, s_a)
            soften(i - 1, s_b, p_b, r_b, n_b)
            weigh(i - 2, p_a, r_a, n_a)
            score(i + 1, s_b)
            soften(i, s_a, p_a, r_a, n_a)
            weigh(i - 1, p_b, r_b, n_b)

        for t in range((hi - lo - 2) // 2):
            body(t)
        soften(hi - 1, s_b, p_b, r_b, n_b)
        weigh(hi - 2, p_a, r_a, n_a)
        weigh(hi - 1, p_b, r_b, n_b)

    return attend


STAGE_BUFS = [pltpu.VMEM((GROUP * H, T), F32)] * 2 + [pltpu.VMEM((GROUP * H, T), BF16)] * 2 + [pltpu.VMEM((GROUP * H, DH), F32)] * 4


def insert_rows(lens, first, kv, pairs, lo, hi, base):
    sub = lax.broadcasted_iota(jnp.int32, (16, DH), 0)

    def insert(b, _):
        row = lens[b] - first
        start = pl.multiple_of((jnp.clip(row, 0, T - 1) // 16) * 16, 16)
        hit = sub == row - start
        for c, buf in enumerate(pairs):
            new = kv[pl.ds(c * B + b, 1), :]
            old = buf[b - base, pl.ds(start, 16), :].astype(F32)
            buf[b - base, pl.ds(start, 16), :] = jnp.where(hit, new, old).astype(BF16)
        return 0

    lax.fori_loop(lo, hi, insert, 0, unroll=4)


def first_kernel(lens_hbm, hid_hbm, k_hbm, v_hbm, gain_hbm, bias_hbm, wq_hbm, bq_hbm, wkv_hbm, bkv_hbm,
                 q3, kv, o_ref, lse_ref, ko_hbm, vo_hbm,
                 lens, gain_ref, bias_ref, bq_ref, bkv_ref, h, mean_ref, rstd_ref, wq, wkv, kbuf, vbuf, b0, b1, b2, b3, b4, b5, b6, b7, wsem, csem, ssem):
    first = lax.axis_index("sq") * T
    small = [pltpu.make_async_copy(src, dst, ssem.at[e]) for e, (src, dst) in enumerate((
        (gain_hbm, gain_ref), (bias_hbm, bias_ref), (bkv_hbm, bkv_ref), (bq_hbm, bq_ref), (lens_hbm, lens)))]
    load_h = []
    for e in range(2):
        rows = pl.ds(e * (B // 2), B // 2)
        load_h.append(pltpu.make_async_copy(hid_hbm.at[rows], h.at[rows], wsem.at[NQ + e]))
        load_h[-1].start()
        if e == 0:
            for cp in small:
                cp.start()
    load_wkv = pltpu.make_async_copy(wkv_hbm, wkv, wsem.at[NQ + 2])
    load_wkv.start()
    load_wq = []
    for j in range(NQ):
        cols = pl.ds(j * QB, QB)
        load_wq.append(pltpu.make_async_copy(wq_hbm.at[:, cols], wq.at[:, cols], wsem.at[j]))
    loads = [pltpu.make_async_copy(src.at[pl.ds(0, AB)], dst, csem.at[e]) for e, (src, dst) in enumerate(((k_hbm, kbuf), (v_hbm, vbuf)))]
    for cp in [*load_wq[:-1], *loads, load_wq[-1]]:
        cp.start()
    small[0].wait()
    small[1].wait()

    def spread(tile):
        return jnp.concatenate([tile] * (D // DH), 1)

    def block(i):
        return pl.ds(pl.multiple_of(i * 16, 16), 16)

    def means(i, _):
        total = jnp.sum(h[block(i), :].astype(F32), axis=-1, keepdims=True)
        mean_ref[block(i), :] = jnp.broadcast_to(total * (1.0 / D), (16, DH))
        return 0

    def scales(i, _):
        cen = h[block(i), :].astype(F32) - spread(mean_ref[block(i), :])
        var = jnp.sum(cen * cen, axis=-1, keepdims=True) * (1.0 / D)
        rstd_ref[block(i), :] = jnp.broadcast_to(lax.rsqrt(var + 1e-5), (16, DH))
        return 0

    def normed(i, _):
        y = (h[block(i), :].astype(F32) - spread(mean_ref[block(i), :])) * spread(rstd_ref[block(i), :])
        h[block(i), :] = (y * gain_ref[...] + bias_ref[...]).astype(BF16)
        return 0

    for e in range(2):
        load_h[e].wait()
        lo, hi = e * (B // 32), (e + 1) * (B // 32)
        lax.fori_loop(lo, hi, means, 0, unroll=4)
        lax.fori_loop(lo, hi, scales, 0, unroll=4)
        lax.fori_loop(lo, hi, normed, 0, unroll=2)
    load_wkv.wait()
    for cp in small[2:]:
        cp.wait()
    load_wq[0].wait()
    new_kv = (jnp.dot(h[...], wkv[...], preferred_element_type=F32) + bkv_ref[...]).astype(BF16).astype(F32)
    kv[0:B, :] = new_kv[:, :DH]
    kv[B:2 * B, :] = new_kv[:, DH:]
    stores = [pltpu.make_async_copy(src, dst.at[pl.ds(0, AB)], csem.at[2 + e]) for e, (src, dst) in enumerate(((kbuf, ko_hbm), (vbuf, vo_hbm)))]
    for j in range(NQ):
        cols = pl.ds(j * QB, QB)
        q = jnp.dot(h[...], wq[:, cols], preferred_element_type=F32) + bq_ref[:, cols]
        q = q.astype(BF16).astype(F32)
        if j < NQ - 2:
            load_wq[j + 1].wait()
        for n in range(QB // DH):
            q3[pl.ds(j * (QB // DH) + n, B, stride=H), :] = q[:, n * DH:(n + 1) * DH]
        if j == NQ - 2:
            for c in loads:
                c.wait()
            insert_rows(lens, first, kv, (kbuf, vbuf), 0, AB, 0)
            for c in stores:
                c.start()
            load_wq[j + 1].wait()
    attention_stages(lens, first, q3, kbuf, vbuf, 0, 0, kv, o_ref, lse_ref, (b0, b1, b2, b3, b4, b5, b6, b7))(0)
    for c in stores:
        c.wait()


def column(tile, j):
    return tile[:, j:j + 1]


def merge(la, lb):
    top = jnp.maximum(la, lb)
    wa, wb = jnp.exp2(la - top), jnp.exp2(lb - top)
    tot = wa + wb
    return wa / tot, wb / tot, top + jnp.log2(tot)


def exchange_kernel(lens_hbm, q3, kv, o_first, lse_first, k_hbm, v_hbm, wo_hbm, y_ref, held,
                    lens, wo, o_ref, lse_ref, b0, b1, b2, b3, b4, b5, b6, b7, o_core, l_core, o_mix, l_mix, l_half, o_x, l_x, a_all, part, p_y,
                    wsem, csem, nsem, a0s, a0r, a1s, a1r, a2s, a2r, bs, br, cs, cr, ds, dr):
    sq, tp = lax.axis_index("sq"), lax.axis_index("tp")
    x, c = sq // 2, sq % 2
    mate = {"sq": x * 2 + 1 - c}
    over_x = {"sq": (1 - x) * 2 + c}
    over_y = {"tp": 1 - tp}
    loads = {}
    bar = pltpu.get_barrier_semaphore()
    for dev in (mate, over_x, over_y):
        pl.semaphore_signal(bar, inc=1, device_id=dev, device_id_type=MESH)
    load_lens = pltpu.make_async_copy(lens_hbm, lens, nsem)
    load_lens.start()

    def fetch(k):
        rows = pl.ds(k * AB, AB)
        loads[k] = [pltpu.make_async_copy(src.at[rows], held.at[pl.ds((k - 1) * AB + e * (B - AB), AB)], csem.at[2 * k + e - 2])
                    for e, src in enumerate((k_hbm, v_hbm))]
        for cp in loads[k]:
            cp.start()

    fetch(1)
    fetch(2)
    load = pltpu.make_async_copy(wo_hbm.at[:, pl.ds(pl.multiple_of(c * DC, DC), DC)], wo, wsem)
    load.start()
    fetch(3)
    load_lens.wait()
    pl.semaphore_wait(bar, 3)

    def send(src, dst, ssem, rsem, dev):
        cp = pltpu.make_async_remote_copy(src, dst, ssem, rsem, device_id=dev, device_id_type=MESH)
        cp.start()
        return cp

    W = S * H
    hop0, hop1, hop2, hopb, hopc, hopd = {}, {}, {}, {}, {}, {}
    stages = attention_stages(lens, sq * T, q3, held, held, AB, AB - (B - AB), kv, o_ref, lse_ref, (b0, b1, b2, b3, b4, b5, b6, b7))
    ready = []
    lane8 = lax.broadcasted_iota(jnp.int32, (H // 2, DH), 1)

    def attend(k):
        block = k * CS // AB
        for cp in loads[block]:
            cp.wait()
        stages(block)

    def source(k):
        return (o_first, lse_first) if k * CS < AB else (o_ref, lse_ref)

    def rows_of_o(k, xx, cc):
        return pl.ds(pl.multiple_of((k * 4 + xx * 2 + cc) * W, W), W)

    def share(k):
        o_k, l_k = source(k)
        hop0[k] = [send(o_k.at[rows_of_o(k, xx, 1 - c)], o_core.at[k, xx], a0s.at[k, xx], a0r.at[k, xx], mate) for xx in range(2)]
        hop0[k].append(send(l_k.at[pl.ds(k * H, H)], l_core.at[k], a0s.at[k, 2], a0r.at[k, 2], mate))

    def mix(k):
        o_k, l_k = source(k)
        for cp in hop0[k]:
            cp.wait_recv()
        shift = lax.rem(DH - c * S, DH)
        fa, fb, lm = merge(pltpu.roll(l_k[pl.ds(k * H, H), :], shift, 1), pltpu.roll(l_core[k], shift, 1))
        l_mix[k] = lm
        theirs = pltpu.roll(lm, lax.rem(DH - (1 - x) * R, DH), 1)
        l_half[k] = jnp.where(lane8 < S, theirs[:H // 2], pltpu.roll(theirs[H // 2:], S, 1))
        for xx in range(2):
            mine = (k * 4 + xx * 2 + c) * W
            for j in range(S):
                oa = o_k[pl.ds(pl.multiple_of(mine + j * H, H), H), :]
                ob = o_core[k, xx, j * H:(j + 1) * H, :]
                at = xx * R + j
                o_mix[k, xx, j * H:(j + 1) * H, :] = column(fa, at) * oa + column(fb, at) * ob
        hop1[k] = [send(o_mix.at[k, 1 - x], o_x.at[k], a1s.at[k, 0], a1r.at[k, 0], over_x),
                   send(l_half.at[k], l_x.at[k], a1s.at[k, 1], a1r.at[k, 1], over_x)]

    def quarter(k):
        for cp in hop1[k]:
            cp.wait_recv()
        shift = lax.rem(DH - x * R, DH)
        l_far = jnp.concatenate([l_x[k], pltpu.roll(l_x[k], DH - S, 1)], 0)
        fa, fb, _ = merge(pltpu.roll(l_mix[k], shift, 1), l_far)
        for j in range(S):
            oa = o_mix[k, x, j * H:(j + 1) * H, :]
            ob = o_x[k, j * H:(j + 1) * H, :]
            a_all[k, pl.ds(pl.multiple_of(c * W + j * H, H), H), :] = column(fa, j) * oa + column(fb, j) * ob
        own = pl.ds(pl.multiple_of(c * W, W), W)
        hop2[k] = send(a_all.at[k, own], a_all.at[k, own], a2s.at[k], a2r.at[k], mate)

    def project(k):
        hop2[k].wait_recv()
        a = jnp.concatenate([a_all[k, pl.ds(n, R, stride=H), :].astype(BF16) for n in range(H)], 1)
        if not ready:
            load.wait()
            ready.append(1)
        theirs, ours = (pl.ds(pl.multiple_of(t * DY, DY), DY) for t in (1 - tp, tp))
        part[k, :, theirs] = jnp.dot(a, wo[:, theirs], preferred_element_type=F32)
        hopb[k] = send(part.at[k, :, theirs], p_y.at[k], bs.at[k], br.at[k], over_y)
        part[k, :, ours] = jnp.dot(a, wo[:, ours], preferred_element_type=F32)

    def piece(k, xx, yy, lo=0, width=DY):
        return (pl.ds(pl.multiple_of(k * CS + xx * R, R), R), pl.ds(pl.multiple_of(c * DC + yy * DY + lo, 128), width))

    def pass_on(at, ssem, rsem, dev):
        return send(y_ref.at[at], y_ref.at[at], ssem, rsem, dev)

    def finish(k):
        hopb[k].wait_recv()
        at = piece(k, x, tp)
        y_ref[at] = part[k, :, pl.ds(pl.multiple_of(tp * DY, DY), DY)] + p_y[k]
        hopc[k] = [pass_on(at, cs.at[k, 0], cr.at[k, 0], over_x), pass_on(at, cs.at[k, 1], cr.at[k, 1], over_y)]
        hopd[k] = [pass_on(at, ds.at[k, 0], dr.at[k, 0], mate)]

    def relay(k):
        hopc[k][1].wait_recv()
        hopc[k].append(pass_on(piece(k, x, 1 - tp, VIA_Y, DY - VIA_Y), cs.at[k, 2], cr.at[k, 2], over_x))
        hopd[k].append(pass_on(piece(k, x, 1 - tp), ds.at[k, 1], dr.at[k, 1], mate))
        hopc[k][0].wait_recv()
        hopc[k].append(pass_on(piece(k, 1 - x, tp, 0, VIA_Y), cs.at[k, 3], cr.at[k, 3], over_y))
        hopd[k].append(pass_on(piece(k, 1 - x, tp), ds.at[k, 2], dr.at[k, 2], mate))

    def last(k):
        hopc[k][2].wait_recv()
        hopc[k][3].wait_recv()
        hopd[k].append(pass_on(piece(k, 1 - x, 1 - tp), ds.at[k, 3], dr.at[k, 3], mate))

    for step, k in SCHEDULE:
        {"a": attend, "s": share, "m": mix, "q": quarter, "p": project, "f": finish, "r": relay, "l": last}[step](k)
    for k in range(NC):
        for cp in hopd[k]:
            cp.wait_recv()
    for k in range(NC):
        for cp in [*hop0[k], *hop1[k], hop2[k], hopb[k], *hopc[k], *hopd[k]]:
            cp.wait_send()


def last_kernel(lens_hbm, kv, y_in, hid, bo_ref, held_in, k_part, v_part, ko_hbm, vo_hbm, out_hbm, held, lens, out, sem, osem, nsem):
    load_lens = pltpu.make_async_copy(lens_hbm, lens, nsem)
    load_lens.start()

    def rows(i, _):
        r = pl.ds(pl.multiple_of(i * 16, 16), 16)
        out[r, :] = (hid[r, :].astype(F32) + y_in[r, :] + bo_ref[...]).astype(BF16)
        return 0

    half = B // 2
    store_out = []

    def finish_rows(e):
        lax.fori_loop(e * (B // 32), (e + 1) * (B // 32), rows, 0, unroll=2)
        store_out.append(pltpu.make_async_copy(out.at[pl.ds(e * half, half)], out_hbm.at[pl.ds(e * half, half)], osem.at[e]))
        store_out[-1].start()

    finish_rows(0)
    load_lens.wait()
    first = lax.axis_index("sq") * T
    n = B - AB
    copies = []

    def put(lo, hi):
        insert_rows(lens, first, kv, (held.at[pl.ds(0, n)], held.at[pl.ds(n, n)]), lo, hi, AB)
        for e, dst in enumerate((ko_hbm, vo_hbm)):
            copies.append(pltpu.make_async_copy(held.at[pl.ds(e * n + lo - AB, hi - lo)], dst.at[pl.ds(lo, hi - lo)], sem.at[len(copies)]))
            copies[-1].start()

    put(64, 80)
    put(80, 96)
    put(96, 128)
    finish_rows(1)
    put(128, 192)
    put(192, 256)
    for cp in store_out + copies:
        cp.wait()


def solution(mesh):
    def local_step(hidden, cache_lens, k_cache, v_cache, ln_gain, ln_bias, w_query, b_query, w_kv, b_kv, w_out, b_out):
        hbm = pl.BlockSpec(memory_space=pltpu.HBM)
        vm = pl.BlockSpec(memory_space=pltpu.VMEM)
        smem = pl.BlockSpec(memory_space=pltpu.SMEM)
        sem = pltpu.SemaphoreType.DMA

        def pin(*arrays):
            return [pltpu.with_memory_space_constraint(a, pltpu.VMEM) for a in arrays]

        def far(*arrays):
            return [pltpu.with_memory_space_constraint(a, pltpu.HBM) for a in arrays]

        cache = jax.ShapeDtypeStruct((B, T, DH), BF16)
        q3, kv, o0, lse0, k_part, v_part = pl.pallas_call(
            first_kernel,
            out_shape=(pltpu.VMEM((B * H, DH), F32), pltpu.VMEM((2 * B, DH), F32), pltpu.VMEM((AB * H, DH), F32), pltpu.VMEM((AB // CS * H, DH), F32), cache, cache),
            in_specs=[hbm] * 10,
            out_specs=(vm, vm, vm, vm, hbm, hbm),
            scratch_shapes=[
                pltpu.SMEM((B,), jnp.int32), pltpu.VMEM((1, D), F32), pltpu.VMEM((1, D), F32), pltpu.VMEM((1, H * DH), F32), pltpu.VMEM((1, 2 * DH), F32),
                pltpu.VMEM((B, D), BF16), pltpu.VMEM((B, DH), F32), pltpu.VMEM((B, DH), F32), pltpu.VMEM((D, H * DH), BF16), pltpu.VMEM((D, 2 * DH), BF16),
                pltpu.VMEM((AB, T, DH), BF16), pltpu.VMEM((AB, T, DH), BF16), *STAGE_BUFS, sem((NQ + 3,)), sem((4,)), sem((5,)),
            ],
            compiler_params=pltpu.CompilerParams(vmem_limit_bytes=33 * MIB),
            name="first",
        )(*far(cache_lens, hidden, k_cache, v_cache, ln_gain[None], ln_bias[None], w_query, b_query[None], w_kv, b_kv[None]))
        held = pltpu.VMEM((2 * (B - AB), T, DH), BF16)
        y, kv_held = pl.pallas_call(
            exchange_kernel,
            out_shape=(pltpu.VMEM((B, D), F32), held),
            in_specs=[hbm, vm, vm, vm, vm, hbm, hbm, hbm],
            out_specs=(vm, vm),
            scratch_shapes=[
                pltpu.SMEM((B,), jnp.int32),
                pltpu.VMEM((H * DH, DC), BF16), pltpu.VMEM((B * H, DH), F32), pltpu.VMEM((NC * H, DH), F32), *STAGE_BUFS,
                pltpu.VMEM((NC, 2, S * H, DH), F32), pltpu.VMEM((NC, H, DH), F32),
                pltpu.VMEM((NC, 2, S * H, DH), F32), pltpu.VMEM((NC, H, DH), F32), pltpu.VMEM((NC, H // 2, DH), F32),
                pltpu.VMEM((NC, S * H, DH), F32), pltpu.VMEM((NC, H // 2, DH), F32),
                pltpu.VMEM((NC, R * H, DH), F32), pltpu.VMEM((NC, R, DC), F32), pltpu.VMEM((NC, R, DY), F32),
                sem, sem((2 * (B // AB) - 2,)), sem, sem((NC, 3)), sem((NC, 3)), sem((NC, 2)), sem((NC, 2)), sem((NC,)), sem((NC,)),
                sem((NC,)), sem((NC,)), sem((NC, 4)), sem((NC, 4)), sem((NC, 4)), sem((NC, 4)),
            ],
            compiler_params=pltpu.CompilerParams(vmem_limit_bytes=24 * MIB, collective_id=0, has_side_effects=True),
            name="exchange",
        )(*far(cache_lens), *pin(q3, kv, o0, lse0), *far(k_cache, v_cache, w_out))
        k_new, v_new, out_hidden, _ = pl.pallas_call(
            last_kernel,
            out_shape=(cache, cache, jax.ShapeDtypeStruct((B, D), BF16), held),
            in_specs=[hbm, vm, vm, vm, vm, vm, hbm, hbm],
            out_specs=(hbm, hbm, hbm, vm),
            input_output_aliases={5: 3, 6: 0, 7: 1},
            scratch_shapes=[pltpu.SMEM((B,), jnp.int32), pltpu.VMEM((B, D), BF16), sem((10,)), sem((2,)), sem],
            compiler_params=pltpu.CompilerParams(vmem_limit_bytes=6 * MIB),
            name="last",
        )(*far(cache_lens), *pin(kv, y), hidden, b_out[None], *pin(kv_held), k_part, v_part)
        return out_hidden, k_new, v_new

    cache_spec = P("dp", "sq", None)
    row_spec = P("dp", None)
    in_specs = (row_spec, P("dp"), cache_spec, cache_spec, P(None), P(None), P(None, "tp"), P("tp"), P(None, None), P(None), P("tp", None), P(None))
    out_specs = (row_spec, cache_spec, cache_spec)
    return jax.shard_map(local_step, mesh=mesh, in_specs=in_specs, out_specs=out_specs, check_vma=False)
```

```python
import functools
import math

import jax
import jax.numpy as jnp
from jax import lax
from jax.experimental import pallas as pl
from jax.experimental.pallas import tpu as pltpu
from jax.sharding import PartitionSpec as P

MESH = pl.DeviceIdType.MESH
F32 = jnp.float32
BF16 = jnp.bfloat16
NEG = -1e30
B = 256
D = 4096
H = 16
DH = 128
T = 256
AB = 64
NC = 8
CS = B // NC
S = CS // 4
R = 2 * S
DC = D // 2
DY = DC // 2
QB = 512
NQ = H * DH // QB
QSCALE = DH ** -0.5 * math.log2(math.e)
GROUP = 8
MIB = 1024 * 1024
VIA_Y = 128
SCHEDULE = [(s[0], int(s[1])) for s in (
    "s0", "s1", "m0", "a2", "s2", "s3", "m1", "a4", "s4", "s5", "m2", "q0", "m3", "q1", "m4", "m5", "p0", "p1", "q2", "a6", "s6", "s7", "f0", "f1", "q3", "p2", "m6", "m7", "q4", "p3", "r0", "r1", "p4", "f2", "q5", "q6", "q7", "f3", "p5", "l0", "l1", "f4", "p6", "r2", "r3", "p7", "f5", "r4", "f6", "f7", "r5", "l2", "l4", "r6", "r7", "l3", "l5", "l6", "l7")]

def attention_stages(lens, first, q3, kbuf, vbuf, base, vbase, kv, o_ref, lse_ref, bufs):
    lane = lax.broadcasted_iota(jnp.int32, (H, DH), 1)
    pos = lax.broadcasted_iota(jnp.int32, (H, T), 1)
    zero = jnp.zeros((H, DH), BF16)
    s_a, s_b, p_a, p_b, r_a, r_b, n_a, n_b = bufs

    def score(i, s_out):
        for u in range(0, GROUP, 2):
            b = i * GROUP + u
            q0 = q3[pl.ds(pl.multiple_of(b * H, H), H), :].astype(BF16)
            q1 = q3[pl.ds(pl.multiple_of(b * H + H, H), H), :].astype(BF16)
            lhs = jnp.concatenate([jnp.concatenate([q0, zero], 1), jnp.concatenate([zero, q1], 1)], 0)
            keys = jnp.concatenate([kbuf[b - base], kbuf[b + 1 - base]], 1)
            s_out[u * H:(u + 2) * H, :] = lax.dot_general(lhs, keys, (((1,), (1,)), ((), ())), preferred_element_type=F32)

    def soften(i, s_in, p_out, r_out, n_out):
        chunk = lax.div(i * GROUP, CS)
        tile = pl.ds(pl.multiple_of(chunk * H, H), H)
        at = i * GROUP - chunk * CS
        lses = lse_ref[tile, :]
        for u in range(GROUP):
            b = i * GROUP + u
            row = lens[b] - first
            here = jnp.logical_and(row >= 0, row < T)
            k_new = kv[pl.ds(b, 1), :]
            v_new = kv[pl.ds(B + b, 1), :]
            q_row = q3[pl.ds(pl.multiple_of(b * H, H), H), :]
            s_new = jnp.where(here, jnp.sum(q_row * k_new, axis=1, keepdims=True) * QSCALE, NEG)
            se = jnp.where(pos < row, s_in[u * H:(u + 1) * H, :] * QSCALE, NEG)
            m = jnp.maximum(jnp.max(se, axis=1, keepdims=True), s_new)
            p = jnp.exp2(se - m)
            p_new = jnp.exp2(s_new - m)
            l = jnp.sum(p, axis=1, keepdims=True) + p_new
            r = 1.0 / l
            p_out[u * H:(u + 1) * H, :] = p.astype(BF16)
            r_out[u * H:(u + 1) * H, :] = jnp.broadcast_to(r, (H, DH))
            n_out[u * H:(u + 1) * H, :] = (p_new * r) * v_new
            lses = jnp.where(lane == at + u, m + jnp.log2(l), lses)
        lse_ref[tile, :] = lses

    def weigh(i, p_in, r_in, n_in):
        for u in range(0, GROUP, 2):
            b = i * GROUP + u
            vals = jnp.concatenate([vbuf[b - vbase], vbuf[b + 1 - vbase]], 1)
            o = jnp.dot(p_in[u * H:(u + 2) * H, :], vals, preferred_element_type=F32)
            for e in range(2):
                part = slice((u + e) * H, (u + e + 1) * H)
                o_ref[pl.ds(pl.multiple_of((b + e) * H, H), H), :] = (
                    o[e * H:(e + 1) * H, e * DH:(e + 1) * DH] * r_in[part, :] + n_in[part, :])

    def attend(k):
        tiles = slice(k * AB // CS * H, (k + 1) * AB // CS * H)
        lse_ref[tiles, :] = jnp.zeros((AB // CS * H, DH), F32)
        lo, hi = k * AB // GROUP, (k + 1) * AB // GROUP
        score(lo, s_a)
        score(lo + 1, s_b)
        soften(lo, s_a, p_a, r_a, n_a)

        def body(t):
            i = lo + 2 + 2 * t
            score(i, s_a)
            soften(i - 1, s_b, p_b, r_b, n_b)
            weigh(i - 2, p_a, r_a, n_a)
            score(i + 1, s_b)
            soften(i, s_a, p_a, r_a, n_a)
            weigh(i - 1, p_b, r_b, n_b)

        for t in range((hi - lo - 2) // 2):
            body(t)
        soften(hi - 1, s_b, p_b, r_b, n_b)
        weigh(hi - 2, p_a, r_a, n_a)
        weigh(hi - 1, p_b, r_b, n_b)

    return attend


STAGE_BUFS = [pltpu.VMEM((GROUP * H, T), F32)] * 2 + [pltpu.VMEM((GROUP * H, T), BF16)] * 2 + [pltpu.VMEM((GROUP * H, DH), F32)] * 4


def insert_rows(lens, first, kv, pairs, lo, hi, base):
    sub = lax.broadcasted_iota(jnp.int32, (16, DH), 0)

    def insert(b, _):
        row = lens[b] - first
        start = pl.multiple_of((jnp.clip(row, 0, T - 1) // 16) * 16, 16)
        hit = sub == row - start
        for c, buf in enumerate(pairs):
            new = kv[pl.ds(c * B + b, 1), :]
            old = buf[b - base, pl.ds(start, 16), :].astype(F32)
            buf[b - base, pl.ds(start, 16), :] = jnp.where(hit, new, old).astype(BF16)
        return 0

    lax.fori_loop(lo, hi, insert, 0, unroll=4)


def first_kernel(lens_hbm, hid_hbm, k_hbm, v_hbm, gain_hbm, bias_hbm, wq_hbm, bq_hbm, wkv_hbm, bkv_hbm,
                 q3, kv, o_ref, lse_ref, ko_hbm, vo_hbm,
                 lens, gain_ref, bias_ref, bq_ref, bkv_ref, h, mean_ref, rstd_ref, wq, wkv, kbuf, vbuf, b0, b1, b2, b3, b4, b5, b6, b7, wsem, csem, ssem):
    first = lax.axis_index("sq") * T
    small = [pltpu.make_async_copy(src, dst, ssem.at[e]) for e, (src, dst) in enumerate((
        (gain_hbm, gain_ref), (bias_hbm, bias_ref), (bkv_hbm, bkv_ref), (bq_hbm, bq_ref), (lens_hbm, lens)))]
    load_h = []
    for e in range(2):
        rows = pl.ds(e * (B // 2), B // 2)
        load_h.append(pltpu.make_async_copy(hid_hbm.at[rows], h.at[rows], wsem.at[NQ + e]))
        load_h[-1].start()
        if e == 0:
            for cp in small:
                cp.start()
    load_wkv = pltpu.make_async_copy(wkv_hbm, wkv, wsem.at[NQ + 2])
    load_wkv.start()
    load_wq = []
    for j in range(NQ):
        cols = pl.ds(j * QB, QB)
        load_wq.append(pltpu.make_async_copy(wq_hbm.at[:, cols], wq.at[:, cols], wsem.at[j]))
    loads = [pltpu.make_async_copy(src.at[pl.ds(0, AB)], dst, csem.at[e]) for e, (src, dst) in enumerate(((k_hbm, kbuf), (v_hbm, vbuf)))]
    for cp in [*load_wq[:-1], *loads, load_wq[-1]]:
        cp.start()
    small[0].wait()
    small[1].wait()

    def spread(tile):
        return jnp.concatenate([tile] * (D // DH), 1)

    def block(i):
        return pl.ds(pl.multiple_of(i * 16, 16), 16)

    def means(i, _):
        total = jnp.sum(h[block(i), :].astype(F32), axis=-1, keepdims=True)
        mean_ref[block(i), :] = jnp.broadcast_to(total * (1.0 / D), (16, DH))
        return 0

    def scales(i, _):
        cen = h[block(i), :].astype(F32) - spread(mean_ref[block(i), :])
        var = jnp.sum(cen * cen, axis=-1, keepdims=True) * (1.0 / D)
        rstd_ref[block(i), :] = jnp.broadcast_to(lax.rsqrt(var + 1e-5), (16, DH))
        return 0

    def normed(i, _):
        y = (h[block(i), :].astype(F32) - spread(mean_ref[block(i), :])) * spread(rstd_ref[block(i), :])
        h[block(i), :] = (y * gain_ref[...] + bias_ref[...]).astype(BF16)
        return 0

    for e in range(2):
        load_h[e].wait()
        lo, hi = e * (B // 32), (e + 1) * (B // 32)
        lax.fori_loop(lo, hi, means, 0, unroll=4)
        lax.fori_loop(lo, hi, scales, 0, unroll=4)
        lax.fori_loop(lo, hi, normed, 0, unroll=2)
    load_wkv.wait()
    for cp in small[2:]:
        cp.wait()
    load_wq[0].wait()
    new_kv = (jnp.dot(h[...], wkv[...], preferred_element_type=F32) + bkv_ref[...]).astype(BF16).astype(F32)
    kv[0:B, :] = new_kv[:, :DH]
    kv[B:2 * B, :] = new_kv[:, DH:]
    stores = [pltpu.make_async_copy(src, dst.at[pl.ds(0, AB)], csem.at[2 + e]) for e, (src, dst) in enumerate(((kbuf, ko_hbm), (vbuf, vo_hbm)))]
    for j in range(NQ):
        cols = pl.ds(j * QB, QB)
        q = jnp.dot(h[...], wq[:, cols], preferred_element_type=F32) + bq_ref[:, cols]
        q = q.astype(BF16).astype(F32)
        if j < NQ - 2:
            load_wq[j + 1].wait()
        for n in range(QB // DH):
            q3[pl.ds(j * (QB // DH) + n, B, stride=H), :] = q[:, n * DH:(n + 1) * DH]
        if j == NQ - 2:
            for c in loads:
                c.wait()
            insert_rows(lens, first, kv, (kbuf, vbuf), 0, AB, 0)
            for c in stores:
                c.start()
            load_wq[j + 1].wait()
    attention_stages(lens, first, q3, kbuf, vbuf, 0, 0, kv, o_ref, lse_ref, (b0, b1, b2, b3, b4, b5, b6, b7))(0)
    for c in stores:
        c.wait()


def column(tile, j):
    return tile[:, j:j + 1]


def merge(la, lb):
    top = jnp.maximum(la, lb)
    wa, wb = jnp.exp2(la - top), jnp.exp2(lb - top)
    tot = wa + wb
    return wa / tot, wb / tot, top + jnp.log2(tot)


def exchange_kernel(lens_hbm, q3, kv, o_first, lse_first, k_hbm, v_hbm, wo_hbm, y_ref, held,
                    lens, wo, o_ref, lse_ref, b0, b1, b2, b3, b4, b5, b6, b7, o_core, l_core, o_mix, l_mix, l_half, o_x, l_x, a_all, part, p_y,
                    wsem, csem, nsem, a0s, a0r, a1s, a1r, a2s, a2r, bs, br, cs, cr, ds, dr):
    sq, tp = lax.axis_index("sq"), lax.axis_index("tp")
    x, c = sq // 2, sq % 2
    mate = {"sq": x * 2 + 1 - c}
    over_x = {"sq": (1 - x) * 2 + c}
    over_y = {"tp": 1 - tp}
    loads = {}
    bar = pltpu.get_barrier_semaphore()
    for dev in (mate, over_x, over_y):
        pl.semaphore_signal(bar, inc=1, device_id=dev, device_id_type=MESH)
    load_lens = pltpu.make_async_copy(lens_hbm, lens, nsem)
    load_lens.start()

    def fetch(k):
        rows = pl.ds(k * AB, AB)
        loads[k] = [pltpu.make_async_copy(src.at[rows], held.at[pl.ds((k - 1) * AB + e * (B - AB), AB)], csem.at[2 * k + e - 2])
                    for e, src in enumerate((k_hbm, v_hbm))]
        for cp in loads[k]:
            cp.start()

    fetch(1)
    fetch(2)
    load = pltpu.make_async_copy(wo_hbm.at[:, pl.ds(pl.multiple_of(c * DC, DC), DC)], wo, wsem)
    load.start()
    fetch(3)
    load_lens.wait()
    pl.semaphore_wait(bar, 3)

    def send(src, dst, ssem, rsem, dev):
        cp = pltpu.make_async_remote_copy(src, dst, ssem, rsem, device_id=dev, device_id_type=MESH)
        cp.start()
        return cp

    W = S * H
    hop0, hop1, hop2, hopb, hopc, hopd = {}, {}, {}, {}, {}, {}
    stages = attention_stages(lens, sq * T, q3, held, held, AB, AB - (B - AB), kv, o_ref, lse_ref, (b0, b1, b2, b3, b4, b5, b6, b7))
    ready = []
    lane8 = lax.broadcasted_iota(jnp.int32, (H // 2, DH), 1)

    def attend(k):
        block = k * CS // AB
        for cp in loads[block]:
            cp.wait()
        stages(block)

    def source(k):
        return (o_first, lse_first) if k * CS < AB else (o_ref, lse_ref)

    def rows_of_o(k, xx, cc):
        return pl.ds(pl.multiple_of((k * 4 + xx * 2 + cc) * W, W), W)

    def share(k):
        o_k, l_k = source(k)
        hop0[k] = [send(o_k.at[rows_of_o(k, xx, 1 - c)], o_core.at[k, xx], a0s.at[k, xx], a0r.at[k, xx], mate) for xx in range(2)]
        hop0[k].append(send(l_k.at[pl.ds(k * H, H)], l_core.at[k], a0s.at[k, 2], a0r.at[k, 2], mate))

    def mix(k):
        o_k, l_k = source(k)
        for cp in hop0[k]:
            cp.wait_recv()
        shift = lax.rem(DH - c * S, DH)
        fa, fb, lm = merge(pltpu.roll(l_k[pl.ds(k * H, H), :], shift, 1), pltpu.roll(l_core[k], shift, 1))
        l_mix[k] = lm
        theirs = pltpu.roll(lm, lax.rem(DH - (1 - x) * R, DH), 1)
        l_half[k] = jnp.where(lane8 < S, theirs[:H // 2], pltpu.roll(theirs[H // 2:], S, 1))
        for xx in range(2):
            mine = (k * 4 + xx * 2 + c) * W
            for j in range(S):
                oa = o_k[pl.ds(pl.multiple_of(mine + j * H, H), H), :]
                ob = o_core[k, xx, j * H:(j + 1) * H, :]
                at = xx * R + j
                o_mix[k, xx, j * H:(j + 1) * H, :] = column(fa, at) * oa + column(fb, at) * ob
        hop1[k] = [send(o_mix.at[k, 1 - x], o_x.at[k], a1s.at[k, 0], a1r.at[k, 0], over_x),
                   send(l_half.at[k], l_x.at[k], a1s.at[k, 1], a1r.at[k, 1], over_x)]

    def quarter(k):
        for cp in hop1[k]:
            cp.wait_recv()
        shift = lax.rem(DH - x * R, DH)
        l_far = jnp.concatenate([l_x[k], pltpu.roll(l_x[k], DH - S, 1)], 0)
        fa, fb, _ = merge(pltpu.roll(l_mix[k], shift, 1), l_far)
        for j in range(S):
            oa = o_mix[k, x, j * H:(j + 1) * H, :]
            ob = o_x[k, j * H:(j + 1) * H, :]
            a_all[k, pl.ds(pl.multiple_of(c * W + j * H, H), H), :] = column(fa, j) * oa + column(fb, j) * ob
        own = pl.ds(pl.multiple_of(c * W, W), W)
        hop2[k] = send(a_all.at[k, own], a_all.at[k, own], a2s.at[k], a2r.at[k], mate)

    def project(k):
        hop2[k].wait_recv()
        a = jnp.concatenate([a_all[k, pl.ds(n, R, stride=H), :].astype(BF16) for n in range(H)], 1)
        if not ready:
            load.wait()
            ready.append(1)
        theirs, ours = (pl.ds(pl.multiple_of(t * DY, DY), DY) for t in (1 - tp, tp))
        part[k, :, theirs] = jnp.dot(a, wo[:, theirs], preferred_element_type=F32)
        hopb[k] = send(part.at[k, :, theirs], p_y.at[k], bs.at[k], br.at[k], over_y)
        part[k, :, ours] = jnp.dot(a, wo[:, ours], preferred_element_type=F32)

    def piece(k, xx, yy, lo=0, width=DY):
        return (pl.ds(pl.multiple_of(k * CS + xx * R, R), R), pl.ds(pl.multiple_of(c * DC + yy * DY + lo, 128), width))

    def pass_on(at, ssem, rsem, dev):
        return send(y_ref.at[at], y_ref.at[at], ssem, rsem, dev)

    def finish(k):
        hopb[k].wait_recv()
        at = piece(k, x, tp)
        y_ref[at] = part[k, :, pl.ds(pl.multiple_of(tp * DY, DY), DY)] + p_y[k]
        hopc[k] = [pass_on(at, cs.at[k, 0], cr.at[k, 0], over_x), pass_on(at, cs.at[k, 1], cr.at[k, 1], over_y)]
        hopd[k] = [pass_on(at, ds.at[k, 0], dr.at[k, 0], mate)]

    def relay(k):
        hopc[k][1].wait_recv()
        hopc[k].append(pass_on(piece(k, x, 1 - tp, VIA_Y, DY - VIA_Y), cs.at[k, 2], cr.at[k, 2], over_x))
        hopd[k].append(pass_on(piece(k, x, 1 - tp), ds.at[k, 1], dr.at[k, 1], mate))
        hopc[k][0].wait_recv()
        hopc[k].append(pass_on(piece(k, 1 - x, tp, 0, VIA_Y), cs.at[k, 3], cr.at[k, 3], over_y))
        hopd[k].append(pass_on(piece(k, 1 - x, tp), ds.at[k, 2], dr.at[k, 2], mate))

    def last(k):
        hopc[k][2].wait_recv()
        hopc[k][3].wait_recv()
        hopd[k].append(pass_on(piece(k, 1 - x, 1 - tp), ds.at[k, 3], dr.at[k, 3], mate))

    for step, k in SCHEDULE:
        {"a": attend, "s": share, "m": mix, "q": quarter, "p": project, "f": finish, "r": relay, "l": last}[step](k)
    for k in range(NC):
        for cp in hopd[k]:
            cp.wait_recv()
    for k in range(NC):
        for cp in [*hop0[k], *hop1[k], hop2[k], hopb[k], *hopc[k], *hopd[k]]:
            cp.wait_send()


def last_kernel(lens_hbm, kv, y_in, hid, bo_ref, held_in, k_part, v_part, ko_hbm, vo_hbm, out_hbm, held, lens, out, sem, osem, nsem):
    load_lens = pltpu.make_async_copy(lens_hbm, lens, nsem)
    load_lens.start()

    def rows(i, _):
        r = pl.ds(pl.multiple_of(i * 16, 16), 16)
        out[r, :] = (hid[r, :].astype(F32) + y_in[r, :] + bo_ref[...]).astype(BF16)
        return 0

    half = B // 2
    store_out = []

    def finish_rows(e):
        lax.fori_loop(e * (B // 32), (e + 1) * (B // 32), rows, 0, unroll=2)
        store_out.append(pltpu.make_async_copy(out.at[pl.ds(e * half, half)], out_hbm.at[pl.ds(e * half, half)], osem.at[e]))
        store_out[-1].start()

    finish_rows(0)
    load_lens.wait()
    first = lax.axis_index("sq") * T
    n = B - AB
    copies = []

    def put(lo, hi):
        insert_rows(lens, first, kv, (held.at[pl.ds(0, n)], held.at[pl.ds(n, n)]), lo, hi, AB)
        for e, dst in enumerate((ko_hbm, vo_hbm)):
            copies.append(pltpu.make_async_copy(held.at[pl.ds(e * n + lo - AB, hi - lo)], dst.at[pl.ds(lo, hi - lo)], sem.at[len(copies)]))
            copies[-1].start()

    put(64, 80)
    put(80, 96)
    put(96, 128)
    finish_rows(1)
    put(128, 192)
    put(192, 256)
    for cp in store_out + copies:
        cp.wait()


def solution(mesh):
    def local_step(hidden, cache_lens, k_cache, v_cache, ln_gain, ln_bias, w_query, b_query, w_kv, b_kv, w_out, b_out):
        hbm = pl.BlockSpec(memory_space=pltpu.HBM)
        vm = pl.BlockSpec(memory_space=pltpu.VMEM)
        smem = pl.BlockSpec(memory_space=pltpu.SMEM)
        sem = pltpu.SemaphoreType.DMA

        def pin(*arrays):
            return [pltpu.with_memory_space_constraint(a, pltpu.VMEM) for a in arrays]

        def far(*arrays):
            return [pltpu.with_memory_space_constraint(a, pltpu.HBM) for a in arrays]

        cache = jax.ShapeDtypeStruct((B, T, DH), BF16)
        q3, kv, o0, lse0, k_part, v_part = pl.pallas_call(
            first_kernel,
            out_shape=(pltpu.VMEM((B * H, DH), F32), pltpu.VMEM((2 * B, DH), F32), pltpu.VMEM((AB * H, DH), F32), pltpu.VMEM((AB // CS * H, DH), F32), cache, cache),
            in_specs=[hbm] * 10,
            out_specs=(vm, vm, vm, vm, hbm, hbm),
            scratch_shapes=[
                pltpu.SMEM((B,), jnp.int32), pltpu.VMEM((1, D), F32), pltpu.VMEM((1, D), F32), pltpu.VMEM((1, H * DH), F32), pltpu.VMEM((1, 2 * DH), F32),
                pltpu.VMEM((B, D), BF16), pltpu.VMEM((B, DH), F32), pltpu.VMEM((B, DH), F32), pltpu.VMEM((D, H * DH), BF16), pltpu.VMEM((D, 2 * DH), BF16),
                pltpu.VMEM((AB, T, DH), BF16), pltpu.VMEM((AB, T, DH), BF16), *STAGE_BUFS, sem((NQ + 3,)), sem((4,)), sem((5,)),
            ],
            compiler_params=pltpu.CompilerParams(vmem_limit_bytes=33 * MIB),
            name="first",
        )(*far(cache_lens, hidden, k_cache, v_cache, ln_gain[None], ln_bias[None], w_query, b_query[None], w_kv, b_kv[None]))
        held = pltpu.VMEM((2 * (B - AB), T, DH), BF16)
        y, kv_held = pl.pallas_call(
            exchange_kernel,
            out_shape=(pltpu.VMEM((B, D), F32), held),
            in_specs=[hbm, vm, vm, vm, vm, hbm, hbm, hbm],
            out_specs=(vm, vm),
            scratch_shapes=[
                pltpu.SMEM((B,), jnp.int32),
                pltpu.VMEM((H * DH, DC), BF16), pltpu.VMEM((B * H, DH), F32), pltpu.VMEM((NC * H, DH), F32), *STAGE_BUFS,
                pltpu.VMEM((NC, 2, S * H, DH), F32), pltpu.VMEM((NC, H, DH), F32),
                pltpu.VMEM((NC, 2, S * H, DH), F32), pltpu.VMEM((NC, H, DH), F32), pltpu.VMEM((NC, H // 2, DH), F32),
                pltpu.VMEM((NC, S * H, DH), F32), pltpu.VMEM((NC, H // 2, DH), F32),
                pltpu.VMEM((NC, R * H, DH), F32), pltpu.VMEM((NC, R, DC), F32), pltpu.VMEM((NC, R, DY), F32),
                sem, sem((2 * (B // AB) - 2,)), sem, sem((NC, 3)), sem((NC, 3)), sem((NC, 2)), sem((NC, 2)), sem((NC,)), sem((NC,)),
                sem((NC,)), sem((NC,)), sem((NC, 4)), sem((NC, 4)), sem((NC, 4)), sem((NC, 4)),
            ],
            compiler_params=pltpu.CompilerParams(vmem_limit_bytes=24 * MIB, collective_id=0, has_side_effects=True),
            name="exchange",
        )(*far(cache_lens), *pin(q3, kv, o0, lse0), *far(k_cache, v_cache, w_out))
        k_new, v_new, out_hidden, _ = pl.pallas_call(
            last_kernel,
            out_shape=(cache, cache, jax.ShapeDtypeStruct((B, D), BF16), held),
            in_specs=[hbm, vm, vm, vm, vm, vm, hbm, hbm],
            out_specs=(hbm, hbm, hbm, vm),
            input_output_aliases={5: 3, 6: 0, 7: 1},
            scratch_shapes=[pltpu.SMEM((B,), jnp.int32), pltpu.VMEM((B, D), BF16), sem((10,)), sem((2,)), sem],
            compiler_params=pltpu.CompilerParams(vmem_limit_bytes=6 * MIB),
            name="last",
        )(*far(cache_lens), *pin(kv, y), hidden, b_out[None], *pin(kv_held), k_part, v_part)
        return out_hidden, k_new, v_new

    cache_spec = P("dp", "sq", None)
    row_spec = P("dp", None)
    in_specs = (row_spec, P("dp"), cache_spec, cache_spec, P(None), P(None), P(None, "tp"), P("tp"), P(None, None), P(None), P("tp", None), P(None))
    out_specs = (row_spec, cache_spec, cache_spec)
    return jax.shard_map(local_step, mesh=mesh, in_specs=in_specs, out_specs=out_specs, check_vma=False)
```
